512 devices in a mesh: bead: 16 (over z_lo, core), slab: 32 (over z_hi, x, y).
Axes of the slice: x: 4, y: 4, z: 16 (z_hi: 2, z_lo: 8; z = z_hi * 8 + z_lo), core: 2. Of those that a mesh axis runs over, the one named last changes fastest.
Arguments:
- positions: float32 [64, 3, 32768], P('bead', None, 'slab'), may hold values from -0.4 to 64.4, as said below
- velocities: float32 [64, 3, 32768], P('bead', None, 'slab'), may hold values from -5 to 5
- masses: float32 [32768], P('slab'), may hold values from 1 to 16
- amplitudes: float32 [32768], P('slab'), may hold values from 0.15 to 0.6
- charges: float32 [32768], P('slab'), may hold values from -1.2 to 1.2
Outputs:
- moved: float32 [64, 3, 32768], P('bead', None, 'slab')
- final_velocities: float32 [64, 3, 32768], P('bead', None, 'slab')
The draws below stay inside these ranges and needn't reach their ends.
Inputs may be any that keep to these rules, and one draw needn't show every extreme that they name: `positions`: atom n's beads lie within 0.4 of its cell: plane n // 512 spans first coordinates from its index to its index plus one, and cell (n % 512) // 128 = 2 a + e of that plane spans second coordinates a to a + 1 and third coordinates e to e + 1.
All inputs are finite; a program needn't handle non-finite values.
Results may differ from the reference program's by a relative error of at most 0.0003.
Values sent between devices are 32-bit elements; how exact they have to be, the bound alone decides.
No kernel may reach another device: no remote copies, remote signals or barrier semaphores. Data moves between devices by JAX's collectives and lax.ppermute only.
A program may use at most 64 MiB of HBM per device.

```python
import math
import jax
import jax.numpy as jnp
from jax import lax

CELL_ATOMS = 128
INNER_STEPS = 2
OUTER_STEPS = 2
PLANE_ATOMS = 512
BEADS = 64
CBEADS = 16
ATOMS = 32768


def draw_positions(key, part):
    first_key = jax.random.fold_in(key, 11)
    second_key = jax.random.fold_in(key, 23)
    third_key = jax.random.fold_in(key, 37)
    fourth_key = jax.random.fold_in(key, 41)
    index = jnp.arange(ATOMS, dtype=jnp.int32)
    plane = (index // PLANE_ATOMS).astype(jnp.float32)
    cell = index % PLANE_ATOMS // CELL_ATOMS
    corner = jnp.stack([plane, (cell // 2).astype(jnp.float32), (cell % 2).astype(jnp.float32)])
    centre = corner + jax.random.uniform(first_key, (3, ATOMS), jnp.float32)
    mode_count = CBEADS // 2 - 1
    modes = jnp.arange(1, mode_count + 1, dtype=jnp.float32)
    cycle_place = 2.0 * jnp.pi * jnp.arange(BEADS, dtype=jnp.float32) / BEADS
    angle = modes[:, None] * cycle_place[None, :]
    cosine = jnp.cos(angle)
    sine = jnp.sin(angle)
    factor = 0.15 / mode_count ** 0.5
    cos_coef = factor * jax.random.normal(second_key, (mode_count, 3, ATOMS), jnp.float32)
    sin_coef = factor * jax.random.normal(third_key, (mode_count, 3, ATOMS), jnp.float32)
    rough = jax.random.uniform(fourth_key, (BEADS, 3, ATOMS), jnp.float32, -0.08, 0.08)
    smooth = jnp.einsum('kb,kca->bca', cosine, cos_coef, precision=lax.Precision.HIGHEST)
    smooth = smooth + jnp.einsum('kb,kca->bca', sine, sin_coef, precision=lax.Precision.HIGHEST)
    spread = 0.3 * jnp.tanh(smooth / 0.3) + rough
    return centre[None] + spread


def level_of(own_key, shape, pieces, low, largest):
    def one(position, blocks):
        draws = jax.random.uniform(jax.random.fold_in(jax.random.fold_in(own_key, 6), position), (blocks,), jnp.float32, low / len(pieces), largest / len(pieces))
        return jnp.repeat(jnp.exp(draws), shape[position] // blocks).reshape((-1,) + (1,) * (len(shape) - position - 1))

    loudness = one(*pieces[0])
    for cut in pieces[1:]:
        loudness = loudness * one(*cut)
    return loudness


def gaussian(own_key, shape, scale, most, shards=(), kind=jnp.bfloat16):
    array = scale * jax.random.normal(own_key, shape, jnp.float32)
    if shards:
        array = array * level_of(own_key, shape, shards, -0.22, 0.18)
    return jnp.clip(array, -most, most).astype(kind)


def setup_inputs(seed: int = 0) -> dict:
    splits = jax.random.split(jax.random.key(seed), 6)
    positions = draw_positions(jax.random.fold_in(splits[5], 71), 0)
    velocities = gaussian(splits[1], (BEADS, 3, ATOMS), 1.0, 5.0, ((0, 16), (2, 32)), jnp.float32)
    masses = jnp.clip(jnp.exp(math.log(16.0) - 2.7725887 * jax.random.uniform(splits[2], (ATOMS,), jnp.float32) ** level_of(splits[2], (ATOMS,), ((0, 32),), -0.2, 0.2)), 1.0, 16.0)
    amplitudes = jnp.clip(jnp.exp(math.log(0.6) - 1.3862944 * jax.random.uniform(splits[3], (ATOMS,), jnp.float32) ** level_of(splits[3], (ATOMS,), ((0, 32),), -0.2, 0.2)), 0.15, 0.6)
    charges = jnp.clip(jax.random.uniform(splits[4], (ATOMS,), jnp.float32, -1.2, 1.2) * level_of(splits[4], (ATOMS,), ((0, 32),), -0.4, 0.0), -1.2, 1.2)
    return {"positions": positions, "velocities": velocities, "masses": masses, "amplitudes": amplitudes, "charges": charges}


time_step = 0.05
spring_rate = 25.0
near_scale = 4.0
far_scale = 2.0


def contraction(bead_count, small_count):
    bead_place = jnp.arange(bead_count, dtype=jnp.float32) / bead_count
    small_place = jnp.arange(small_count, dtype=jnp.float32) / small_count
    phase = 2.0 * jnp.pi * (bead_place[None, :] - small_place[:, None])
    modes = jnp.arange(1, small_count // 2, dtype=jnp.float32)
    total = 1.0 + jnp.cos(0.5 * small_count * phase) + 2.0 * jnp.sum(jnp.cos(modes[:, None, None] * phase[None]), axis=0)
    return total / bead_count


def pair_force(targets, sources, target_share, source_share, scale):
    between = targets[..., :, :, None] - sources[..., :, None, :]
    square = jnp.sum(between * between, axis=-3)
    weight = target_share[:, None] * source_share[None, :] * jnp.exp(-0.5 * scale * square) * scale
    return jnp.sum(weight[..., None, :, :] * between, axis=-1)


def field_forces(coords, shares, reach, scale):
    plane_size = PLANE_ATOMS
    planes_total = ATOMS // PLANE_ATOMS
    margin = reach * plane_size
    offset = jnp.concatenate([jnp.full((margin,), -float(planes_total), jnp.float32), jnp.zeros((ATOMS,), jnp.float32), jnp.full((margin,), float(planes_total), jnp.float32)])
    shift = jnp.stack([offset, jnp.zeros_like(offset), jnp.zeros_like(offset)])
    extended = jnp.concatenate([coords[..., -margin:], coords, coords[..., :margin]], axis=-1) + shift
    shares_wide = jnp.concatenate([shares[-margin:], shares, shares[:margin]])
    width = (2 * reach + 1) * plane_size

    def one_plane(plane):
        start = plane * plane_size
        targets = lax.dynamic_slice_in_dim(coords, start, plane_size, 2)
        sources = lax.dynamic_slice_in_dim(extended, start, width, 2)
        target_share = lax.dynamic_slice_in_dim(shares, start, plane_size, 0)
        source_share = lax.dynamic_slice_in_dim(shares_wide, start, width, 0)
        return pair_force(targets, sources, target_share, source_share, scale)

    forces = lax.map(one_plane, jnp.arange(planes_total, dtype=jnp.int32))
    return jnp.transpose(forces, (1, 2, 0, 3)).reshape(coords.shape)


def reference(positions, velocities, masses, amplitudes, charges):
    table = contraction(BEADS, CBEADS)

    def fast(coords):
        springs = 2.0 * coords - jnp.roll(coords, 1, 0) - jnp.roll(coords, -1, 0)
        return field_forces(coords, amplitudes, 1, near_scale) - spring_rate * masses * springs

    def slow(coords):
        contracted = jnp.einsum("cb,bka->cka", table, coords, precision=lax.Precision.HIGHEST)
        far = field_forces(contracted, charges, 2, far_scale)
        return (BEADS / CBEADS) * jnp.einsum("cb,cka->bka", table, far, precision=lax.Precision.HIGHEST)

    inverse = 1.0 / masses
    outer_dt = INNER_STEPS * time_step
    coords = positions
    speeds = velocities
    quick = fast(coords)
    gentle = slow(coords)
    for outer_step in range(OUTER_STEPS):
        speeds = speeds + 0.5 * outer_dt * gentle * inverse
        for inner_step in range(INNER_STEPS):
            speeds = speeds + 0.5 * time_step * quick * inverse
            coords = coords + time_step * speeds
            quick = fast(coords)
            speeds = speeds + 0.5 * time_step * quick * inverse
        gentle = slow(coords)
        speeds = speeds + 0.5 * outer_dt * gentle * inverse
    return coords - positions, speeds
```

```python
import math

import jax
import jax.numpy as jnp
import numpy as np
from jax import lax
from jax.experimental import pallas as pl
from jax.experimental.pallas import tpu as pltpu
from jax.sharding import Mesh, PartitionSpec as P

TIME_STEP = 0.05
OUTER_STEP = 0.1
SPRING = 25.0
NEAR = 4.0
FAR = 2.0
BEADS = 64
CBEADS = 16
SLABS = 32
MINE = BEADS // CBEADS
STEP = 256
WIDTH = 256
AHEAD = 4

X_ROWS = 0
V_ROWS = 96
M_ROW = 192
A_ROW = 200
Q_ROW = 208
PACKED = 216

AXES = ("z2", "z1", "z0", "core", "zh", "x1", "x0", "y1", "y0")
TEAM = ("x0", "y1", "y0", "core")
f32 = jnp.float32
bf16 = jnp.bfloat16


def _place():
    ring = [(0, z) for z in range(16)] + [(1, z) for z in range(15, -1, -1)]
    cycle = [(0, 0), (0, 1), (0, 2), (0, 3), (1, 3), (1, 2), (1, 1), (1, 0)]
    device = np.zeros((CBEADS, SLABS), np.int64)
    role = np.zeros((512, 2), np.int64)
    member = np.zeros((2, 16), np.int64)
    half_of = np.zeros(SLABS, np.int64)
    for s in range(SLABS):
        half, z = ring[(s - 8) % SLABS]
        half_of[s] = half
        for b in range(CBEADS):
            q, core = divmod(b, 2)
            xx, y = cycle[q]
            x = xx if half == 0 else 3 - xx
            d = ((z % 8) * 2 + core) * 32 + (z // 8) * 16 + x * 4 + y
            device[b, s] = d
            role[d] = (b, s)
            member[half, (x % 2) * 8 + y * 2 + core] = b
    return device, role, member, half_of


DEVICE, ROLE, MEMBER, HALF = _place()


def _table():
    b = np.arange(BEADS)[None, :] / BEADS
    c = np.arange(CBEADS)[:, None] / CBEADS
    t = 2.0 * np.pi * (b - c)
    total = 1.0 + np.cos(0.5 * CBEADS * t)
    for k in range(1, CBEADS // 2):
        total = total + 2.0 * np.cos(k * t)
    return (total / BEADS).astype(np.float32)


def _settings():
    table = _table()
    out = np.zeros((CBEADS * SLABS, 128), np.float32)
    for d in range(CBEADS * SLABS):
        b, s = ROLE[d]
        out[d, : 16 * MINE] = table[MEMBER[HALF[s]]][:, b * MINE : (b + 1) * MINE].reshape(-1)
        out[d, SLAB_AT] = s
        out[d, CORE_AT] = b % 2
    return out


SLAB_AT = 16 * MINE
CORE_AT = SLAB_AT + 1
SETTINGS = _settings()


def _moves(f):
    return [
        (int(DEVICE[b, s]), int(DEVICE[f(b, s)]))
        for b in range(CBEADS)
        for s in range(SLABS)
    ]


SLAB_UP = _moves(lambda b, s: (b, (s + 1) % SLABS))
SLAB_DOWN = _moves(lambda b, s: (b, (s - 1) % SLABS))
BEAD_SWAP = _moves(lambda b, s: ((b + (1 if b % 2 else -1)) % CBEADS, s))
MOVE_IN = [(b * SLABS + s, int(DEVICE[b, s])) for b in range(CBEADS) for s in range(SLABS)]
MOVE_OUT = [(d, h) for h, d in MOVE_IN]


def pieces(v):
    high = v.astype(bf16).astype(f32)
    rest = v - high
    mid = rest.astype(bf16).astype(f32)
    return high, mid, rest - mid


def halves(lower, upper):
    return jnp.concatenate([lower, upper], axis=0)


def put(ref, row, value):
    ref[pl.ds(row, 8, stride=8), :] = value


def wide(ref):
    return jnp.concatenate([ref[8 * k : 8 * k + 8, :] for k in range(8)], axis=1)


def init_rows(src, tgt):
    ones = jnp.ones((8, 128), f32)
    zeros = jnp.zeros((8, 128), f32)
    put(src, 4, ones)
    put(tgt, 3, ones)
    for k in range(5, 8):
        put(src, k, zeros)
        put(tgt, k, zeros)


def scaled(coords, scale):
    alpha = math.sqrt(scale * math.log2(math.e))
    a = [alpha * y for y in coords]
    return a, -0.5 * (a[0] * a[0] + a[1] * a[1] + a[2] * a[2])


def put_sources(src, qs, lhs, coords, share, scale):
    a, norm = scaled(coords, scale)
    for k, v in enumerate(a + [norm]):
        put(src, k, v)
    for k, v in enumerate([share] + [share * y for y in coords]):
        put(qs, k, v)
        put(qs, 4 + k, v)
    high, mid, low = pieces(wide(src))
    rows = jnp.concatenate([high, high, mid, mid, high, low], axis=0)
    for block in range(8):
        part = slice(128 * block, 128 * block + 128)
        lhs[part, :] = rows[:, part].T.astype(bf16)
    high, mid, low = pieces(wide(qs))
    upper = lax.broadcasted_iota(jnp.int32, (8, 1024), 0) < 4
    return jnp.concatenate([jnp.where(upper, high, mid), jnp.where(upper, low, 0.0)], axis=0).astype(bf16)


def put_targets(tgt, coords, scale):
    a, norm = scaled(coords, scale)
    for k, v in enumerate(a):
        put(tgt, k, v)
    put(tgt, 4, norm)
    high, mid, low = pieces(wide(tgt))
    return jnp.concatenate([high, mid, high, mid, low, high], axis=0).astype(bf16)


def stream(tasks, ahead=AHEAD):
    totals = {}
    ready = []
    for t in range(len(tasks) + ahead):
        if t < len(tasks):
            lhs, first, rhs, q, key = tasks[t]
            ready.append(jnp.dot(lhs[first : first + STEP, :], rhs, preferred_element_type=f32))
        if t < ahead:
            continue
        lhs, first, rhs, q, key = tasks[t - ahead]
        weight = jnp.exp2(ready[t - ahead])
        high = weight.astype(bf16)
        low = (weight - high.astype(f32)).astype(bf16)
        mine = q[:, first : first + STEP]
        part = jnp.dot(mine, high, preferred_element_type=f32)
        part = part + jnp.dot(mine, low, preferred_element_type=f32)
        totals[key] = totals[key] + part if key in totals else part
    return totals


def chunks(lhs, first, last, rhs, start, stop, q, key):
    return [
        (lhs, j, rhs[:, i : i + WIDTH], q, (key, i))
        for j in range(first, last, STEP)
        for i in range(start, stop, WIDTH)
    ]


def joined(totals, key):
    return jnp.concatenate([totals[key, i] for i in range(0, 1024, WIDTH)], axis=1)


def sums_of(total, rows):
    r = total[0:8]
    r = r + jnp.concatenate([r[4:8], r[0:4]], axis=0) + total[8:16]
    for block in range(8):
        rows[8 * block : 8 * block + 8, :] = r[:, 128 * block : 128 * block + 128]
    return [rows[pl.ds(k, 8, stride=8), :] for k in range(4)]


def field(coords, sums, share, scale):
    return [share * scale * (coords[k] * sums[0] - sums[1 + k]) for k in range(3)]


def slot(scr, i):
    return scr[5 * i : 5 * i + 5]


SCRATCH = 2 * [
    pltpu.VMEM((64, 128), f32),
    pltpu.VMEM((64, 128), f32),
    pltpu.VMEM((64, 128), f32),
    pltpu.VMEM((1024, 48), bf16),
    pltpu.VMEM((64, 128), f32),
]


def bead_at(ref, b):
    return [ref[pl.ds(24 * b + 8 * k, 8), :] for k in range(3)]


def near_own_kernel(y_ref, p_ref, out_ref, *scr):
    share = p_ref[A_ROW : A_ROW + 8, :]
    for i in range(2):
        init_rows(*slot(scr, i)[:2])

    def two(i, carry):
        tasks = []
        for j in range(2):
            src, tgt, qs, lhs, rows = slot(scr, j)
            coords = bead_at(y_ref, 2 * i + j)
            q = put_sources(src, qs, lhs, coords, share, NEAR)
            rhs = put_targets(tgt, coords, NEAR)
            tasks += chunks(lhs, 0, 1024, rhs, 0, 1024, q, j)
        totals = stream(tasks)
        for j in range(2):
            for k, r in enumerate(sums_of(joined(totals, j), slot(scr, j)[4])):
                out_ref[pl.ds(64 * i + 32 * j + 8 * k, 8), :] = r
        return carry

    lax.fori_loop(0, MINE // 2, two, 0)


def emit(y_refs, up_ref, down_ref, inner_ref, outer_ref, core):
    for i in range(12):
        y = y_refs[8 * i : 8 * i + 8, :]
        down_ref[4 * i : 4 * i + 4, :] = y[0:4]
        up_ref[4 * i : 4 * i + 4, :] = y[4:8]
    first = y_refs[0:24, :]
    last = y_refs[72:96, :]
    odd = core > 0.5
    inner_ref[...] = jnp.where(odd, first, last)
    outer_ref[...] = jnp.where(odd, last, first)


def emit_partial(y_refs, cols_ref, part_ref):
    y = [y_refs[24 * b : 24 * b + 24, :] for b in range(MINE)]
    for r in range(16):
        total = cols_ref[0, MINE * r] * y[0]
        for b in range(1, MINE):
            total = total + cols_ref[0, MINE * r + b] * y[b]
        part_ref[24 * r : 24 * r + 24, :] = total


def pack_kernel(x_ref, v_ref, m_ref, a_ref, q_ref, out_ref):
    for base, ref in ((X_ROWS, x_ref), (V_ROWS, v_ref)):
        for k in range(3):
            for block in range(8):
                row = base + 8 * k + block
                out_ref[pl.ds(row, 4, stride=24), :] = ref[k, :, 128 * block : 128 * block + 128]
    out_ref[M_ROW : M_ROW + 8, :] = m_ref[...]
    out_ref[A_ROW : A_ROW + 8, :] = a_ref[...]
    out_ref[Q_ROW : Q_ROW + 8, :] = q_ref[...]


def unpack(value_ref, out_ref):
    for k in range(3):
        for block in range(8):
            out_ref[k, :, 128 * block : 128 * block + 128] = value_ref[pl.ds(8 * k + block, 4, stride=24), :]


def start_kernel(cols_ref, p_ref, y_ref, up_ref, down_ref, inner_ref, outer_ref, part_ref):
    centre = 2.0 * cols_ref[0, SLAB_AT] + 1.0
    for b in range(MINE):
        for k in range(3):
            i = 8 * (3 * b + k)
            y_ref[i : i + 8, :] = p_ref[i : i + 8, :] - (centre if k == 0 else 1.0)
    emit(y_ref, up_ref, down_ref, inner_ref, outer_ref, cols_ref[0, CORE_AT])
    up_ref[48:64, :] = p_ref[A_ROW : A_ROW + 16, :]
    down_ref[48:64, :] = p_ref[A_ROW : A_ROW + 16, :]
    emit_partial(y_ref, cols_ref, part_ref)


def near_halo_body(rate, cols_ref, p_ref, y_ref, v_ref, r_ref, left, right, wide_l, wide_r, inner, outer, scr):
    for i in range(2):
        init_rows(*slot(scr, i)[:2])
    own = p_ref[A_ROW : A_ROW + 8, :]
    mass = p_ref[M_ROW : M_ROW + 8, :]
    inverse = 1.0 / mass
    share = halves(wide_l[52:56, :], wide_r[48:52, :])
    odd = cols_ref[0, CORE_AT] > 0.5
    from_pair = jnp.where(odd, inner[0:24, :], inner[24:48, :])
    before = jnp.where(odd, from_pair, outer[...])
    after = jnp.where(odd, outer[...], from_pair)
    shift = jnp.where(lax.broadcasted_iota(jnp.int32, (8, 128), 0) < 4, -2.0, 2.0).astype(f32)
    tasks = []
    for b in range(MINE):
        src, tgt, qs, lhs, rows = slot(scr, b % 2)
        coords = bead_at(y_ref, b)
        far = [
            halves(left[12 * b + 4 * k : 12 * b + 4 * k + 4, :], right[12 * b + 4 * k : 12 * b + 4 * k + 4, :])
            for k in range(3)
        ]
        far[0] = far[0] + shift
        q = put_sources(src, qs, lhs, far, share, NEAR)
        rhs = put_targets(tgt, coords, NEAR)
        tasks += chunks(lhs, 0, 512, rhs, 0, 512, q, b)
        tasks += chunks(lhs, 512, 1024, rhs, 512, 1024, q, b)
        if b % 2 == 1:
            totals = stream(tasks) if b == 1 else {**totals, **stream(tasks)}
            tasks = []
    out = []
    for b in range(MINE):
        coords = bead_at(y_ref, b)
        sums = sums_of(joined(totals, b), slot(scr, b % 2)[4])
        sums = [s + r_ref[32 * b + 8 * k : 32 * b + 8 * k + 8, :] for k, s in enumerate(sums)]
        force = field(coords, sums, own, NEAR)
        for k in range(3):
            i = 8 * (3 * b + k)
            prev = before[8 * k : 8 * k + 8] if b == 0 else y_ref[i - 24 : i - 16, :]
            nxt = after[8 * k : 8 * k + 8] if b == MINE - 1 else y_ref[i + 24 : i + 32, :]
            spring = 2.0 * coords[k] - prev - nxt
            total = force[k] - SPRING * mass * spring
            out.append(v_ref[V_AT(v_ref) + i : V_AT(v_ref) + i + 8, :] + rate * total * inverse)
    return out


def V_AT(ref):
    return V_ROWS if ref.shape[0] == PACKED else 0


def near_slow_kernel(rate, cols_ref, p_ref, y_ref, v_ref, r_ref, left, right, wide_l, wide_r, inner, outer, vo_ref, *scr):
    out = near_halo_body(rate, cols_ref, p_ref, y_ref, v_ref, r_ref, left, right, wide_l, wide_r, inner, outer, scr)
    for i, v in enumerate(out):
        vo_ref[8 * i : 8 * i + 8, :] = v


def near_fast_kernel(last, cols_ref, p_ref, y_ref, v_ref, r_ref, left, right, wide_l, wide_r, inner, outer, *rest):
    if last:
        first_ref, vo_ref, yo_ref, up_ref, down_ref, in_ref, ou_ref, part_ref, moved_ref = rest[:9]
        scr = rest[9:]
    else:
        vo_ref, yo_ref, up_ref, down_ref, in_ref, ou_ref, part_ref = rest[:7]
        scr = rest[7:]
    out = near_halo_body(TIME_STEP, cols_ref, p_ref, y_ref, v_ref, r_ref, left, right, wide_l, wide_r, inner, outer, scr)
    for i, v in enumerate(out):
        vo_ref[8 * i : 8 * i + 8, :] = v
        yo_ref[8 * i : 8 * i + 8, :] = y_ref[8 * i : 8 * i + 8, :] + TIME_STEP * v
    emit(yo_ref, up_ref, down_ref, in_ref, ou_ref, cols_ref[0, CORE_AT])
    emit_partial(yo_ref, cols_ref, part_ref)
    if last:
        rows = scr[-1]
        rows[...] = yo_ref[...] - first_ref[...]
        unpack(rows, moved_ref)


def gather_kernel(recv_ref, after_ref, yc_ref):
    total = recv_ref[0:24, :]
    for r in range(1, 16):
        total = total + recv_ref[24 * r : 24 * r + 24, :]
    yc_ref[...] = total


def far_own_kernel(yc_ref, p_ref, out_ref, src, tgt, qs, lhs, rows):
    init_rows(src, tgt)
    coords = bead_at(yc_ref, 0)
    q = put_sources(src, qs, lhs, coords, p_ref[Q_ROW : Q_ROW + 8, :], FAR)
    rhs = put_targets(tgt, coords, FAR)
    total = joined(stream(chunks(lhs, 0, 1024, rhs, 0, 1024, q, 0)), 0)
    for k, r in enumerate(sums_of(total, rows)):
        out_ref[8 * k : 8 * k + 8, :] = r


def far_halo_kernel(yc_ref, p_ref, r_ref, left, right, wide_l, wide_r, out_ref, *scr):
    coords = bead_at(yc_ref, 0)
    tasks = []
    for i, (block, rows) in enumerate(((left, wide_l), (right, wide_r))):
        src, tgt, qs, lhs, _ = slot(scr, i)
        init_rows(src, tgt)
        if i == 0:
            rhs = put_targets(tgt, coords, FAR)
        there = bead_at(block, 0)
        there[0] = there[0] + (2.0 if i else -2.0)
        q = put_sources(src, qs, lhs, there, rows[56:64, :], FAR)
        if i == 0:
            tasks += chunks(lhs, 0, 512, rhs, 0, 512, q, 0)
            tasks += chunks(lhs, 512, 1024, rhs, 0, 1024, q, 0)
        else:
            tasks += chunks(lhs, 0, 512, rhs, 0, 1024, q, 0)
            tasks += chunks(lhs, 512, 1024, rhs, 512, 1024, q, 0)
    totals = stream(tasks)
    total = joined(totals, 0)
    sums = [s + r_ref[8 * k : 8 * k + 8, :] for k, s in enumerate(sums_of(total, slot(scr, 0)[4]))]
    force = field(coords, sums, p_ref[Q_ROW : Q_ROW + 8, :], FAR)
    for r in range(16):
        for k in range(3):
            out_ref[24 * r + 8 * k : 24 * r + 8 * k + 8, :] = force[k]


def kick(rate, cols_ref, p_ref, v_ref, far_ref):
    inverse = (rate * BEADS / CBEADS) / p_ref[M_ROW : M_ROW + 8, :]
    inverse = jnp.concatenate([inverse] * 3, axis=0)
    out = []
    far = [far_ref[24 * r : 24 * r + 24, :] for r in range(16)]
    for b in range(MINE):
        total = cols_ref[0, b] * far[0]
        for r in range(1, 16):
            total = total + cols_ref[0, MINE * r + b] * far[r]
        out.append(v_ref[24 * b : 24 * b + 24, :] + inverse * total)
    return out


def update_kernel(rate, cols_ref, p_ref, y_ref, v_ref, far_ref, vo_ref, yo_ref, up_ref, down_ref, in_ref, ou_ref):
    for b, v in enumerate(kick(rate, cols_ref, p_ref, v_ref, far_ref)):
        vo_ref[24 * b : 24 * b + 24, :] = v
        yo_ref[24 * b : 24 * b + 24, :] = y_ref[24 * b : 24 * b + 24, :] + TIME_STEP * v
    emit(yo_ref, up_ref, down_ref, in_ref, ou_ref, cols_ref[0, CORE_AT])


def final_kernel(rate, cols_ref, p_ref, v_ref, far_ref, out_ref, rows):
    for b, v in enumerate(kick(rate, cols_ref, p_ref, v_ref, far_ref)):
        rows[24 * b : 24 * b + 24, :] = v
    unpack(rows, out_ref)


def call(kernel, outs, cols, args, scratch=(), flops=1000, name=None, order=()):
    specs = [] if cols is None else [pl.BlockSpec(memory_space=pltpu.SMEM)]
    specs += [pl.BlockSpec(memory_space=pltpu.VMEM)] * len(args)
    specs += [pl.BlockSpec(memory_space=pl.ANY)] * len(order)
    given = ([] if cols is None else [cols]) + list(args) + list(order)
    result = pl.pallas_call(
        kernel,
        out_shape=[jax.ShapeDtypeStruct(s, f32) for s in outs],
        in_specs=specs,
        out_specs=[pl.BlockSpec(memory_space=pltpu.VMEM)] * len(outs),
        scratch_shapes=list(scratch),
        cost_estimate=pl.CostEstimate(flops=flops, bytes_accessed=400000, transcendentals=0),
        compiler_params=pltpu.CompilerParams(vmem_limit_bytes=12 * 1024 * 1024),
        name=name,
    )(*given)
    return result


HALO = (48, 128)
BEAD = (24, 128)
STATE = (96, 128)
TEAM_ROWS = (16, 24, 128)
PLAIN = (3, 4, 1024)


def exchange_team(x):
    return lax.all_to_all(x.reshape(TEAM_ROWS), TEAM, split_axis=0, concat_axis=0, tiled=True).reshape(384, 128)


def shards(positions, velocities, masses, amplitudes, charges):
    (packed,) = call(
        pack_kernel,
        [(PACKED, 128)],
        None,
        [
            jnp.transpose(positions, (1, 0, 2)),
            jnp.transpose(velocities, (1, 0, 2)),
            masses.reshape(8, 128),
            amplitudes.reshape(8, 128),
            charges.reshape(8, 128),
        ],
        name="pack",
    )
    p = lax.ppermute(packed, AXES, MOVE_IN)
    cols = lax.dynamic_slice_in_dim(jnp.asarray(SETTINGS), lax.axis_index(AXES), 1, 0)

    y, up, down, inner, outer, part = call(
        start_kernel, [STATE, (64, 128), (64, 128), BEAD, BEAD, (384, 128)], cols, [p], name="start"
    )
    first = y
    v = p
    wide_l = wide_r = None
    big = 400_000_000
    for stage in range(5):
        slow = stage % 2 == 0
        if slow:
            got = exchange_team(part)
        left = lax.ppermute(up, AXES, SLAB_UP)
        right = lax.ppermute(down, AXES, SLAB_DOWN)
        if stage == 0:
            wide_l, wide_r = left, right
        outer = lax.ppermute(outer, AXES, BEAD_SWAP)
        inner = lax.all_gather(inner, "core", axis=0, tiled=True)
        (sums,) = call(near_own_kernel, [(128, 128)], None, [y, p], SCRATCH, big, "near_own")
        near_args = [p, y, v, sums, left, right, wide_l, wide_r, inner, outer]
        if not slow:
            last = stage == 3

            def near_fast(*refs, last=last):
                near_fast_kernel(last, *refs)

            result = call(
                near_fast,
                [STATE, STATE, HALO, HALO, BEAD, BEAD, (384, 128)] + [PLAIN] * last,
                cols,
                near_args + [first] * last,
                SCRATCH + [pltpu.VMEM(STATE, f32)] * last,
                big // 2,
                "near_fast",
            )
            v, y, up, down, inner, outer, part = result[:7]
            if last:
                moved = lax.ppermute(result[7], AXES, MOVE_OUT)
            continue
        edge = stage in (0, 4)
        rate = TIME_STEP * (0.5 if edge else 1.0)

        def near_slow(*refs, rate=rate):
            near_slow_kernel(rate, *refs)

        (v,) = call(near_slow, [STATE], cols, near_args, SCRATCH, big // 2, "near_slow")
        (yc,) = call(gather_kernel, [BEAD], None, [got], name="gather", order=[sums])
        far_l = lax.ppermute(yc, AXES, SLAB_UP)
        far_r = lax.ppermute(yc, AXES, SLAB_DOWN)
        (far_sums,) = call(far_own_kernel, [(32, 128)], None, [yc, p], SCRATCH[:5], big // 4, "far_own")
        (copies,) = call(
            far_halo_kernel, [(384, 128)], None, [yc, p, far_sums, far_l, far_r, wide_l, wide_r], SCRATCH, big // 4, "far_halo"
        )
        far = exchange_team(copies)
        rate = OUTER_STEP * (0.5 if edge else 1.0)
        if stage == 4:

            def final(*refs, rate=rate):
                final_kernel(rate, *refs)

            (v,) = call(final, [PLAIN], cols, [p, v, far], [pltpu.VMEM(STATE, f32)], name="final")
        else:

            def update(*refs, rate=rate):
                update_kernel(rate, *refs)

            v, y, up, down, inner, outer = call(
                update, [STATE, STATE, HALO, HALO, BEAD, BEAD], cols, [p, y, v, far], name="update"
            )
    speeds = lax.ppermute(v, AXES, MOVE_OUT)
    return jnp.transpose(moved, (1, 0, 2)), jnp.transpose(speeds, (1, 0, 2))


def solution(mesh):
    fine = Mesh(mesh.devices.reshape((2,) * 9), AXES)
    bead = ("z2", "z1", "z0", "core")
    slab = ("zh", "x1", "x0", "y1", "y0")
    wide = P(bead, None, slab)
    flat = P(slab)
    return jax.shard_map(
        shards,
        mesh=fine,
        in_specs=(wide, wide, flat, flat, flat),
        out_specs=(wide, wide),
        check_vma=False,
    )
```

```python
import math

import jax
import jax.numpy as jnp
import numpy as np
from jax import lax
from jax.experimental import pallas as pl
from jax.experimental.pallas import tpu as pltpu
from jax.sharding import Mesh, PartitionSpec as P


TIME_STEP = 0.05
OUTER_STEP = 0.1
SPRING = 25.0
NEAR = 4.0
FAR = 2.0
BEADS = 64
CBEADS = 16
SLABS = 32
MINE = BEADS // CBEADS
STEP = 256
WIDTH = 256
AHEAD = 4

X_ROWS = 0
V_ROWS = 96
M_ROW = 192
A_ROW = 200
Q_ROW = 208
PACKED = 216

AXES = ("z2", "z1", "z0", "core", "zh", "x1", "x0", "y1", "y0")
TEAM = ("x0", "y1", "y0", "core")
f32 = jnp.float32
bf16 = jnp.bfloat16


def _place():
    ring = [(0, z) for z in range(16)] + [(1, z) for z in range(15, -1, -1)]
    cycle = [(0, 0), (0, 1), (0, 2), (0, 3), (1, 3), (1, 2), (1, 1), (1, 0)]
    device = np.zeros((CBEADS, SLABS), np.int64)
    role = np.zeros((512, 2), np.int64)
    member = np.zeros((2, 16), np.int64)
    half_of = np.zeros(SLABS, np.int64)
    for s in range(SLABS):
        half, z = ring[(s - 8) % SLABS]
        half_of[s] = half
        for b in range(CBEADS):
            q, core = divmod(b, 2)
            xx, y = cycle[q]
            x = xx if half == 0 else 3 - xx
            d = ((z % 8) * 2 + core) * 32 + (z // 8) * 16 + x * 4 + y
            device[b, s] = d
            role[d] = (b, s)
            member[half, (x % 2) * 8 + y * 2 + core] = b
    return device, role, member, half_of


DEVICE, ROLE, MEMBER, HALF = _place()


def _table():
    b = np.arange(BEADS)[None, :] / BEADS
    c = np.arange(CBEADS)[:, None] / CBEADS
    t = 2.0 * np.pi * (b - c)
    total = 1.0 + np.cos(0.5 * CBEADS * t)
    for k in range(1, CBEADS // 2):
        total = total + 2.0 * np.cos(k * t)
    return (total / BEADS).astype(np.float32)


def _settings():
    table = _table()
    out = np.zeros((CBEADS * SLABS, 128), np.float32)
    for d in range(CBEADS * SLABS):
        b, s = ROLE[d]
        out[d, : 16 * MINE] = table[MEMBER[HALF[s]]][:, b * MINE : (b + 1) * MINE].reshape(-1)
        out[d, SLAB_AT] = s
        out[d, CORE_AT] = b % 2
    return out


SLAB_AT = 16 * MINE
CORE_AT = SLAB_AT + 1
SETTINGS = _settings()


def _moves(f):
    return [
        (int(DEVICE[b, s]), int(DEVICE[f(b, s)]))
        for b in range(CBEADS)
        for s in range(SLABS)
    ]


SLAB_UP = _moves(lambda b, s: (b, (s + 1) % SLABS))
SLAB_DOWN = _moves(lambda b, s: (b, (s - 1) % SLABS))
BEAD_SWAP = _moves(lambda b, s: ((b + (1 if b % 2 else -1)) % CBEADS, s))
MOVE_IN = [(b * SLABS + s, int(DEVICE[b, s])) for b in range(CBEADS) for s in range(SLABS)]
MOVE_OUT = [(d, h) for h, d in MOVE_IN]


def pieces(v):
    high = v.astype(bf16).astype(f32)
    rest = v - high
    mid = rest.astype(bf16).astype(f32)
    return high, mid, rest - mid


def halves(lower, upper):
    return jnp.concatenate([lower, upper], axis=0)


def put(ref, row, value):
    ref[pl.ds(row, 8, stride=8), :] = value


def wide(ref):
    return jnp.concatenate([ref[8 * k : 8 * k + 8, :] for k in range(8)], axis=1)


def init_rows(src, tgt):
    ones = jnp.ones((8, 128), f32)
    zeros = jnp.zeros((8, 128), f32)
    put(src, 4, ones)
    put(tgt, 3, ones)
    for k in range(5, 8):
        put(src, k, zeros)
        put(tgt, k, zeros)


def scaled(coords, scale):
    alpha = math.sqrt(scale * math.log2(math.e))
    a = [alpha * y for y in coords]
    return a, -0.5 * (a[0] * a[0] + a[1] * a[1] + a[2] * a[2])


def put_sources(src, qs, lhs, coords, share, scale):
    a, norm = scaled(coords, scale)
    for k, v in enumerate(a + [norm]):
        put(src, k, v)
    for k, v in enumerate([share] + [share * y for y in coords]):
        put(qs, k, v)
        put(qs, 4 + k, v)
    high, mid, low = pieces(wide(src))
    rows = jnp.concatenate([high, high, mid, mid, high, low], axis=0)
    for block in range(8):
        part = slice(128 * block, 128 * block + 128)
        lhs[part, :] = rows[:, part].T.astype(bf16)
    high, mid, low = pieces(wide(qs))
    upper = lax.broadcasted_iota(jnp.int32, (8, 1024), 0) < 4
    return jnp.concatenate([jnp.where(upper, high, mid), jnp.where(upper, low, 0.0)], axis=0).astype(bf16)


def put_targets(tgt, coords, scale):
    a, norm = scaled(coords, scale)
    for k, v in enumerate(a):
        put(tgt, k, v)
    put(tgt, 4, norm)
    high, mid, low = pieces(wide(tgt))
    return jnp.concatenate([high, mid, high, mid, low, high], axis=0).astype(bf16)


def stream(tasks, ahead=AHEAD):
    totals = {}
    ready = []
    for t in range(len(tasks) + ahead):
        if t < len(tasks):
            lhs, first, rhs, q, key = tasks[t]
            ready.append(jnp.dot(lhs[first : first + STEP, :], rhs, preferred_element_type=f32))
        if t < ahead:
            continue
        lhs, first, rhs, q, key = tasks[t - ahead]
        weight = jnp.exp2(ready[t - ahead])
        high = weight.astype(bf16)
        low = (weight - high.astype(f32)).astype(bf16)
        mine = q[:, first : first + STEP]
        part = jnp.dot(mine, high, preferred_element_type=f32)
        part = part + jnp.dot(mine, low, preferred_element_type=f32)
        totals[key] = totals[key] + part if key in totals else part
    return totals


def chunks(lhs, first, last, rhs, start, stop, q, key):
    return [
        (lhs, j, rhs[:, i : i + WIDTH], q, (key, i))
        for j in range(first, last, STEP)
        for i in range(start, stop, WIDTH)
    ]


def joined(totals, key):
    return jnp.concatenate([totals[key, i] for i in range(0, 1024, WIDTH)], axis=1)


def sums_of(total, rows):
    r = total[0:8]
    r = r + jnp.concatenate([r[4:8], r[0:4]], axis=0) + total[8:16]
    for block in range(8):
        rows[8 * block : 8 * block + 8, :] = r[:, 128 * block : 128 * block + 128]
    return [rows[pl.ds(k, 8, stride=8), :] for k in range(4)]


def field(coords, sums, share, scale):
    return [share * scale * (coords[k] * sums[0] - sums[1 + k]) for k in range(3)]


def slot(scr, i):
    return scr[5 * i : 5 * i + 5]


SCRATCH = 2 * [
    pltpu.VMEM((64, 128), f32),
    pltpu.VMEM((64, 128), f32),
    pltpu.VMEM((64, 128), f32),
    pltpu.VMEM((1024, 48), bf16),
    pltpu.VMEM((64, 128), f32),
]


def bead_at(ref, b):
    return [ref[pl.ds(24 * b + 8 * k, 8), :] for k in range(3)]


def near_own_kernel(start, y_ref, p_ref, out_ref, *scr):
    share = p_ref[A_ROW : A_ROW + 8, :]
    tasks = []
    for j in range(2):
        src, tgt, qs, lhs, _ = slot(scr, j)
        init_rows(src, tgt)
        coords = bead_at(y_ref, start + j)
        q = put_sources(src, qs, lhs, coords, share, NEAR)
        rhs = put_targets(tgt, coords, NEAR)
        tasks += chunks(lhs, 0, 1024, rhs, 0, 1024, q, j)
    totals = stream(tasks)
    for j in range(2):
        for k, r in enumerate(sums_of(joined(totals, j), slot(scr, j)[4])):
            out_ref[32 * j + 8 * k : 32 * j + 8 * k + 8, :] = r


def emit(y_refs, up_ref, down_ref, inner_ref, outer_ref, core):
    for i in range(12):
        y = y_refs[8 * i : 8 * i + 8, :]
        down_ref[4 * i : 4 * i + 4, :] = y[0:4]
        up_ref[4 * i : 4 * i + 4, :] = y[4:8]
    first = y_refs[0:24, :]
    last = y_refs[72:96, :]
    odd = core > 0.5
    inner_ref[...] = jnp.where(odd, first, last)
    outer_ref[...] = jnp.where(odd, last, first)


def emit_partial(y_refs, cols_ref, part_ref):
    y = [y_refs[24 * b : 24 * b + 24, :] for b in range(MINE)]
    for r in range(16):
        total = cols_ref[0, MINE * r] * y[0]
        for b in range(1, MINE):
            total = total + cols_ref[0, MINE * r + b] * y[b]
        part_ref[24 * r : 24 * r + 24, :] = total


def pack_kernel(x_ref, v_ref, m_ref, a_ref, q_ref, out_ref):
    for base, ref in ((X_ROWS, x_ref), (V_ROWS, v_ref)):
        for k in range(3):
            for block in range(8):
                row = base + 8 * k + block
                out_ref[pl.ds(row, 4, stride=24), :] = ref[k, :, 128 * block : 128 * block + 128]
    out_ref[M_ROW : M_ROW + 8, :] = m_ref[...]
    out_ref[A_ROW : A_ROW + 8, :] = a_ref[...]
    out_ref[Q_ROW : Q_ROW + 8, :] = q_ref[...]


def unpack(value_ref, out_ref):
    for k in range(3):
        for block in range(8):
            out_ref[k, :, 128 * block : 128 * block + 128] = value_ref[pl.ds(8 * k + block, 4, stride=24), :]


def start_kernel(cols_ref, p_ref, y_ref, up_ref, down_ref, inner_ref, outer_ref, part_ref):
    centre = 2.0 * cols_ref[0, SLAB_AT] + 1.0
    for b in range(MINE):
        for k in range(3):
            i = 8 * (3 * b + k)
            y_ref[i : i + 8, :] = p_ref[i : i + 8, :] - (centre if k == 0 else 1.0)
    emit(y_ref, up_ref, down_ref, inner_ref, outer_ref, cols_ref[0, CORE_AT])
    up_ref[48:64, :] = p_ref[A_ROW : A_ROW + 16, :]
    down_ref[48:64, :] = p_ref[A_ROW : A_ROW + 16, :]
    emit_partial(y_ref, cols_ref, part_ref)


def near_halo_body(rate, cols_ref, p_ref, y_ref, v_ref, ra_ref, rb_ref, left, right, wide_l, wide_r, inner, outer, scr):
    for i in range(2):
        init_rows(*slot(scr, i)[:2])
    own = p_ref[A_ROW : A_ROW + 8, :]
    mass = p_ref[M_ROW : M_ROW + 8, :]
    inverse = 1.0 / mass
    share = halves(wide_l[52:56, :], wide_r[48:52, :])
    odd = cols_ref[0, CORE_AT] > 0.5
    from_pair = jnp.where(odd, inner[0:24, :], inner[24:48, :])
    before = jnp.where(odd, from_pair, outer[...])
    after = jnp.where(odd, outer[...], from_pair)
    shift = jnp.where(lax.broadcasted_iota(jnp.int32, (8, 128), 0) < 4, -2.0, 2.0).astype(f32)
    tasks = []
    for b in range(MINE):
        src, tgt, qs, lhs, _ = slot(scr, b % 2)
        coords = bead_at(y_ref, b)
        far = [
            halves(left[12 * b + 4 * k : 12 * b + 4 * k + 4, :], right[12 * b + 4 * k : 12 * b + 4 * k + 4, :])
            for k in range(3)
        ]
        far[0] = far[0] + shift
        q = put_sources(src, qs, lhs, far, share, NEAR)
        rhs = put_targets(tgt, coords, NEAR)
        tasks += chunks(lhs, 0, 512, rhs, 0, 512, q, b)
        tasks += chunks(lhs, 512, 1024, rhs, 512, 1024, q, b)
        if b % 2 == 1:
            totals = stream(tasks) if b == 1 else {**totals, **stream(tasks)}
            tasks = []
    out = []
    for b in range(MINE):
        coords = bead_at(y_ref, b)
        sums = sums_of(joined(totals, b), slot(scr, b % 2)[4])
        mine = rb_ref if b >= 2 else ra_ref
        at = 32 * (b % 2)
        sums = [s + mine[at + 8 * k : at + 8 * k + 8, :] for k, s in enumerate(sums)]
        force = field(coords, sums, own, NEAR)
        for k in range(3):
            i = 8 * (3 * b + k)
            prev = before[8 * k : 8 * k + 8] if b == 0 else y_ref[i - 24 : i - 16, :]
            nxt = after[8 * k : 8 * k + 8] if b == MINE - 1 else y_ref[i + 24 : i + 32, :]
            spring = 2.0 * coords[k] - prev - nxt
            total = force[k] - SPRING * mass * spring
            out.append(v_ref[V_AT(v_ref) + i : V_AT(v_ref) + i + 8, :] + rate * total * inverse)
    return out


def V_AT(ref):
    return V_ROWS if ref.shape[0] == PACKED else 0


def near_slow_kernel(rate, cols_ref, p_ref, y_ref, v_ref, ra_ref, rb_ref, left, right, wide_l, wide_r, inner, outer, vo_ref, *scr):
    out = near_halo_body(rate, cols_ref, p_ref, y_ref, v_ref, ra_ref, rb_ref, left, right, wide_l, wide_r, inner, outer, scr)
    for i, v in enumerate(out):
        vo_ref[8 * i : 8 * i + 8, :] = v


def near_fast_kernel(last, cols_ref, p_ref, y_ref, v_ref, ra_ref, rb_ref, left, right, wide_l, wide_r, inner, outer, *rest):
    if last:
        first_ref, vo_ref, yo_ref, up_ref, down_ref, in_ref, ou_ref, part_ref, moved_ref = rest[:9]
        scr = rest[9:]
    else:
        vo_ref, yo_ref, up_ref, down_ref, in_ref, ou_ref, part_ref = rest[:7]
        scr = rest[7:]
    out = near_halo_body(TIME_STEP, cols_ref, p_ref, y_ref, v_ref, ra_ref, rb_ref, left, right, wide_l, wide_r, inner, outer, scr)
    for i, v in enumerate(out):
        vo_ref[8 * i : 8 * i + 8, :] = v
        yo_ref[8 * i : 8 * i + 8, :] = y_ref[8 * i : 8 * i + 8, :] + TIME_STEP * v
    emit(yo_ref, up_ref, down_ref, in_ref, ou_ref, cols_ref[0, CORE_AT])
    emit_partial(yo_ref, cols_ref, part_ref)
    if last:
        rows = scr[-1]
        rows[...] = yo_ref[...] - first_ref[...]
        unpack(rows, moved_ref)


def gather_kernel(recv_ref, yc_ref, same_ref):
    total = recv_ref[0:24, :]
    for r in range(1, 16):
        total = total + recv_ref[24 * r : 24 * r + 24, :]
    yc_ref[...] = total
    same_ref[...] = total


def far_own_kernel(yc_ref, p_ref, out_ref, src, tgt, qs, lhs, rows):
    init_rows(src, tgt)
    coords = bead_at(yc_ref, 0)
    q = put_sources(src, qs, lhs, coords, p_ref[Q_ROW : Q_ROW + 8, :], FAR)
    rhs = put_targets(tgt, coords, FAR)
    total = joined(stream(chunks(lhs, 0, 1024, rhs, 0, 1024, q, 0)), 0)
    for k, r in enumerate(sums_of(total, rows)):
        out_ref[8 * k : 8 * k + 8, :] = r


def far_halo_kernel(yc_ref, p_ref, r_ref, left, right, wide_l, wide_r, out_ref, *scr):
    coords = bead_at(yc_ref, 0)
    tasks = []
    for i, (block, rows) in enumerate(((left, wide_l), (right, wide_r))):
        src, tgt, qs, lhs, _ = slot(scr, i)
        init_rows(src, tgt)
        if i == 0:
            rhs = put_targets(tgt, coords, FAR)
        there = bead_at(block, 0)
        there[0] = there[0] + (2.0 if i else -2.0)
        q = put_sources(src, qs, lhs, there, rows[56:64, :], FAR)
        if i == 0:
            tasks += chunks(lhs, 0, 512, rhs, 0, 512, q, 0)
            tasks += chunks(lhs, 512, 1024, rhs, 0, 1024, q, 0)
        else:
            tasks += chunks(lhs, 0, 512, rhs, 0, 1024, q, 0)
            tasks += chunks(lhs, 512, 1024, rhs, 512, 1024, q, 0)
    totals = stream(tasks)
    total = joined(totals, 0)
    sums = [s + r_ref[8 * k : 8 * k + 8, :] for k, s in enumerate(sums_of(total, slot(scr, 0)[4]))]
    force = field(coords, sums, p_ref[Q_ROW : Q_ROW + 8, :], FAR)
    for r in range(16):
        for k in range(3):
            out_ref[24 * r + 8 * k : 24 * r + 8 * k + 8, :] = force[k]


def kick(rate, cols_ref, p_ref, v_ref, far_ref):
    inverse = (rate * BEADS / CBEADS) / p_ref[M_ROW : M_ROW + 8, :]
    inverse = jnp.concatenate([inverse] * 3, axis=0)
    out = []
    far = [far_ref[24 * r : 24 * r + 24, :] for r in range(16)]
    for b in range(MINE):
        total = cols_ref[0, b] * far[0]
        for r in range(1, 16):
            total = total + cols_ref[0, MINE * r + b] * far[r]
        out.append(v_ref[24 * b : 24 * b + 24, :] + inverse * total)
    return out


def update_kernel(rate, cols_ref, p_ref, y_ref, v_ref, far_ref, vo_ref, yo_ref, up_ref, down_ref, in_ref, ou_ref):
    for b, v in enumerate(kick(rate, cols_ref, p_ref, v_ref, far_ref)):
        vo_ref[24 * b : 24 * b + 24, :] = v
        yo_ref[24 * b : 24 * b + 24, :] = y_ref[24 * b : 24 * b + 24, :] + TIME_STEP * v
    emit(yo_ref, up_ref, down_ref, in_ref, ou_ref, cols_ref[0, CORE_AT])


def final_kernel(rate, cols_ref, p_ref, v_ref, far_ref, out_ref, rows):
    for b, v in enumerate(kick(rate, cols_ref, p_ref, v_ref, far_ref)):
        rows[24 * b : 24 * b + 24, :] = v
    unpack(rows, out_ref)


def call(kernel, outs, cols, args, scratch=(), flops=1000, order=(), passed=()):
    specs = [] if cols is None else [pl.BlockSpec(memory_space=pltpu.SMEM)]
    specs += [pl.BlockSpec(memory_space=pltpu.VMEM)] * len(args)
    used = len(specs)
    specs += [pl.BlockSpec(memory_space=pl.ANY)] * (len(order) + len(passed))
    given = ([] if cols is None else [cols]) + list(args) + list(order) + list(passed)
    base = used + len(order)

    def body(*refs):
        kernel(*refs[:used], *refs[len(given) : len(given) + len(outs)], *refs[len(given) + len(outs) + len(passed) :])

    shapes = [jax.ShapeDtypeStruct(s, f32) for s in outs] + [jax.ShapeDtypeStruct(x.shape, f32) for x in passed]
    return pl.pallas_call(
        body,
        out_shape=shapes,
        in_specs=specs,
        out_specs=[pl.BlockSpec(memory_space=pltpu.VMEM)] * len(outs) + [pl.BlockSpec(memory_space=pl.ANY)] * len(passed),
        scratch_shapes=list(scratch),
        input_output_aliases={base + i: len(outs) + i for i in range(len(passed))},
        cost_estimate=pl.CostEstimate(flops=flops, bytes_accessed=400000, transcendentals=0),
        compiler_params=pltpu.CompilerParams(vmem_limit_bytes=12 * 1024 * 1024),
    )(*given)


HALO = (48, 128)
BEAD = (24, 128)
STATE = (96, 128)
TEAM_ROWS = (16, 24, 128)
PLAIN = (3, 4, 1024)


def exchange_team(x):
    x = lax.all_to_all(x.reshape(TEAM_ROWS), TEAM, split_axis=0, concat_axis=0, tiled=True)
    return x.reshape(384, 128)


def send(x, moves):
    return lax.ppermute(x, AXES, moves)


def own(start):
    def kernel(*refs):
        near_own_kernel(start, *refs)

    return kernel


def shards(positions, velocities, masses, amplitudes, charges):
    (packed,) = call(
        pack_kernel,
        [(PACKED, 128)],
        None,
        [
            jnp.transpose(positions, (1, 0, 2)),
            jnp.transpose(velocities, (1, 0, 2)),
            masses.reshape(8, 128),
            amplitudes.reshape(8, 128),
            charges.reshape(8, 128),
        ],
    )
    p = lax.ppermute(packed, AXES, MOVE_IN)
    cols = lax.dynamic_slice_in_dim(jnp.asarray(SETTINGS), lax.axis_index(AXES), 1, 0)

    y, up, down, inner, outer, part = call(
        start_kernel, [STATE, (64, 128), (64, 128), BEAD, BEAD, (384, 128)], cols, [p]
    )
    first = y
    v = p
    wide_l = wide_r = None
    big = 400_000_000
    for stage in range(5):
      slow = stage % 2 == 0
      if slow:
          got = exchange_team(part)
      left = send(up, SLAB_UP)
      sums_a, down = call(own(0), [(64, 128)], None, [y, p], SCRATCH, big, passed=[down])
      right = send(down, SLAB_DOWN)
      if slow:
          (sums_b,) = call(own(2), [(64, 128)], None, [y, p], SCRATCH, big, order=[sums_a])
      else:
          sums_b, outer, inner = call(
              own(2), [(64, 128)], None, [y, p], SCRATCH, big, order=[sums_a], passed=[outer, inner]
          )
      if stage == 0:
          wide_l, wide_r = left, right
      if not slow:
          outer = send(outer, BEAD_SWAP)
          inner = lax.all_gather(inner, "core", axis=0, tiled=True)
          near_args = [p, y, v, sums_a, sums_b, left, right, wide_l, wide_r, inner, outer]
          last = stage == 3

          def near_fast(*refs, last=last):
              near_fast_kernel(last, *refs)

          result = call(
              near_fast,
              [STATE, STATE, HALO, HALO, BEAD, BEAD, (384, 128)] + [PLAIN] * last,
              cols,
              near_args + [first] * last,
              SCRATCH + [pltpu.VMEM(STATE, f32)] * last,
              big // 2,
          )
          v, y, up, down, inner, outer, part = result[:7]
          if last:
              moved = result[7]
          continue
      edge = stage in (0, 4)
      rate = TIME_STEP * (0.5 if edge else 1.0)

      def near_slow(*refs, rate=rate):
          near_slow_kernel(rate, *refs)

      yc, shown = call(gather_kernel, [BEAD, BEAD], None, [got], order=[sums_b])
      far_l = send(yc, SLAB_UP)
      far_sums, shown, inner = call(
          far_own_kernel, [(32, 128)], None, [yc, p], SCRATCH[:5], big // 4, passed=[shown, inner]
      )
      far_r = send(shown, SLAB_DOWN)
      inner = lax.all_gather(inner, "core", axis=0, tiled=True)
      copies, outer = call(
          far_halo_kernel,
          [(384, 128)],
          None,
          [shown, p, far_sums, far_l, far_r, wide_l, wide_r],
          SCRATCH,
          big // 4,
          order=[inner],
          passed=[outer],
      )
      far = exchange_team(copies)
      outer = send(outer, BEAD_SWAP)
      near_args = [p, y, v, sums_a, sums_b, left, right, wide_l, wide_r, inner, outer]
      (v,) = call(near_slow, [STATE], cols, near_args, SCRATCH, big // 2)
      rate = OUTER_STEP * (0.5 if edge else 1.0)
      if stage == 4:

          def final(*refs, rate=rate):
              final_kernel(rate, *refs)

          (v,) = call(final, [PLAIN], cols, [p, v, far], [pltpu.VMEM(STATE, f32)])
      else:

          def update(*refs, rate=rate):
              update_kernel(rate, *refs)

          v, y, up, down, inner, outer = call(update, [STATE, STATE, HALO, HALO, BEAD, BEAD], cols, [p, y, v, far])
    moved = lax.ppermute(moved, AXES, MOVE_OUT)
    speeds = lax.ppermute(v, AXES, MOVE_OUT)
    return jnp.transpose(moved, (1, 0, 2)), jnp.transpose(speeds, (1, 0, 2))


def solution(mesh):
    fine = Mesh(mesh.devices.reshape((2,) * 9), AXES)
    bead = ("z2", "z1", "z0", "core")
    slab = ("zh", "x1", "x0", "y1", "y0")
    wide = P(bead, None, slab)
    flat = P(slab)
    return jax.shard_map(
        shards,
        mesh=fine,
        in_specs=(wide, wide, flat, flat, flat),
        out_specs=(wide, wide),
        check_vma=False,
    )
```

```python
import math

import jax
import jax.numpy as jnp
import numpy as np
from jax import lax
from jax.experimental import pallas as pl
from jax.experimental.pallas import tpu as pltpu
from jax.sharding import Mesh, PartitionSpec as P


TIME_STEP = 0.05
OUTER_STEP = 0.1
SPRING = 25.0
NEAR = 4.0
FAR = 2.0
BEADS = 64
CBEADS = 16
SLABS = 32
MINE = BEADS // CBEADS
STEP = 256
WIDTH = 256
AHEAD = 4

X_ROWS = 0
V_ROWS = 96
M_ROW = 192
A_ROW = 200
Q_ROW = 208
PACKED = 216
WIDE = 72

AXES = ("z2", "z1", "z0", "core", "zh", "x1", "x0", "y1", "y0")
TEAM = ("x0", "y1", "y0", "core")
f32 = jnp.float32
bf16 = jnp.bfloat16


def _place():
    ring = [(0, z) for z in range(16)] + [(1, z) for z in range(15, -1, -1)]
    cycle = [(0, 0), (0, 1), (0, 2), (0, 3), (1, 3), (1, 2), (1, 1), (1, 0)]
    device = np.zeros((CBEADS, SLABS), np.int64)
    role = np.zeros((512, 2), np.int64)
    member = np.zeros((2, 16), np.int64)
    half_of = np.zeros(SLABS, np.int64)
    for s in range(SLABS):
        half, z = ring[(s - 8) % SLABS]
        half_of[s] = half
        for b in range(CBEADS):
            q, core = divmod(b, 2)
            xx, y = cycle[q]
            x = xx if half == 0 else 3 - xx
            d = ((z % 8) * 2 + core) * 32 + (z // 8) * 16 + x * 4 + y
            device[b, s] = d
            role[d] = (b, s)
            member[half, (x % 2) * 8 + y * 2 + core] = b
    return device, role, member, half_of


DEVICE, ROLE, MEMBER, HALF = _place()


def _table():
    b = np.arange(BEADS)[None, :] / BEADS
    c = np.arange(CBEADS)[:, None] / CBEADS
    t = 2.0 * np.pi * (b - c)
    total = 1.0 + np.cos(0.5 * CBEADS * t)
    for k in range(1, CBEADS // 2):
        total = total + 2.0 * np.cos(k * t)
    return (total / BEADS).astype(np.float32)


def _settings():
    table = _table()
    out = np.zeros((CBEADS * SLABS, 128), np.float32)
    for d in range(CBEADS * SLABS):
        b, s = ROLE[d]
        out[d, : 16 * MINE] = table[MEMBER[HALF[s]]][:, b * MINE : (b + 1) * MINE].reshape(-1)
        out[d, SLAB_AT] = s
        out[d, CORE_AT] = b % 2
    return out


SLAB_AT = 16 * MINE
CORE_AT = SLAB_AT + 1
SETTINGS = _settings()


def _moves(f):
    return [
        (int(DEVICE[b, s]), int(DEVICE[f(b, s)]))
        for b in range(CBEADS)
        for s in range(SLABS)
    ]


SLAB_UP = _moves(lambda b, s: (b, (s + 1) % SLABS))
SLAB_DOWN = _moves(lambda b, s: (b, (s - 1) % SLABS))
BEAD_SWAP = _moves(lambda b, s: ((b + (1 if b % 2 else -1)) % CBEADS, s))
MOVE_IN = [(b * SLABS + s, int(DEVICE[b, s])) for b in range(CBEADS) for s in range(SLABS)]
MOVE_OUT = [(d, h) for h, d in MOVE_IN]


def pieces(v):
    high = v.astype(bf16).astype(f32)
    rest = v - high
    mid = rest.astype(bf16).astype(f32)
    return high, mid, rest - mid


def halves(lower, upper):
    return jnp.concatenate([lower, upper], axis=0)


def put(ref, row, value):
    ref[pl.ds(row, 8, stride=8), :] = value


def wide(ref):
    return jnp.concatenate([ref[8 * k : 8 * k + 8, :] for k in range(8)], axis=1)


def init_rows(src, tgt):
    ones = jnp.ones((8, 128), f32)
    zeros = jnp.zeros((8, 128), f32)
    put(src, 4, ones)
    put(tgt, 3, ones)
    for k in range(5, 8):
        put(src, k, zeros)
        put(tgt, k, zeros)


def scaled(coords, scale):
    alpha = math.sqrt(scale * math.log2(math.e))
    a = [alpha * y for y in coords]
    return a, -0.5 * (a[0] * a[0] + a[1] * a[1] + a[2] * a[2])


def put_sources(src, qs, lhs, coords, share, scale):
    a, norm = scaled(coords, scale)
    for k, v in enumerate(a + [norm]):
        put(src, k, v)
    for k, v in enumerate([share] + [share * y for y in coords]):
        put(qs, k, v)
        put(qs, 4 + k, v)
    high, mid, low = pieces(wide(src))
    rows = jnp.concatenate([high, high, mid, mid, high, low], axis=0)
    for block in range(8):
        part = slice(128 * block, 128 * block + 128)
        lhs[part, :] = rows[:, part].T.astype(bf16)
    high, mid, low = pieces(wide(qs))
    upper = lax.broadcasted_iota(jnp.int32, (8, 1024), 0) < 4
    return jnp.concatenate([jnp.where(upper, high, mid), jnp.where(upper, low, 0.0)], axis=0).astype(bf16)


def put_targets(tgt, coords, scale):
    a, norm = scaled(coords, scale)
    for k, v in enumerate(a):
        put(tgt, k, v)
    put(tgt, 4, norm)
    high, mid, low = pieces(wide(tgt))
    return jnp.concatenate([high, mid, high, mid, low, high], axis=0).astype(bf16)


def stream(tasks, ahead=AHEAD):
    totals = {}
    ready = []
    for t in range(len(tasks) + ahead):
        if t < len(tasks):
            lhs, first, rhs, q, key = tasks[t]
            ready.append(jnp.dot(lhs[first : first + STEP, :], rhs, preferred_element_type=f32))
        if t < ahead:
            continue
        lhs, first, rhs, q, key = tasks[t - ahead]
        weight = jnp.exp2(ready[t - ahead])
        high = weight.astype(bf16)
        low = (weight - high.astype(f32)).astype(bf16)
        mine = q[:, first : first + STEP]
        part = jnp.dot(mine, high, preferred_element_type=f32)
        part = part + jnp.dot(mine, low, preferred_element_type=f32)
        totals[key] = totals[key] + part if key in totals else part
    return totals


def chunks(lhs, first, last, rhs, start, stop, q, key):
    return [
        (lhs, j, rhs[:, i : i + WIDTH], q, (key, i))
        for j in range(first, last, STEP)
        for i in range(start, stop, WIDTH)
    ]


def joined(totals, key):
    return jnp.concatenate([totals[key, i] for i in range(0, 1024, WIDTH)], axis=1)


def sums_of(total, rows):
    r = total[0:8]
    r = r + jnp.concatenate([r[4:8], r[0:4]], axis=0) + total[8:16]
    for block in range(8):
        rows[8 * block : 8 * block + 8, :] = r[:, 128 * block : 128 * block + 128]
    return [rows[pl.ds(k, 8, stride=8), :] for k in range(4)]


def field(coords, sums, share, scale):
    return [share * scale * (coords[k] * sums[0] - sums[1 + k]) for k in range(3)]


def slot(scr, i):
    return scr[5 * i : 5 * i + 5]


SCRATCH = 2 * [
    pltpu.VMEM((64, 128), f32),
    pltpu.VMEM((64, 128), f32),
    pltpu.VMEM((64, 128), f32),
    pltpu.VMEM((1024, 48), bf16),
    pltpu.VMEM((64, 128), f32),
]


def bead_at(ref, b):
    return [ref[pl.ds(24 * b + 8 * k, 8), :] for k in range(3)]


def near_own_kernel(y_ref, p_ref, out_ref, *scr):
    share = p_ref[A_ROW : A_ROW + 8, :]
    for i in range(2):
        init_rows(*slot(scr, i)[:2])

    def two(i, carry):
        tasks = []
        for j in range(2):
            src, tgt, qs, lhs, _ = slot(scr, j)
            coords = bead_at(y_ref, 2 * i + j)
            q = put_sources(src, qs, lhs, coords, share, NEAR)
            rhs = put_targets(tgt, coords, NEAR)
            tasks += chunks(lhs, 0, 1024, rhs, 0, 1024, q, j)
        totals = stream(tasks)
        for j in range(2):
            for k, r in enumerate(sums_of(joined(totals, j), slot(scr, j)[4])):
                out_ref[pl.ds(64 * i + 32 * j + 8 * k, 8), :] = r
        return carry

    lax.fori_loop(0, MINE // 2, two, 0)


def emit(y_refs, up_ref, down_ref, inner_ref, outer_ref, core):
    for i in range(12):
        y = y_refs[8 * i : 8 * i + 8, :]
        down_ref[4 * i : 4 * i + 4, :] = y[0:4]
        up_ref[4 * i : 4 * i + 4, :] = y[4:8]
    first = y_refs[0:24, :]
    last = y_refs[72:96, :]
    odd = core > 0.5
    inner_ref[...] = jnp.where(odd, first, last)
    outer_ref[...] = jnp.where(odd, last, first)


def emit_partial(y_refs, cols_ref, part_ref):
    y = [y_refs[24 * b : 24 * b + 24, :] for b in range(MINE)]
    for r in range(16):
        total = cols_ref[0, MINE * r] * y[0]
        for b in range(1, MINE):
            total = total + cols_ref[0, MINE * r + b] * y[b]
        part_ref[24 * r : 24 * r + 24, :] = total


def pack_kernel(x_ref, v_ref, m_ref, a_ref, q_ref, out_ref):
    for base, ref in ((X_ROWS, x_ref), (V_ROWS, v_ref)):
        for k in range(3):
            for block in range(8):
                row = base + 8 * k + block
                out_ref[pl.ds(row, 4, stride=24), :] = ref[k, :, 128 * block : 128 * block + 128]
    out_ref[M_ROW : M_ROW + 8, :] = m_ref[...]
    out_ref[A_ROW : A_ROW + 8, :] = a_ref[...]
    out_ref[Q_ROW : Q_ROW + 8, :] = q_ref[...]


def unpack(value_ref, out_ref):
    for k in range(3):
        for block in range(8):
            out_ref[k, :, 128 * block : 128 * block + 128] = value_ref[pl.ds(8 * k + block, 4, stride=24), :]


def start_kernel(cols_ref, p_ref, y_ref, up_ref, down_ref, inner_ref, outer_ref, part_ref):
    centre = 2.0 * cols_ref[0, SLAB_AT] + 1.0
    for b in range(MINE):
        for k in range(3):
            i = 8 * (3 * b + k)
            y_ref[i : i + 8, :] = p_ref[i : i + 8, :] - (centre if k == 0 else 1.0)
    emit(y_ref, up_ref, down_ref, inner_ref, outer_ref, cols_ref[0, CORE_AT])
    emit_partial(y_ref, cols_ref, part_ref)


def near_halo_body(rate, cols_ref, p_ref, y_ref, v_ref, r_ref, left, right, wide_l, wide_r, inner, outer, store, scr):
    chain = scr[10]
    for i in range(2):
        init_rows(*slot(scr, i)[:2])
    own = p_ref[A_ROW : A_ROW + 8, :]
    mass = p_ref[M_ROW : M_ROW + 8, :]
    inverse = 1.0 / mass
    share = halves(wide_l[WIDE + 4 : WIDE + 8, :], wide_r[WIDE : WIDE + 4, :])
    odd = cols_ref[0, CORE_AT] > 0.5
    from_pair = jnp.where(odd, inner[0:24, :], inner[24:48, :])
    chain[0:24, :] = jnp.where(odd, from_pair, outer[...])
    chain[24:120, :] = y_ref[...]
    chain[120:144, :] = jnp.where(odd, outer[...], from_pair)
    shift = jnp.where(lax.broadcasted_iota(jnp.int32, (8, 128), 0) < 4, -2.0, 2.0).astype(f32)

    def two(i, carry):
        at = pl.multiple_of(48 * i, 8)
        lows = left[pl.ds(pl.multiple_of(24 * i, 8), 24), :]
        highs = right[pl.ds(pl.multiple_of(24 * i, 8), 24), :]
        tasks = []
        places = []
        for j in range(2):
            src, tgt, qs, lhs, _ = slot(scr, j)
            coords = [y_ref[pl.ds(at + 24 * j + 8 * k, 8), :] for k in range(3)]
            far = []
            for k in range(3):
                h = 12 * j + 4 * k
                far.append(halves(lows[h : h + 4], highs[h : h + 4]))
            far[0] = far[0] + shift
            q = put_sources(src, qs, lhs, far, share, NEAR)
            rhs = put_targets(tgt, coords, NEAR)
            tasks += chunks(lhs, 0, 512, rhs, 0, 512, q, j)
            tasks += chunks(lhs, 512, 1024, rhs, 512, 1024, q, j)
            places.append(coords)
        totals = stream(tasks)
        for j in range(2):
            coords = places[j]
            sums = sums_of(joined(totals, j), slot(scr, j)[4])
            mine = pl.multiple_of(64 * i, 8) + 32 * j
            sums = [s + r_ref[pl.ds(mine + 8 * k, 8), :] for k, s in enumerate(sums)]
            force = field(coords, sums, own, NEAR)
            for k in range(3):
                r = at + 24 * j + 8 * k
                spring = 2.0 * coords[k] - chain[pl.ds(r, 8), :] - chain[pl.ds(r + 48, 8), :]
                total = force[k] - SPRING * mass * spring
                store(r, coords[k], v_ref[pl.ds(V_AT(v_ref) + r, 8), :] + rate * total * inverse)
        return carry

    lax.fori_loop(0, MINE // 2, two, 0)


def V_AT(ref):
    return V_ROWS if ref.shape[0] == PACKED else 0


def near_slow_kernel(rate, cols_ref, p_ref, y_ref, v_ref, r_ref, left, right, wide_l, wide_r, inner, outer, vo_ref, *scr):
    def store(r, y, v):
        vo_ref[pl.ds(r, 8), :] = v

    near_halo_body(rate, cols_ref, p_ref, y_ref, v_ref, r_ref, left, right, wide_l, wide_r, inner, outer, store, scr)


def near_fast_kernel(last, cols_ref, p_ref, y_ref, v_ref, r_ref, left, right, wide_l, wide_r, inner, outer, *rest):
    if last:
        first_ref, vo_ref, yo_ref, up_ref, down_ref, in_ref, ou_ref, part_ref, moved_ref = rest[:9]
        scr = rest[9:]
    else:
        vo_ref, yo_ref, up_ref, down_ref, in_ref, ou_ref, part_ref = rest[:7]
        scr = rest[7:]

    def store(r, y, v):
        vo_ref[pl.ds(r, 8), :] = v
        yo_ref[pl.ds(r, 8), :] = y + TIME_STEP * v

    near_halo_body(TIME_STEP, cols_ref, p_ref, y_ref, v_ref, r_ref, left, right, wide_l, wide_r, inner, outer, store, scr)
    emit(yo_ref, up_ref, down_ref, in_ref, ou_ref, cols_ref[0, CORE_AT])
    emit_partial(yo_ref, cols_ref, part_ref)
    if last:
        rows = scr[-1]
        rows[...] = yo_ref[...] - first_ref[...]
        unpack(rows, moved_ref)


def gather_kernel(wide, recv_ref, up_ref, down_ref, p_ref, yc_ref, up_out, down_out):
    total = recv_ref[0:24, :]
    for r in range(1, 16):
        total = total + recv_ref[24 * r : 24 * r + 24, :]
    yc_ref[...] = total
    for out, ref in ((up_out, up_ref), (down_out, down_ref)):
        out[0:48, :] = ref[...]
        out[48:72, :] = total
        if wide:
            out[WIDE : WIDE + 16, :] = p_ref[A_ROW : A_ROW + 16, :]


def far_own_kernel(yc_ref, p_ref, out_ref, src, tgt, qs, lhs, rows):
    init_rows(src, tgt)
    coords = bead_at(yc_ref, 0)
    q = put_sources(src, qs, lhs, coords, p_ref[Q_ROW : Q_ROW + 8, :], FAR)
    rhs = put_targets(tgt, coords, FAR)
    total = joined(stream(chunks(lhs, 0, 1024, rhs, 0, 1024, q, 0)), 0)
    for k, r in enumerate(sums_of(total, rows)):
        out_ref[8 * k : 8 * k + 8, :] = r


def far_halo_kernel(yc_ref, p_ref, r_ref, left, right, wide_l, wide_r, out_ref, *scr):
    coords = bead_at(yc_ref, 0)
    tasks = []
    for i, (block, rows) in enumerate(((left, wide_l), (right, wide_r))):
        src, tgt, qs, lhs, _ = slot(scr, i)
        init_rows(src, tgt)
        if i == 0:
            rhs = put_targets(tgt, coords, FAR)
        there = [block[48 + 8 * k : 56 + 8 * k, :] for k in range(3)]
        there[0] = there[0] + (2.0 if i else -2.0)
        q = put_sources(src, qs, lhs, there, rows[WIDE + 8 : WIDE + 16, :], FAR)
        if i == 0:
            tasks += chunks(lhs, 0, 512, rhs, 0, 512, q, 0)
            tasks += chunks(lhs, 512, 1024, rhs, 0, 1024, q, 0)
        else:
            tasks += chunks(lhs, 0, 512, rhs, 0, 1024, q, 0)
            tasks += chunks(lhs, 512, 1024, rhs, 512, 1024, q, 0)
    totals = stream(tasks)
    total = joined(totals, 0)
    sums = [s + r_ref[8 * k : 8 * k + 8, :] for k, s in enumerate(sums_of(total, slot(scr, 0)[4]))]
    force = field(coords, sums, p_ref[Q_ROW : Q_ROW + 8, :], FAR)
    for r in range(16):
        for k in range(3):
            out_ref[24 * r + 8 * k : 24 * r + 8 * k + 8, :] = force[k]


def kick(rate, cols_ref, p_ref, v_ref, far_ref):
    inverse = (rate * BEADS / CBEADS) / p_ref[M_ROW : M_ROW + 8, :]
    inverse = jnp.concatenate([inverse] * 3, axis=0)
    out = []
    far = [far_ref[24 * r : 24 * r + 24, :] for r in range(16)]
    for b in range(MINE):
        total = cols_ref[0, b] * far[0]
        for r in range(1, 16):
            total = total + cols_ref[0, MINE * r + b] * far[r]
        out.append(v_ref[24 * b : 24 * b + 24, :] + inverse * total)
    return out


def update_kernel(rate, cols_ref, p_ref, y_ref, v_ref, far_ref, vo_ref, yo_ref, up_ref, down_ref, in_ref, ou_ref):
    for b, v in enumerate(kick(rate, cols_ref, p_ref, v_ref, far_ref)):
        vo_ref[24 * b : 24 * b + 24, :] = v
        yo_ref[24 * b : 24 * b + 24, :] = y_ref[24 * b : 24 * b + 24, :] + TIME_STEP * v
    emit(yo_ref, up_ref, down_ref, in_ref, ou_ref, cols_ref[0, CORE_AT])


def final_kernel(rate, cols_ref, p_ref, v_ref, far_ref, out_ref, rows):
    for b, v in enumerate(kick(rate, cols_ref, p_ref, v_ref, far_ref)):
        rows[24 * b : 24 * b + 24, :] = v
    unpack(rows, out_ref)


def call(kernel, outs, cols, args, scratch=(), flops=1000, order=(), passed=()):
    specs = [] if cols is None else [pl.BlockSpec(memory_space=pltpu.SMEM)]
    specs += [pl.BlockSpec(memory_space=pltpu.VMEM)] * len(args)
    used = len(specs)
    specs += [pl.BlockSpec(memory_space=pl.ANY)] * (len(order) + len(passed))
    given = ([] if cols is None else [cols]) + list(args) + list(order) + list(passed)
    base = used + len(order)

    def body(*refs):
        kernel(*refs[:used], *refs[len(given) : len(given) + len(outs)], *refs[len(given) + len(outs) + len(passed) :])

    shapes = [jax.ShapeDtypeStruct(s, f32) for s in outs] + [jax.ShapeDtypeStruct(x.shape, f32) for x in passed]
    return pl.pallas_call(
        body,
        out_shape=shapes,
        in_specs=specs,
        out_specs=[pl.BlockSpec(memory_space=pltpu.VMEM)] * len(outs) + [pl.BlockSpec(memory_space=pl.ANY)] * len(passed),
        scratch_shapes=list(scratch),
        input_output_aliases={base + i: len(outs) + i for i in range(len(passed))},
        cost_estimate=pl.CostEstimate(flops=flops, bytes_accessed=400000, transcendentals=0),
        compiler_params=pltpu.CompilerParams(vmem_limit_bytes=12 * 1024 * 1024),
    )(*given)


HALO = (48, 128)
BEAD = (24, 128)
STATE = (96, 128)
TEAM_ROWS = (16, 24, 128)
PLAIN = (3, 4, 1024)


def exchange_team(x):
    x = lax.all_to_all(x.reshape(TEAM_ROWS), TEAM, split_axis=0, concat_axis=0, tiled=True)
    return x.reshape(384, 128)


def send(x, moves):
    return lax.ppermute(x, AXES, moves)


def pair(x):
    return lax.all_gather(x, "core", axis=0, tiled=True)


CHAIN = pltpu.VMEM((144, 128), f32)


def shards(positions, velocities, masses, amplitudes, charges):
    (packed,) = call(
        pack_kernel,
        [(PACKED, 128)],
        None,
        [
            jnp.transpose(positions, (1, 0, 2)),
            jnp.transpose(velocities, (1, 0, 2)),
            masses.reshape(8, 128),
            amplitudes.reshape(8, 128),
            charges.reshape(8, 128),
        ],
    )
    p = lax.ppermute(packed, AXES, MOVE_IN)
    cols = lax.dynamic_slice_in_dim(jnp.asarray(SETTINGS), lax.axis_index(AXES), 1, 0)

    y, up, down, inner, outer, part = call(start_kernel, [STATE, HALO, HALO, BEAD, BEAD, (384, 128)], cols, [p])
    first = y
    v = p
    wide_l = wide_r = None
    big = 400_000_000
    for stage in range(5):
        slow = stage % 2 == 0
        if not slow:
            left = send(up, SLAB_UP)
            right = send(down, SLAB_DOWN)
            outer = send(outer, BEAD_SWAP)
            inner = pair(inner)
            (sums,) = call(near_own_kernel, [(128, 128)], None, [y, p], SCRATCH, big)
            last = stage == 3

            def near_fast(*refs, last=last):
                near_fast_kernel(last, *refs)

            result = call(
                near_fast,
                [STATE, STATE, HALO, HALO, BEAD, BEAD, (384, 128)] + [PLAIN] * last,
                cols,
                [p, y, v, sums, left, right, wide_l, wide_r, inner, outer] + [first] * last,
                SCRATCH + [CHAIN] + [pltpu.VMEM(STATE, f32)] * last,
                big // 2,
            )
            v, y, up, down, inner, outer, part = result[:7]
            if last:
                moved = result[7]
            continue
        edge = stage in (0, 4)
        got = exchange_team(part)
        inner = pair(inner)
        (sums,) = call(near_own_kernel, [(128, 128)], None, [y, p], SCRATCH, big)

        def gather(*refs, wide=stage == 0):
            gather_kernel(wide, *refs)

        size = (WIDE + 16 * (stage == 0), 128)
        yc, up, down, outer = call(gather, [BEAD, size, size], None, [got, up, down, p], order=[sums], passed=[outer])
        left = send(up, SLAB_UP)
        right = send(down, SLAB_DOWN)
        outer = send(outer, BEAD_SWAP)
        if stage == 0:
            wide_l, wide_r = left, right
        (far_sums,) = call(far_own_kernel, [(32, 128)], None, [yc, p], SCRATCH[:5], big // 4)
        (copies,) = call(
            far_halo_kernel, [(384, 128)], None, [yc, p, far_sums, left, right, wide_l, wide_r], SCRATCH, big // 4
        )
        far = exchange_team(copies)
        rate = TIME_STEP * (0.5 if edge else 1.0)

        def near_slow(*refs, rate=rate):
            near_slow_kernel(rate, *refs)

        (v,) = call(
            near_slow,
            [STATE],
            cols,
            [p, y, v, sums, left, right, wide_l, wide_r, inner, outer],
            SCRATCH + [CHAIN],
            big // 2,
        )
        rate = OUTER_STEP * (0.5 if edge else 1.0)
        if stage == 4:

            def final(*refs, rate=rate):
                final_kernel(rate, *refs)

            (v,) = call(final, [PLAIN], cols, [p, v, far], [pltpu.VMEM(STATE, f32)])
        else:

            def update(*refs, rate=rate):
                update_kernel(rate, *refs)

            v, y, up, down, inner, outer = call(update, [STATE, STATE, HALO, HALO, BEAD, BEAD], cols, [p, y, v, far])
    moved = lax.ppermute(moved, AXES, MOVE_OUT)
    speeds = lax.ppermute(v, AXES, MOVE_OUT)
    return jnp.transpose(moved, (1, 0, 2)), jnp.transpose(speeds, (1, 0, 2))


def solution(mesh):
    fine = Mesh(mesh.devices.reshape((2,) * 9), AXES)
    bead = ("z2", "z1", "z0", "core")
    slab = ("zh", "x1", "x0", "y1", "y0")
    wide = P(bead, None, slab)
    flat = P(slab)
    return jax.shard_map(
        shards,
        mesh=fine,
        in_specs=(wide, wide, flat, flat, flat),
        out_specs=(wide, wide),
        check_vma=False,
    )
```

```python
import math

import jax
import jax.numpy as jnp
import numpy as np
from jax import lax
from jax.experimental import pallas as pl
from jax.experimental.pallas import tpu as pltpu
from jax.sharding import Mesh, PartitionSpec as P


TIME_STEP = 0.05
OUTER_STEP = 0.1
SPRING = 25.0
NEAR = 4.0
FAR = 2.0
BEADS = 64
CBEADS = 16
SLABS = 32
MINE = BEADS // CBEADS
STEP = 256
WIDTH = 256
AHEAD = 4

M_ROW = 96
A_ROW = 104
Q_ROW = 112
PACKED = 120
WIDE = 72

AXES = ("z2", "z1", "z0", "core", "zh", "x1", "x0", "y1", "y0")
TEAM = ("x0", "y1", "y0", "core")
f32 = jnp.float32
bf16 = jnp.bfloat16


def _place():
    ring = [(0, z) for z in range(16)] + [(1, z) for z in range(15, -1, -1)]
    cycle = [(0, 0), (0, 1), (0, 2), (0, 3), (1, 3), (1, 2), (1, 1), (1, 0)]
    device = np.zeros((CBEADS, SLABS), np.int64)
    role = np.zeros((512, 2), np.int64)
    member = np.zeros((2, 16), np.int64)
    half_of = np.zeros(SLABS, np.int64)
    for s in range(SLABS):
        half, z = ring[(s - 8) % SLABS]
        half_of[s] = half
        for b in range(CBEADS):
            q, core = divmod(b, 2)
            xx, y = cycle[q]
            x = xx if half == 0 else 3 - xx
            d = ((z % 8) * 2 + core) * 32 + (z // 8) * 16 + x * 4 + y
            device[b, s] = d
            role[d] = (b, s)
            member[half, (x % 2) * 8 + y * 2 + core] = b
    return device, role, member, half_of


DEVICE, ROLE, MEMBER, HALF = _place()


def _table():
    b = np.arange(BEADS)[None, :] / BEADS
    c = np.arange(CBEADS)[:, None] / CBEADS
    t = 2.0 * np.pi * (b - c)
    total = 1.0 + np.cos(0.5 * CBEADS * t)
    for k in range(1, CBEADS // 2):
        total = total + 2.0 * np.cos(k * t)
    return (total / BEADS).astype(np.float32)


def _settings():
    table = _table()
    out = np.zeros((CBEADS * SLABS, 128), np.float32)
    for d in range(CBEADS * SLABS):
        b, s = ROLE[d]
        out[d, : 16 * MINE] = table[MEMBER[HALF[s]]][:, b * MINE : (b + 1) * MINE].reshape(-1)
        out[d, SLAB_AT] = s
        out[d, CORE_AT] = b % 2
        edges = table[MEMBER[HALF[s]]][:, [(b * MINE - 1) % BEADS, (b * MINE + MINE) % BEADS]]
        out[d, EDGE_AT : EDGE_AT + 32] = edges.reshape(-1)
    return out


SLAB_AT = 16 * MINE
CORE_AT = SLAB_AT + 1
EDGE_AT = SLAB_AT + 2
SETTINGS = _settings()


def _moves(f):
    return [
        (int(DEVICE[b, s]), int(DEVICE[f(b, s)]))
        for b in range(CBEADS)
        for s in range(SLABS)
    ]


SLAB_UP = _moves(lambda b, s: (b, (s + 1) % SLABS))
SLAB_DOWN = _moves(lambda b, s: (b, (s - 1) % SLABS))
BEAD_SWAP = _moves(lambda b, s: ((b + (1 if b % 2 else -1)) % CBEADS, s))
MOVE_IN = [(b * SLABS + s, int(DEVICE[b, s])) for b in range(CBEADS) for s in range(SLABS)]
MOVE_OUT = [(d, h) for h, d in MOVE_IN]


def pieces(v):
    high = v.astype(bf16).astype(f32)
    rest = v - high
    mid = rest.astype(bf16).astype(f32)
    return high, mid, rest - mid


def halves(lower, upper):
    return jnp.concatenate([lower, upper], axis=0)


def put(ref, row, value):
    ref[pl.ds(row, 8, stride=8), :] = value


def wide(ref):
    return jnp.concatenate([ref[8 * k : 8 * k + 8, :] for k in range(8)], axis=1)


def init_rows(src, tgt):
    ones = jnp.ones((8, 128), f32)
    zeros = jnp.zeros((8, 128), f32)
    put(src, 4, ones)
    put(tgt, 3, ones)
    for k in range(5, 8):
        put(src, k, zeros)
        put(tgt, k, zeros)


def scaled(coords, scale):
    alpha = math.sqrt(scale * math.log2(math.e))
    a = [alpha * y for y in coords]
    return a, -0.5 * (a[0] * a[0] + a[1] * a[1] + a[2] * a[2])


def put_sources(src, qs, lhs, coords, share, scale):
    a, norm = scaled(coords, scale)
    for k, v in enumerate(a + [norm]):
        put(src, k, v)
    for k, v in enumerate([share] + [share * y for y in coords]):
        put(qs, k, v)
        put(qs, 4 + k, v)
    high, mid, low = pieces(wide(src))
    rows = jnp.concatenate([high, high, mid, mid, high, low], axis=0)
    for block in range(8):
        part = slice(128 * block, 128 * block + 128)
        lhs[part, :] = rows[:, part].T.astype(bf16)
    high, mid, low = pieces(wide(qs))
    upper = lax.broadcasted_iota(jnp.int32, (8, 1024), 0) < 4
    return jnp.concatenate([jnp.where(upper, high, mid), jnp.where(upper, low, 0.0)], axis=0).astype(bf16)


def put_targets(tgt, coords, scale):
    a, norm = scaled(coords, scale)
    for k, v in enumerate(a):
        put(tgt, k, v)
    put(tgt, 4, norm)
    high, mid, low = pieces(wide(tgt))
    return jnp.concatenate([high, mid, high, mid, low, high], axis=0).astype(bf16)


def stream(tasks, ahead=AHEAD):
    totals = {}
    ready = []
    for t in range(len(tasks) + ahead):
        if t < len(tasks):
            lhs, first, rhs, q, key = tasks[t]
            ready.append(jnp.dot(lhs[first : first + STEP, :], rhs, preferred_element_type=f32))
        if t < ahead:
            continue
        lhs, first, rhs, q, key = tasks[t - ahead]
        weight = jnp.exp2(ready[t - ahead])
        high = weight.astype(bf16)
        low = (weight - high.astype(f32)).astype(bf16)
        mine = q[:, first : first + STEP]
        part = jnp.dot(mine, high, preferred_element_type=f32)
        part = part + jnp.dot(mine, low, preferred_element_type=f32)
        totals[key] = totals[key] + part if key in totals else part
    return totals


def chunks(lhs, first, last, rhs, start, stop, q, key):
    return [
        (lhs, j, rhs[:, i : i + WIDTH], q, (key, i))
        for j in range(first, last, STEP)
        for i in range(start, stop, WIDTH)
    ]


def joined(totals, key):
    return jnp.concatenate([totals[key, i] for i in range(0, 1024, WIDTH)], axis=1)


def sums_of(total, rows):
    r = total[0:8]
    r = r + jnp.concatenate([r[4:8], r[0:4]], axis=0) + total[8:16]
    for block in range(8):
        rows[8 * block : 8 * block + 8, :] = r[:, 128 * block : 128 * block + 128]
    return [rows[pl.ds(k, 8, stride=8), :] for k in range(4)]


def field(coords, sums, share, scale):
    return [share * scale * (coords[k] * sums[0] - sums[1 + k]) for k in range(3)]


def slot(scr, i):
    return scr[5 * i : 5 * i + 5]


SCRATCH = 2 * [
    pltpu.VMEM((64, 128), f32),
    pltpu.VMEM((64, 128), f32),
    pltpu.VMEM((64, 128), f32),
    pltpu.VMEM((1024, 48), bf16),
    pltpu.VMEM((64, 128), f32),
]


def bead_at(ref, b):
    return [ref[pl.ds(24 * b + 8 * k, 8), :] for k in range(3)]


def near_own_kernel(y_ref, p_ref, out_ref, *scr):
    share = p_ref[A_ROW : A_ROW + 8, :]
    for i in range(2):
        init_rows(*slot(scr, i)[:2])

    def two(i, carry):
        tasks = []
        for j in range(2):
            src, tgt, qs, lhs, _ = slot(scr, j)
            coords = bead_at(y_ref, 2 * i + j)
            q = put_sources(src, qs, lhs, coords, share, NEAR)
            rhs = put_targets(tgt, coords, NEAR)
            tasks += chunks(lhs, 0, 1024, rhs, 0, 1024, q, j)
        totals = stream(tasks)
        for j in range(2):
            for k, r in enumerate(sums_of(joined(totals, j), slot(scr, j)[4])):
                out_ref[pl.ds(64 * i + 32 * j + 8 * k, 8), :] = r
        return carry

    lax.fori_loop(0, MINE // 2, two, 0)


def emit(y_refs, up_ref, down_ref):
    for i in range(12):
        y = y_refs[8 * i : 8 * i + 8, :]
        down_ref[4 * i : 4 * i + 4, :] = y[0:4]
        up_ref[4 * i : 4 * i + 4, :] = y[4:8]


def emit_edges(first, last, inner_ref, outer_ref, core):
    odd = core > 0.5
    inner_ref[...] = jnp.where(odd, first, last)
    outer_ref[...] = jnp.where(odd, last, first)


def edges_of(inner, outer, core):
    odd = core > 0.5
    from_pair = jnp.where(odd, inner[0:24, :], inner[24:48, :])
    return jnp.where(odd, from_pair, outer[...]), jnp.where(odd, outer[...], from_pair)


def emit_partial(y_refs, cols_ref, part_ref):
    y = [y_refs[24 * b : 24 * b + 24, :] for b in range(MINE)]
    for r in range(16):
        total = cols_ref[0, MINE * r] * y[0]
        for b in range(1, MINE):
            total = total + cols_ref[0, MINE * r + b] * y[b]
        part_ref[24 * r : 24 * r + 24, :] = total


def spread(ref, out_ref, centre):
    for k in range(3):
        for block in range(8):
            value = ref[k, :, 128 * block : 128 * block + 128]
            out_ref[pl.ds(8 * k + block, 4, stride=24), :] = value if centre is None else value - centre[k]


def pack_kernel(v_ref, m_ref, a_ref, q_ref, out_ref):
    spread(v_ref, out_ref, None)
    out_ref[M_ROW : M_ROW + 8, :] = m_ref[...]
    out_ref[A_ROW : A_ROW + 8, :] = a_ref[...]
    out_ref[Q_ROW : Q_ROW + 8, :] = q_ref[...]


def unpack(value_ref, out_ref):
    for k in range(3):
        for block in range(8):
            out_ref[k, :, 128 * block : 128 * block + 128] = value_ref[pl.ds(8 * k + block, 4, stride=24), :]


def start_kernel(cols_ref, x_ref, y_ref, up_ref, down_ref, inner_ref, outer_ref, part_ref):
    spread(x_ref, y_ref, (2.0 * cols_ref[0, SLAB_AT] + 1.0, 1.0, 1.0))
    emit(y_ref, up_ref, down_ref)
    emit_edges(y_ref[0:24, :], y_ref[72:96, :], inner_ref, outer_ref, cols_ref[0, CORE_AT])
    emit_partial(y_ref, cols_ref, part_ref)


def near_halo_body(rate, p_ref, y_ref, v_ref, r_ref, left, right, wide_l, wide_r, edges, store, scr):
    chain = scr[10]
    for i in range(2):
        init_rows(*slot(scr, i)[:2])
    own = p_ref[A_ROW : A_ROW + 8, :]
    mass = p_ref[M_ROW : M_ROW + 8, :]
    inverse = 1.0 / mass
    share = halves(wide_l[WIDE + 4 : WIDE + 8, :], wide_r[WIDE : WIDE + 4, :])
    chain[0:24, :], chain[120:144, :] = edges
    chain[24:120, :] = y_ref[...]
    shift = jnp.where(lax.broadcasted_iota(jnp.int32, (8, 128), 0) < 4, -2.0, 2.0).astype(f32)

    def two(i, carry):
        at = pl.multiple_of(48 * i, 8)
        lows = left[pl.ds(pl.multiple_of(24 * i, 8), 24), :]
        highs = right[pl.ds(pl.multiple_of(24 * i, 8), 24), :]
        tasks = []
        places = []
        for j in range(2):
            src, tgt, qs, lhs, _ = slot(scr, j)
            coords = [y_ref[pl.ds(at + 24 * j + 8 * k, 8), :] for k in range(3)]
            far = []
            for k in range(3):
                h = 12 * j + 4 * k
                far.append(halves(lows[h : h + 4], highs[h : h + 4]))
            far[0] = far[0] + shift
            q = put_sources(src, qs, lhs, far, share, NEAR)
            rhs = put_targets(tgt, coords, NEAR)
            tasks += chunks(lhs, 0, 512, rhs, 0, 512, q, j)
            tasks += chunks(lhs, 512, 1024, rhs, 512, 1024, q, j)
            places.append(coords)
        totals = stream(tasks)
        for j in range(2):
            coords = places[j]
            sums = sums_of(joined(totals, j), slot(scr, j)[4])
            mine = pl.multiple_of(64 * i, 8) + 32 * j
            sums = [s + r_ref[pl.ds(mine + 8 * k, 8), :] for k, s in enumerate(sums)]
            force = field(coords, sums, own, NEAR)
            for k in range(3):
                r = at + 24 * j + 8 * k
                spring = 2.0 * coords[k] - chain[pl.ds(r, 8), :] - chain[pl.ds(r + 48, 8), :]
                total = force[k] - SPRING * mass * spring
                store(r, coords[k], v_ref[pl.ds(r, 8), :] + rate * total * inverse)
        return carry

    lax.fori_loop(0, MINE // 2, two, 0)


def near_slow_kernel(rate, cols_ref, p_ref, y_ref, v_ref, r_ref, left, right, wide_l, wide_r, inner, outer, vo_ref, *rest):
    def store(r, y, v):
        vo_ref[pl.ds(r, 8), :] = v

    core = cols_ref[0, CORE_AT]
    edges = edges_of(inner, outer, core)
    scr = rest[-len(SCRATCH) - 1 :]
    near_halo_body(rate, p_ref, y_ref, v_ref, r_ref, left, right, wide_l, wide_r, edges, store, scr)
    if len(rest) > len(scr):
        first = y_ref[0:24, :] + TIME_STEP * vo_ref[0:24, :]
        last = y_ref[72:96, :] + TIME_STEP * vo_ref[72:96, :]
        emit_edges(first, last, rest[0], rest[1], core)


def near_fast_kernel(last, cols_ref, p_ref, y_ref, v_ref, r_ref, left, right, wide_l, wide_r, before, after, *rest):
    if last:
        first_ref, vo_ref, yo_ref, up_ref, down_ref, in_ref, ou_ref, part_ref, moved_ref = rest[:9]
        scr = rest[9:]
    else:
        vo_ref, yo_ref, up_ref, down_ref, in_ref, ou_ref, part_ref = rest[:7]
        scr = rest[7:]

    def store(r, y, v):
        vo_ref[pl.ds(r, 8), :] = v
        yo_ref[pl.ds(r, 8), :] = y + TIME_STEP * v

    edges = (before[...], after[...])
    near_halo_body(TIME_STEP, p_ref, y_ref, v_ref, r_ref, left, right, wide_l, wide_r, edges, store, scr)
    emit(yo_ref, up_ref, down_ref)
    emit_edges(yo_ref[0:24, :], yo_ref[72:96, :], in_ref, ou_ref, cols_ref[0, CORE_AT])
    emit_partial(yo_ref, cols_ref, part_ref)
    if last:
        rows = scr[-1]
        rows[...] = yo_ref[...] - first_ref[...]
        unpack(rows, moved_ref)


def gather_kernel(wide, recv_ref, up_ref, down_ref, p_ref, yc_ref, up_out, down_out):
    total = recv_ref[0:24, :]
    for r in range(1, 16):
        total = total + recv_ref[24 * r : 24 * r + 24, :]
    yc_ref[...] = total
    for out, ref in ((up_out, up_ref), (down_out, down_ref)):
        out[0:48, :] = ref[...]
        out[48:72, :] = total
        if wide:
            out[WIDE : WIDE + 16, :] = p_ref[A_ROW : A_ROW + 16, :]


def far_own_kernel(yc_ref, p_ref, out_ref, src, tgt, qs, lhs, rows):
    init_rows(src, tgt)
    coords = bead_at(yc_ref, 0)
    q = put_sources(src, qs, lhs, coords, p_ref[Q_ROW : Q_ROW + 8, :], FAR)
    rhs = put_targets(tgt, coords, FAR)
    total = joined(stream(chunks(lhs, 0, 1024, rhs, 0, 1024, q, 0)), 0)
    for k, r in enumerate(sums_of(total, rows)):
        out_ref[8 * k : 8 * k + 8, :] = r


def far_halo_kernel(yc_ref, p_ref, r_ref, left, right, wide_l, wide_r, out_ref, *scr):
    coords = bead_at(yc_ref, 0)
    tasks = []
    for i, (block, rows) in enumerate(((left, wide_l), (right, wide_r))):
        src, tgt, qs, lhs, _ = slot(scr, i)
        init_rows(src, tgt)
        if i == 0:
            rhs = put_targets(tgt, coords, FAR)
        there = [block[48 + 8 * k : 56 + 8 * k, :] for k in range(3)]
        there[0] = there[0] + (2.0 if i else -2.0)
        q = put_sources(src, qs, lhs, there, rows[WIDE + 8 : WIDE + 16, :], FAR)
        if i == 0:
            tasks += chunks(lhs, 0, 512, rhs, 0, 512, q, 0)
            tasks += chunks(lhs, 512, 1024, rhs, 0, 1024, q, 0)
        else:
            tasks += chunks(lhs, 0, 512, rhs, 0, 1024, q, 0)
            tasks += chunks(lhs, 512, 1024, rhs, 512, 1024, q, 0)
    totals = stream(tasks)
    total = joined(totals, 0)
    sums = [s + r_ref[8 * k : 8 * k + 8, :] for k, s in enumerate(sums_of(total, slot(scr, 0)[4]))]
    force = field(coords, sums, p_ref[Q_ROW : Q_ROW + 8, :], FAR)
    for r in range(16):
        for k in range(3):
            out_ref[24 * r + 8 * k : 24 * r + 8 * k + 8, :] = force[k]


def kick(rate, cols_ref, p_ref, v_ref, far_ref):
    inverse = (rate * BEADS / CBEADS) / p_ref[M_ROW : M_ROW + 8, :]
    inverse = jnp.concatenate([inverse] * 3, axis=0)
    out = []
    far = [far_ref[24 * r : 24 * r + 24, :] for r in range(16)]
    for b in range(MINE):
        total = cols_ref[0, b] * far[0]
        for r in range(1, 16):
            total = total + cols_ref[0, MINE * r + b] * far[r]
        out.append(v_ref[24 * b : 24 * b + 24, :] + inverse * total)
    return out


def update_kernel(rate, cols_ref, p_ref, y_ref, v_ref, far_ref, inner, outer,
                  vo_ref, yo_ref, up_ref, down_ref, before_ref, after_ref):
    for b, v in enumerate(kick(rate, cols_ref, p_ref, v_ref, far_ref)):
        vo_ref[24 * b : 24 * b + 24, :] = v
        yo_ref[24 * b : 24 * b + 24, :] = y_ref[24 * b : 24 * b + 24, :] + TIME_STEP * v
    emit(yo_ref, up_ref, down_ref)
    inverse = (TIME_STEP * rate * BEADS / CBEADS) / p_ref[M_ROW : M_ROW + 8, :]
    inverse = jnp.concatenate([inverse] * 3, axis=0)
    edges = edges_of(inner, outer, cols_ref[0, CORE_AT])
    for e, out in enumerate((before_ref, after_ref)):
        total = cols_ref[0, EDGE_AT + e] * far_ref[0:24, :]
        for r in range(1, 16):
            total = total + cols_ref[0, EDGE_AT + 2 * r + e] * far_ref[24 * r : 24 * r + 24, :]
        out[...] = edges[e] + inverse * total


def final_kernel(rate, cols_ref, p_ref, v_ref, far_ref, out_ref, rows):
    for b, v in enumerate(kick(rate, cols_ref, p_ref, v_ref, far_ref)):
        rows[24 * b : 24 * b + 24, :] = v
    unpack(rows, out_ref)


def call(kernel, outs, cols, args, scratch=(), flops=1000, order=(), passed=()):
    specs = [] if cols is None else [pl.BlockSpec(memory_space=pltpu.SMEM)]
    specs += [pl.BlockSpec(memory_space=pltpu.VMEM)] * len(args)
    used = len(specs)
    specs += [pl.BlockSpec(memory_space=pl.ANY)] * (len(order) + len(passed))
    given = ([] if cols is None else [cols]) + list(args) + list(order) + list(passed)
    base = used + len(order)

    def body(*refs):
        kernel(*refs[:used], *refs[len(given) : len(given) + len(outs)], *refs[len(given) + len(outs) + len(passed) :])

    shapes = [jax.ShapeDtypeStruct(s, f32) for s in outs] + [jax.ShapeDtypeStruct(x.shape, f32) for x in passed]
    return pl.pallas_call(
        body,
        out_shape=shapes,
        in_specs=specs,
        out_specs=[pl.BlockSpec(memory_space=pltpu.VMEM)] * len(outs) + [pl.BlockSpec(memory_space=pl.ANY)] * len(passed),
        scratch_shapes=list(scratch),
        input_output_aliases={base + i: len(outs) + i for i in range(len(passed))},
        cost_estimate=pl.CostEstimate(flops=flops, bytes_accessed=400000, transcendentals=0),
        compiler_params=pltpu.CompilerParams(vmem_limit_bytes=12 * 1024 * 1024),
    )(*given)


HALO = (48, 128)
BEAD = (24, 128)
STATE = (96, 128)
TEAM_ROWS = (16, 24, 128)
PLAIN = (3, 4, 1024)


def exchange_team(x):
    x = lax.all_to_all(x.reshape(TEAM_ROWS), TEAM, split_axis=0, concat_axis=0, tiled=True)
    return x.reshape(384, 128)


def send(x, moves):
    return lax.ppermute(x, AXES, moves)


def pair(x):
    return lax.all_gather(x, "core", axis=0, tiled=True)


CHAIN = pltpu.VMEM((144, 128), f32)


def shards(positions, velocities, masses, amplitudes, charges):
    x = send(jnp.transpose(positions, (1, 0, 2)), MOVE_IN)
    (packed,) = call(
        pack_kernel,
        [(PACKED, 128)],
        None,
        [
            jnp.transpose(velocities, (1, 0, 2)),
            masses.reshape(8, 128),
            amplitudes.reshape(8, 128),
            charges.reshape(8, 128),
        ],
    )
    p = send(packed, MOVE_IN)
    cols = lax.dynamic_slice_in_dim(jnp.asarray(SETTINGS), lax.axis_index(AXES), 1, 0)
    y, up, down, inner, outer, part = call(start_kernel, [STATE, HALO, HALO, BEAD, BEAD, (384, 128)], cols, [x])
    first = y
    v = p
    wide_l = wide_r = None
    big = 400_000_000
    for stage in range(5):
        slow = stage % 2 == 0
        if not slow:
            left = send(up, SLAB_UP)
            right = send(down, SLAB_DOWN)
            (sums,) = call(near_own_kernel, [(128, 128)], None, [y, p], SCRATCH, big)
            last = stage == 3

            def near_fast(*refs, last=last):
                near_fast_kernel(last, *refs)

            result = call(
                near_fast,
                [STATE, STATE, HALO, HALO, BEAD, BEAD, (384, 128)] + [PLAIN] * last,
                cols,
                [p, y, v, sums, left, right, wide_l, wide_r, before, after] + [first] * last,
                SCRATCH + [CHAIN] + [pltpu.VMEM(STATE, f32)] * last,
                big // 2,
            )
            v, y, up, down, inner, outer, part = result[:7]
            if last:
                moved = result[7]
            continue
        edge = stage in (0, 4)
        got = exchange_team(part)
        inner = pair(inner)
        (sums,) = call(near_own_kernel, [(128, 128)], None, [y, p], SCRATCH, big)

        def gather(*refs, wide=stage == 0):
            gather_kernel(wide, *refs)

        size = (WIDE + 16 * (stage == 0), 128)
        yc, up, down, outer = call(gather, [BEAD, size, size], None, [got, up, down, p], order=[sums], passed=[outer])
        left = send(up, SLAB_UP)
        right = send(down, SLAB_DOWN)
        outer = send(outer, BEAD_SWAP)
        if stage == 0:
            wide_l, wide_r = left, right
        (far_sums,) = call(far_own_kernel, [(32, 128)], None, [yc, p], SCRATCH[:5], big // 4)
        (copies,) = call(
            far_halo_kernel, [(384, 128)], None, [yc, p, far_sums, left, right, wide_l, wide_r], SCRATCH, big // 4
        )
        far = exchange_team(copies)
        rate = TIME_STEP * (0.5 if edge else 1.0)

        def near_slow(*refs, rate=rate):
            near_slow_kernel(rate, *refs)

        v, *ends = call(
            near_slow,
            [STATE] + [BEAD] * (2 * (stage < 4)),
            cols,
            [p, y, v, sums, left, right, wide_l, wide_r, inner, outer],
            SCRATCH + [CHAIN],
            big // 2,
        )
        rate = OUTER_STEP * (0.5 if edge else 1.0)
        if stage == 4:

            def final(*refs, rate=rate):
                final_kernel(rate, *refs)

            (v,) = call(final, [PLAIN], cols, [p, v, far], [pltpu.VMEM(STATE, f32)])
        else:

            def update(*refs, rate=rate):
                update_kernel(rate, *refs)

            inner = pair(ends[0])
            outer = send(ends[1], BEAD_SWAP)
            v, y, up, down, before, after = call(
                update, [STATE, STATE, HALO, HALO, BEAD, BEAD], cols, [p, y, v, far, inner, outer]
            )
    moved = lax.ppermute(moved, AXES, MOVE_OUT)
    speeds = lax.ppermute(v, AXES, MOVE_OUT)
    return jnp.transpose(moved, (1, 0, 2)), jnp.transpose(speeds, (1, 0, 2))


def solution(mesh):
    fine = Mesh(mesh.devices.reshape((2,) * 9), AXES)
    bead = ("z2", "z1", "z0", "core")
    slab = ("zh", "x1", "x0", "y1", "y0")
    wide = P(bead, None, slab)
    flat = P(slab)
    return jax.shard_map(
        shards,
        mesh=fine,
        in_specs=(wide, wide, flat, flat, flat),
        out_specs=(wide, wide),
        check_vma=False,
    )
```

```python
import math

import jax
import jax.numpy as jnp
import numpy as np
from jax import lax
from jax.experimental import pallas as pl
from jax.experimental.pallas import tpu as pltpu
from jax.sharding import Mesh, PartitionSpec as P


TIME_STEP = 0.05
OUTER_STEP = 0.1
SPRING = 25.0
NEAR = 4.0
FAR = 2.0
BEADS = 64
CBEADS = 16
SLABS = 32
MINE = BEADS // CBEADS
STEP = 256
WIDTH = 256
AHEAD = 4

M_ROW = 96
A_ROW = 104
Q_ROW = 112
PACKED = 120
WIDE = 72

AXES = ("z2", "z1", "z0", "core", "zh", "x1", "x0", "y1", "y0")
TEAM = ("x0", "y1", "y0", "core")
f32 = jnp.float32
bf16 = jnp.bfloat16


def _place():
    ring = [(0, z) for z in range(16)] + [(1, z) for z in range(15, -1, -1)]
    cycle = [(0, 0), (0, 1), (0, 2), (0, 3), (1, 3), (1, 2), (1, 1), (1, 0)]
    device = np.zeros((CBEADS, SLABS), np.int64)
    role = np.zeros((512, 2), np.int64)
    member = np.zeros((2, 16), np.int64)
    half_of = np.zeros(SLABS, np.int64)
    for s in range(SLABS):
        half, z = ring[(s - 8) % SLABS]
        half_of[s] = half
        for b in range(CBEADS):
            q, core = divmod(b, 2)
            xx, y = cycle[q]
            x = xx if half == 0 else 3 - xx
            d = ((z % 8) * 2 + core) * 32 + (z // 8) * 16 + x * 4 + y
            device[b, s] = d
            role[d] = (b, s)
            member[half, (x % 2) * 8 + y * 2 + core] = b
    return device, role, member, half_of


DEVICE, ROLE, MEMBER, HALF = _place()


def _table():
    b = np.arange(BEADS)[None, :] / BEADS
    c = np.arange(CBEADS)[:, None] / CBEADS
    t = 2.0 * np.pi * (b - c)
    total = 1.0 + np.cos(0.5 * CBEADS * t)
    for k in range(1, CBEADS // 2):
        total = total + 2.0 * np.cos(k * t)
    return (total / BEADS).astype(np.float32)


def _settings():
    table = _table()
    out = np.zeros((CBEADS * SLABS, 128), np.float32)
    for d in range(CBEADS * SLABS):
        b, s = ROLE[d]
        out[d, : 16 * MINE] = table[MEMBER[HALF[s]]][:, b * MINE : (b + 1) * MINE].reshape(-1)
        out[d, SLAB_AT] = s
        out[d, CORE_AT] = b % 2
        edges = table[MEMBER[HALF[s]]][:, [(b * MINE - 1) % BEADS, (b * MINE + MINE) % BEADS]]
        out[d, EDGE_AT : EDGE_AT + 32] = edges.reshape(-1)
    return out


SLAB_AT = 16 * MINE
CORE_AT = SLAB_AT + 1
EDGE_AT = SLAB_AT + 2
SETTINGS = _settings()


def _moves(f):
    return [
        (int(DEVICE[b, s]), int(DEVICE[f(b, s)]))
        for b in range(CBEADS)
        for s in range(SLABS)
    ]


SLAB_UP = _moves(lambda b, s: (b, (s + 1) % SLABS))
SLAB_DOWN = _moves(lambda b, s: (b, (s - 1) % SLABS))
BEAD_SWAP = _moves(lambda b, s: ((b + (1 if b % 2 else -1)) % CBEADS, s))
MOVE_IN = [(b * SLABS + s, int(DEVICE[b, s])) for b in range(CBEADS) for s in range(SLABS)]
MOVE_OUT = [(d, h) for h, d in MOVE_IN]


def pieces(v):
    high = v.astype(bf16).astype(f32)
    rest = v - high
    mid = rest.astype(bf16).astype(f32)
    return high, mid, rest - mid


def halves(lower, upper):
    return jnp.concatenate([lower, upper], axis=0)


def put(ref, row, value):
    ref[pl.ds(row, 8, stride=8), :] = value


def wide(ref):
    return jnp.concatenate([ref[8 * k : 8 * k + 8, :] for k in range(8)], axis=1)


def init_rows(src, tgt):
    ones = jnp.ones((8, 128), f32)
    zeros = jnp.zeros((8, 128), f32)
    put(src, 4, ones)
    put(tgt, 3, ones)
    for k in range(5, 8):
        put(src, k, zeros)
        put(tgt, k, zeros)


def scaled(coords, scale):
    alpha = math.sqrt(scale * math.log2(math.e))
    a = [alpha * y for y in coords]
    return a, -0.5 * (a[0] * a[0] + a[1] * a[1] + a[2] * a[2])


def put_sources(src, qs, lhs, coords, share, scale):
    a, norm = scaled(coords, scale)
    for k, v in enumerate(a + [norm]):
        put(src, k, v)
    for k, v in enumerate([share] + [share * y for y in coords]):
        put(qs, k, v)
        put(qs, 4 + k, v)
    high, mid, low = pieces(wide(src))
    rows = jnp.concatenate([high, high, mid, mid, high, low], axis=0)
    for block in range(8):
        part = slice(128 * block, 128 * block + 128)
        lhs[part, :] = rows[:, part].T.astype(bf16)
    high, mid, low = pieces(wide(qs))
    upper = lax.broadcasted_iota(jnp.int32, (8, 1024), 0) < 4
    return jnp.concatenate([jnp.where(upper, high, mid), jnp.where(upper, low, 0.0)], axis=0).astype(bf16)


def put_targets(tgt, coords, scale):
    a, norm = scaled(coords, scale)
    for k, v in enumerate(a):
        put(tgt, k, v)
    put(tgt, 4, norm)
    high, mid, low = pieces(wide(tgt))
    return jnp.concatenate([high, mid, high, mid, low, high], axis=0).astype(bf16)


def stream(tasks, ahead=AHEAD):
    totals = {}
    ready = []
    for t in range(len(tasks) + ahead):
        if t < len(tasks):
            lhs, first, rhs, q, key = tasks[t]
            ready.append(jnp.dot(lhs[first : first + STEP, :], rhs, preferred_element_type=f32))
        if t < ahead:
            continue
        lhs, first, rhs, q, key = tasks[t - ahead]
        weight = jnp.exp2(ready[t - ahead])
        high = weight.astype(bf16)
        low = (weight - high.astype(f32)).astype(bf16)
        mine = q[:, first : first + STEP]
        part = jnp.dot(mine, high, preferred_element_type=f32)
        part = part + jnp.dot(mine, low, preferred_element_type=f32)
        totals[key] = totals[key] + part if key in totals else part
    return totals


def chunks(lhs, first, last, rhs, start, stop, q, key):
    return [
        (lhs, j, rhs[:, i : i + WIDTH], q, (key, i))
        for j in range(first, last, STEP)
        for i in range(start, stop, WIDTH)
    ]


def joined(totals, key):
    return jnp.concatenate([totals[key, i] for i in range(0, 1024, WIDTH)], axis=1)


def sums_of(total, rows):
    r = total[0:8]
    r = r + jnp.concatenate([r[4:8], r[0:4]], axis=0) + total[8:16]
    for block in range(8):
        rows[8 * block : 8 * block + 8, :] = r[:, 128 * block : 128 * block + 128]
    return [rows[pl.ds(k, 8, stride=8), :] for k in range(4)]


def field(coords, sums, share, scale):
    return [share * scale * (coords[k] * sums[0] - sums[1 + k]) for k in range(3)]


def slot(scr, i):
    return scr[5 * i : 5 * i + 5]


SCRATCH = 2 * [
    pltpu.VMEM((64, 128), f32),
    pltpu.VMEM((64, 128), f32),
    pltpu.VMEM((64, 128), f32),
    pltpu.VMEM((1024, 48), bf16),
    pltpu.VMEM((64, 128), f32),
]


def bead_at(ref, b):
    return [ref[pl.ds(24 * b + 8 * k, 8), :] for k in range(3)]


def near_own_kernel(y_ref, p_ref, out_ref, *scr):
    share = p_ref[A_ROW : A_ROW + 8, :]
    for i in range(2):
        init_rows(*slot(scr, i)[:2])

    def two(i, carry):
        tasks = []
        for j in range(2):
            src, tgt, qs, lhs, _ = slot(scr, j)
            coords = bead_at(y_ref, 2 * i + j)
            q = put_sources(src, qs, lhs, coords, share, NEAR)
            rhs = put_targets(tgt, coords, NEAR)
            tasks += chunks(lhs, 0, 1024, rhs, 0, 1024, q, j)
        totals = stream(tasks)
        for j in range(2):
            for k, r in enumerate(sums_of(joined(totals, j), slot(scr, j)[4])):
                out_ref[pl.ds(64 * i + 32 * j + 8 * k, 8), :] = r
        return carry

    lax.fori_loop(0, MINE // 2, two, 0)


def emit(y_refs, up_ref, down_ref):
    for i in range(12):
        y = y_refs[8 * i : 8 * i + 8, :]
        down_ref[4 * i : 4 * i + 4, :] = y[0:4]
        up_ref[4 * i : 4 * i + 4, :] = y[4:8]


def emit_edges(first, last, inner_ref, outer_ref, core):
    odd = core > 0.5
    inner_ref[...] = jnp.where(odd, first, last)
    outer_ref[...] = jnp.where(odd, last, first)


def edges_of(inner, outer, core):
    odd = core > 0.5
    from_pair = jnp.where(odd, inner[0:24, :], inner[24:48, :])
    return jnp.where(odd, from_pair, outer[...]), jnp.where(odd, outer[...], from_pair)


def emit_partial(y_refs, cols_ref, part_ref):
    y = [y_refs[24 * b : 24 * b + 24, :] for b in range(MINE)]
    for r in range(16):
        total = cols_ref[0, MINE * r] * y[0]
        for b in range(1, MINE):
            total = total + cols_ref[0, MINE * r + b] * y[b]
        part_ref[24 * r : 24 * r + 24, :] = total


def spread(ref, out_ref, centre):
    for k in range(3):
        for block in range(8):
            value = ref[k, :, 128 * block : 128 * block + 128]
            out_ref[pl.ds(8 * k + block, 4, stride=24), :] = value if centre is None else value - centre[k]


def pack_kernel(v_ref, m_ref, a_ref, q_ref, out_ref):
    spread(v_ref, out_ref, None)
    out_ref[M_ROW : M_ROW + 8, :] = m_ref[...]
    out_ref[A_ROW : A_ROW + 8, :] = a_ref[...]
    out_ref[Q_ROW : Q_ROW + 8, :] = q_ref[...]


def unpack(value_ref, out_ref, base):
    for k in range(3):
        for block in range(8):
            out_ref[base + k, :, 128 * block : 128 * block + 128] = value_ref[pl.ds(8 * k + block, 4, stride=24), :]


def start_kernel(cols_ref, x_ref, y_ref, up_ref, down_ref, inner_ref, outer_ref, part_ref):
    spread(x_ref, y_ref, (2.0 * cols_ref[0, SLAB_AT] + 1.0, 1.0, 1.0))
    emit(y_ref, up_ref, down_ref)
    emit_edges(y_ref[0:24, :], y_ref[72:96, :], inner_ref, outer_ref, cols_ref[0, CORE_AT])
    emit_partial(y_ref, cols_ref, part_ref)


def near_halo_body(rate, p_ref, y_ref, v_ref, r_ref, left, right, wide_l, wide_r, edges, store, scr):
    chain = scr[10]
    for i in range(2):
        init_rows(*slot(scr, i)[:2])
    own = p_ref[A_ROW : A_ROW + 8, :]
    mass = p_ref[M_ROW : M_ROW + 8, :]
    inverse = 1.0 / mass
    share = halves(wide_l[WIDE + 4 : WIDE + 8, :], wide_r[WIDE : WIDE + 4, :])
    chain[0:24, :], chain[120:144, :] = edges
    chain[24:120, :] = y_ref[...]
    shift = jnp.where(lax.broadcasted_iota(jnp.int32, (8, 128), 0) < 4, -2.0, 2.0).astype(f32)

    def two(i, carry):
        at = pl.multiple_of(48 * i, 8)
        lows = left[pl.ds(pl.multiple_of(24 * i, 8), 24), :]
        highs = right[pl.ds(pl.multiple_of(24 * i, 8), 24), :]
        tasks = []
        places = []
        for j in range(2):
            src, tgt, qs, lhs, _ = slot(scr, j)
            coords = [y_ref[pl.ds(at + 24 * j + 8 * k, 8), :] for k in range(3)]
            far = []
            for k in range(3):
                h = 12 * j + 4 * k
                far.append(halves(lows[h : h + 4], highs[h : h + 4]))
            far[0] = far[0] + shift
            q = put_sources(src, qs, lhs, far, share, NEAR)
            rhs = put_targets(tgt, coords, NEAR)
            tasks += chunks(lhs, 0, 512, rhs, 0, 512, q, j)
            tasks += chunks(lhs, 512, 1024, rhs, 512, 1024, q, j)
            places.append(coords)
        totals = stream(tasks)
        for j in range(2):
            coords = places[j]
            sums = sums_of(joined(totals, j), slot(scr, j)[4])
            mine = pl.multiple_of(64 * i, 8) + 32 * j
            sums = [s + r_ref[pl.ds(mine + 8 * k, 8), :] for k, s in enumerate(sums)]
            force = field(coords, sums, own, NEAR)
            for k in range(3):
                r = at + 24 * j + 8 * k
                spring = 2.0 * coords[k] - chain[pl.ds(r, 8), :] - chain[pl.ds(r + 48, 8), :]
                total = force[k] - SPRING * mass * spring
                store(r, coords[k], v_ref[pl.ds(r, 8), :] + rate * total * inverse)
        return carry

    lax.fori_loop(0, MINE // 2, two, 0)


def near_slow_kernel(rate, cols_ref, p_ref, y_ref, v_ref, r_ref, left, right, wide_l, wide_r, inner, outer, vo_ref, *rest):
    def store(r, y, v):
        vo_ref[pl.ds(r, 8), :] = v

    core = cols_ref[0, CORE_AT]
    edges = edges_of(inner, outer, core)
    scr = rest[-len(SCRATCH) - 1 :]
    near_halo_body(rate, p_ref, y_ref, v_ref, r_ref, left, right, wide_l, wide_r, edges, store, scr)
    if len(rest) > len(scr):
        first = y_ref[0:24, :] + TIME_STEP * vo_ref[0:24, :]
        last = y_ref[72:96, :] + TIME_STEP * vo_ref[72:96, :]
        emit_edges(first, last, rest[0], rest[1], core)


def near_fast_kernel(cols_ref, p_ref, y_ref, v_ref, r_ref, left, right, wide_l, wide_r, before, after, *rest):
    vo_ref, yo_ref, up_ref, down_ref, in_ref, ou_ref, part_ref = rest[:7]
    scr = rest[7:]

    def store(r, y, v):
        vo_ref[pl.ds(r, 8), :] = v
        yo_ref[pl.ds(r, 8), :] = y + TIME_STEP * v

    edges = (before[...], after[...])
    near_halo_body(TIME_STEP, p_ref, y_ref, v_ref, r_ref, left, right, wide_l, wide_r, edges, store, scr)
    emit(yo_ref, up_ref, down_ref)
    emit_edges(yo_ref[0:24, :], yo_ref[72:96, :], in_ref, ou_ref, cols_ref[0, CORE_AT])
    emit_partial(yo_ref, cols_ref, part_ref)


def gather_kernel(wide, recv_ref, up_ref, down_ref, p_ref, yc_ref, up_out, down_out):
    total = recv_ref[0:24, :]
    for r in range(1, 16):
        total = total + recv_ref[24 * r : 24 * r + 24, :]
    yc_ref[...] = total
    for out, ref in ((up_out, up_ref), (down_out, down_ref)):
        out[0:48, :] = ref[...]
        out[48:72, :] = total
        if wide:
            out[WIDE : WIDE + 16, :] = p_ref[A_ROW : A_ROW + 16, :]


def far_own_kernel(yc_ref, p_ref, out_ref, src, tgt, qs, lhs, rows):
    init_rows(src, tgt)
    coords = bead_at(yc_ref, 0)
    q = put_sources(src, qs, lhs, coords, p_ref[Q_ROW : Q_ROW + 8, :], FAR)
    rhs = put_targets(tgt, coords, FAR)
    total = joined(stream(chunks(lhs, 0, 1024, rhs, 0, 1024, q, 0)), 0)
    for k, r in enumerate(sums_of(total, rows)):
        out_ref[8 * k : 8 * k + 8, :] = r


def far_halo_kernel(yc_ref, p_ref, r_ref, left, right, wide_l, wide_r, out_ref, *scr):
    coords = bead_at(yc_ref, 0)
    tasks = []
    for i, (block, rows) in enumerate(((left, wide_l), (right, wide_r))):
        src, tgt, qs, lhs, _ = slot(scr, i)
        init_rows(src, tgt)
        if i == 0:
            rhs = put_targets(tgt, coords, FAR)
        there = [block[48 + 8 * k : 56 + 8 * k, :] for k in range(3)]
        there[0] = there[0] + (2.0 if i else -2.0)
        q = put_sources(src, qs, lhs, there, rows[WIDE + 8 : WIDE + 16, :], FAR)
        if i == 0:
            tasks += chunks(lhs, 0, 512, rhs, 0, 512, q, 0)
            tasks += chunks(lhs, 512, 1024, rhs, 0, 1024, q, 0)
        else:
            tasks += chunks(lhs, 0, 512, rhs, 0, 1024, q, 0)
            tasks += chunks(lhs, 512, 1024, rhs, 512, 1024, q, 0)
    totals = stream(tasks)
    total = joined(totals, 0)
    sums = [s + r_ref[8 * k : 8 * k + 8, :] for k, s in enumerate(sums_of(total, slot(scr, 0)[4]))]
    force = field(coords, sums, p_ref[Q_ROW : Q_ROW + 8, :], FAR)
    for r in range(16):
        for k in range(3):
            out_ref[24 * r + 8 * k : 24 * r + 8 * k + 8, :] = force[k]


def kick(rate, cols_ref, p_ref, v_ref, far_ref):
    inverse = (rate * BEADS / CBEADS) / p_ref[M_ROW : M_ROW + 8, :]
    inverse = jnp.concatenate([inverse] * 3, axis=0)
    out = []
    far = [far_ref[24 * r : 24 * r + 24, :] for r in range(16)]
    for b in range(MINE):
        total = cols_ref[0, b] * far[0]
        for r in range(1, 16):
            total = total + cols_ref[0, MINE * r + b] * far[r]
        out.append(v_ref[24 * b : 24 * b + 24, :] + inverse * total)
    return out


def update_kernel(rate, cols_ref, p_ref, y_ref, v_ref, far_ref, inner, outer,
                  vo_ref, yo_ref, up_ref, down_ref, before_ref, after_ref):
    for b, v in enumerate(kick(rate, cols_ref, p_ref, v_ref, far_ref)):
        vo_ref[24 * b : 24 * b + 24, :] = v
        yo_ref[24 * b : 24 * b + 24, :] = y_ref[24 * b : 24 * b + 24, :] + TIME_STEP * v
    emit(yo_ref, up_ref, down_ref)
    inverse = (TIME_STEP * rate * BEADS / CBEADS) / p_ref[M_ROW : M_ROW + 8, :]
    inverse = jnp.concatenate([inverse] * 3, axis=0)
    edges = edges_of(inner, outer, cols_ref[0, CORE_AT])
    for e, out in enumerate((before_ref, after_ref)):
        total = cols_ref[0, EDGE_AT + e] * far_ref[0:24, :]
        for r in range(1, 16):
            total = total + cols_ref[0, EDGE_AT + 2 * r + e] * far_ref[24 * r : 24 * r + 24, :]
        out[...] = edges[e] + inverse * total


def final_kernel(rate, cols_ref, p_ref, v_ref, y_ref, first_ref, far_ref, out_ref, rows):
    for i in range(12):
        rows[8 * i : 8 * i + 8, :] = y_ref[8 * i : 8 * i + 8, :] - first_ref[8 * i : 8 * i + 8, :]
    unpack(rows, out_ref, 0)
    for b, v in enumerate(kick(rate, cols_ref, p_ref, v_ref, far_ref)):
        rows[24 * b : 24 * b + 24, :] = v
    unpack(rows, out_ref, 3)


def call(kernel, outs, cols, args, scratch=(), flops=1000, order=(), passed=()):
    specs = [] if cols is None else [pl.BlockSpec(memory_space=pltpu.SMEM)]
    specs += [pl.BlockSpec(memory_space=pltpu.VMEM)] * len(args)
    used = len(specs)
    specs += [pl.BlockSpec(memory_space=pl.ANY)] * (len(order) + len(passed))
    given = ([] if cols is None else [cols]) + list(args) + list(order) + list(passed)
    base = used + len(order)

    def body(*refs):
        kernel(*refs[:used], *refs[len(given) : len(given) + len(outs)], *refs[len(given) + len(outs) + len(passed) :])

    shapes = [jax.ShapeDtypeStruct(s, f32) for s in outs] + [jax.ShapeDtypeStruct(x.shape, f32) for x in passed]
    return pl.pallas_call(
        body,
        out_shape=shapes,
        in_specs=specs,
        out_specs=[pl.BlockSpec(memory_space=pltpu.VMEM)] * len(outs) + [pl.BlockSpec(memory_space=pl.ANY)] * len(passed),
        scratch_shapes=list(scratch),
        input_output_aliases={base + i: len(outs) + i for i in range(len(passed))},
        cost_estimate=pl.CostEstimate(flops=flops, bytes_accessed=400000, transcendentals=0),
        compiler_params=pltpu.CompilerParams(vmem_limit_bytes=12 * 1024 * 1024),
    )(*given)


HALO = (48, 128)
BEAD = (24, 128)
STATE = (96, 128)
TEAM_ROWS = (16, 24, 128)
BOTH = (6, 4, 1024)


def exchange_team(x):
    x = lax.all_to_all(x.reshape(TEAM_ROWS), TEAM, split_axis=0, concat_axis=0, tiled=True)
    return x.reshape(384, 128)


def send(x, moves):
    return lax.ppermute(x, AXES, moves)


def pair(x):
    return lax.all_gather(x, "core", axis=0, tiled=True)


CHAIN = pltpu.VMEM((144, 128), f32)


def shards(positions, velocities, masses, amplitudes, charges):
    x = send(jnp.transpose(positions, (1, 0, 2)), MOVE_IN)
    (packed,) = call(
        pack_kernel,
        [(PACKED, 128)],
        None,
        [
            jnp.transpose(velocities, (1, 0, 2)),
            masses.reshape(8, 128),
            amplitudes.reshape(8, 128),
            charges.reshape(8, 128),
        ],
    )
    p = send(packed, MOVE_IN)
    cols = lax.dynamic_slice_in_dim(jnp.asarray(SETTINGS), lax.axis_index(AXES), 1, 0)
    y, up, down, inner, outer, part = call(start_kernel, [STATE, HALO, HALO, BEAD, BEAD, (384, 128)], cols, [x])
    first = y
    v = p
    wide_l = wide_r = None
    big = 400_000_000
    for stage in range(5):
        slow = stage % 2 == 0
        if not slow:
            left = send(up, SLAB_UP)
            right = send(down, SLAB_DOWN)
            (sums,) = call(near_own_kernel, [(128, 128)], None, [y, p], SCRATCH, big)
            v, y, up, down, inner, outer, part = call(
                near_fast_kernel,
                [STATE, STATE, HALO, HALO, BEAD, BEAD, (384, 128)],
                cols,
                [p, y, v, sums, left, right, wide_l, wide_r, before, after],
                SCRATCH + [CHAIN],
                big // 2,
            )
            continue
        edge = stage in (0, 4)
        got = exchange_team(part)
        inner = pair(inner)
        (sums,) = call(near_own_kernel, [(128, 128)], None, [y, p], SCRATCH, big)

        def gather(*refs, wide=stage == 0):
            gather_kernel(wide, *refs)

        size = (WIDE + 16 * (stage == 0), 128)
        yc, up, down, outer = call(gather, [BEAD, size, size], None, [got, up, down, p], order=[sums], passed=[outer])
        left = send(up, SLAB_UP)
        right = send(down, SLAB_DOWN)
        outer = send(outer, BEAD_SWAP)
        if stage == 0:
            wide_l, wide_r = left, right
        (far_sums,) = call(far_own_kernel, [(32, 128)], None, [yc, p], SCRATCH[:5], big // 4)
        (copies,) = call(
            far_halo_kernel, [(384, 128)], None, [yc, p, far_sums, left, right, wide_l, wide_r], SCRATCH, big // 4
        )
        far = exchange_team(copies)
        rate = TIME_STEP * (0.5 if edge else 1.0)

        def near_slow(*refs, rate=rate):
            near_slow_kernel(rate, *refs)

        v, *ends = call(
            near_slow,
            [STATE] + [BEAD] * (2 * (stage < 4)),
            cols,
            [p, y, v, sums, left, right, wide_l, wide_r, inner, outer],
            SCRATCH + [CHAIN],
            big // 2,
        )
        rate = OUTER_STEP * (0.5 if edge else 1.0)
        if stage == 4:

            def final(*refs, rate=rate):
                final_kernel(rate, *refs)

            (both,) = call(final, [BOTH], cols, [p, v, y, first, far], [pltpu.VMEM(STATE, f32)])
        else:

            def update(*refs, rate=rate):
                update_kernel(rate, *refs)

            inner = pair(ends[0])
            outer = send(ends[1], BEAD_SWAP)
            v, y, up, down, before, after = call(
                update, [STATE, STATE, HALO, HALO, BEAD, BEAD], cols, [p, y, v, far, inner, outer]
            )
    both = jnp.transpose(lax.ppermute(both, AXES, MOVE_OUT), (1, 0, 2))
    return both[:, 0:3], both[:, 3:6]


def solution(mesh):
    fine = Mesh(mesh.devices.reshape((2,) * 9), AXES)
    bead = ("z2", "z1", "z0", "core")
    slab = ("zh", "x1", "x0", "y1", "y0")
    wide = P(bead, None, slab)
    flat = P(slab)
    return jax.shard_map(
        shards,
        mesh=fine,
        in_specs=(wide, wide, flat, flat, flat),
        out_specs=(wide, wide),
        check_vma=False,
    )
```

```python
import math

import jax
import jax.numpy as jnp
import numpy as np
from jax import lax
from jax.experimental import pallas as pl
from jax.experimental.pallas import tpu as pltpu
from jax.sharding import Mesh, PartitionSpec as P


TIME_STEP = 0.05
OUTER_STEP = 0.1
SPRING = 25.0
NEAR = 4.0
FAR = 2.0
BEADS = 64
CBEADS = 16
SLABS = 32
MINE = BEADS // CBEADS
STEP = 256
WIDTH = 512
AHEAD = 2

A_ROW = 96
Q_ROW = 104
M_ROW = 96
PLACES = (112, 128)
MOTION = (104, 128)
WIDE = 72

AXES = ("z2", "z1", "z0", "core", "zh", "x1", "x0", "y1", "y0")
TEAM = ("x0", "y1", "y0", "core")
f32 = jnp.float32
bf16 = jnp.bfloat16


def _place():
    ring = [(0, z) for z in range(16)] + [(1, z) for z in range(15, -1, -1)]
    cycle = [(0, 0), (0, 1), (0, 2), (0, 3), (1, 3), (1, 2), (1, 1), (1, 0)]
    device = np.zeros((CBEADS, SLABS), np.int64)
    role = np.zeros((512, 2), np.int64)
    member = np.zeros((2, 16), np.int64)
    half_of = np.zeros(SLABS, np.int64)
    for s in range(SLABS):
        half, z = ring[(s - 8) % SLABS]
        half_of[s] = half
        for b in range(CBEADS):
            q, core = divmod(b, 2)
            xx, y = cycle[q]
            x = xx if half == 0 else 3 - xx
            d = ((z % 8) * 2 + core) * 32 + (z // 8) * 16 + x * 4 + y
            device[b, s] = d
            role[d] = (b, s)
            member[half, (x % 2) * 8 + y * 2 + core] = b
    return device, role, member, half_of


DEVICE, ROLE, MEMBER, HALF = _place()


def _table():
    b = np.arange(BEADS)[None, :] / BEADS
    c = np.arange(CBEADS)[:, None] / CBEADS
    t = 2.0 * np.pi * (b - c)
    total = 1.0 + np.cos(0.5 * CBEADS * t)
    for k in range(1, CBEADS // 2):
        total = total + 2.0 * np.cos(k * t)
    return (total / BEADS).astype(np.float32)


def _settings():
    table = _table()
    out = np.zeros((CBEADS * SLABS, 128), np.float32)
    for d in range(CBEADS * SLABS):
        b, s = ROLE[d]
        out[d, : 16 * MINE] = table[MEMBER[HALF[s]]][:, b * MINE : (b + 1) * MINE].reshape(-1)
        out[d, SLAB_AT] = s
        out[d, CORE_AT] = b % 2
        edges = table[MEMBER[HALF[s]]][:, [(b * MINE - 1) % BEADS, (b * MINE + MINE) % BEADS]]
        out[d, EDGE_AT : EDGE_AT + 32] = edges.reshape(-1)
    return out


SLAB_AT = 16 * MINE
CORE_AT = SLAB_AT + 1
EDGE_AT = SLAB_AT + 2
SETTINGS = _settings()


def _moves(f):
    return [
        (int(DEVICE[b, s]), int(DEVICE[f(b, s)]))
        for b in range(CBEADS)
        for s in range(SLABS)
    ]


SLAB_UP = _moves(lambda b, s: (b, (s + 1) % SLABS))
SLAB_DOWN = _moves(lambda b, s: (b, (s - 1) % SLABS))
BEAD_SWAP = _moves(lambda b, s: ((b + (1 if b % 2 else -1)) % CBEADS, s))
MOVE_IN = [(b * SLABS + s, int(DEVICE[b, s])) for b in range(CBEADS) for s in range(SLABS)]
MOVE_OUT = [(d, h) for h, d in MOVE_IN]


def pieces(v):
    high = v.astype(bf16).astype(f32)
    rest = v - high
    mid = rest.astype(bf16).astype(f32)
    return high, mid, rest - mid


def halves(lower, upper):
    return jnp.concatenate([lower, upper], axis=0)


def put(ref, row, value):
    ref[pl.ds(row, 8, stride=8), :] = value


def wide(ref):
    return jnp.concatenate([ref[8 * k : 8 * k + 8, :] for k in range(8)], axis=1)


def init_rows(src, tgt):
    ones = jnp.ones((8, 128), f32)
    zeros = jnp.zeros((8, 128), f32)
    put(src, 4, ones)
    put(tgt, 3, ones)
    for k in range(5, 8):
        put(src, k, zeros)
        put(tgt, k, zeros)


def scaled(coords, scale):
    alpha = math.sqrt(scale * math.log2(math.e))
    a = [alpha * y for y in coords]
    return a, -0.5 * (a[0] * a[0] + a[1] * a[1] + a[2] * a[2])


def put_sources(src, qs, lhs, coords, share, scale):
    a, norm = scaled(coords, scale)
    for k, v in enumerate(a + [norm]):
        put(src, k, v)
    for k, v in enumerate([share] + [share * y for y in coords]):
        put(qs, k, v)
        put(qs, 4 + k, v)
    high, mid, low = pieces(wide(src))
    rows = jnp.concatenate([high, high, mid, mid, high, low], axis=0)
    for block in range(8):
        part = slice(128 * block, 128 * block + 128)
        lhs[part, :] = rows[:, part].T.astype(bf16)
    high, mid, low = pieces(wide(qs))
    upper = lax.broadcasted_iota(jnp.int32, (8, 1024), 0) < 4
    return jnp.concatenate([jnp.where(upper, high, mid), jnp.where(upper, low, 0.0)], axis=0).astype(bf16)


def put_targets(tgt, coords, scale):
    a, norm = scaled(coords, scale)
    for k, v in enumerate(a):
        put(tgt, k, v)
    put(tgt, 4, norm)
    high, mid, low = pieces(wide(tgt))
    return jnp.concatenate([high, mid, high, mid, low, high], axis=0).astype(bf16)


def stream(tasks, ahead=AHEAD):
    totals = {}
    ready = []
    for t in range(len(tasks) + ahead):
        if t < len(tasks):
            lhs, first, rhs, q, key = tasks[t]
            ready.append(jnp.dot(lhs[first : first + STEP, :], rhs, preferred_element_type=f32))
        if t < ahead:
            continue
        lhs, first, rhs, q, key = tasks[t - ahead]
        weight = jnp.exp2(ready[t - ahead])
        high = weight.astype(bf16)
        low = (weight - high.astype(f32)).astype(bf16)
        mine = q[:, first : first + STEP]
        part = jnp.dot(mine, high, preferred_element_type=f32)
        part = part + jnp.dot(mine, low, preferred_element_type=f32)
        totals[key] = totals[key] + part if key in totals else part
    return totals


def chunks(lhs, first, last, rhs, start, stop, q, key):
    return [
        (lhs, j, rhs[:, i : i + WIDTH], q, (key, i))
        for j in range(first, last, STEP)
        for i in range(start, stop, WIDTH)
    ]


def joined(totals, key):
    return jnp.concatenate([totals[key, i] for i in range(0, 1024, WIDTH)], axis=1)


def sums_of(total, rows):
    r = total[0:8]
    r = r + jnp.concatenate([r[4:8], r[0:4]], axis=0) + total[8:16]
    for block in range(8):
        rows[8 * block : 8 * block + 8, :] = r[:, 128 * block : 128 * block + 128]
    return [rows[pl.ds(k, 8, stride=8), :] for k in range(4)]


def field(coords, sums, share, scale):
    return [share * scale * (coords[k] * sums[0] - sums[1 + k]) for k in range(3)]


def slot(scr, i):
    return scr[5 * i : 5 * i + 5]


SCRATCH = 2 * [
    pltpu.VMEM((64, 128), f32),
    pltpu.VMEM((64, 128), f32),
    pltpu.VMEM((64, 128), f32),
    pltpu.VMEM((1024, 48), bf16),
    pltpu.VMEM((64, 128), f32),
]


def bead_at(ref, b):
    return [ref[pl.ds(24 * b + 8 * k, 8), :] for k in range(3)]


def near_own_kernel(y_ref, p_ref, out_ref, *scr):
    share = p_ref[A_ROW : A_ROW + 8, :]
    for i in range(2):
        init_rows(*slot(scr, i)[:2])

    def two(i, carry):
        tasks = []
        for j in range(2):
            src, tgt, qs, lhs, _ = slot(scr, j)
            coords = bead_at(y_ref, 2 * i + j)
            q = put_sources(src, qs, lhs, coords, share, NEAR)
            rhs = put_targets(tgt, coords, NEAR)
            tasks += chunks(lhs, 0, 1024, rhs, 0, 1024, q, j)
        totals = stream(tasks)
        for j in range(2):
            for k, r in enumerate(sums_of(joined(totals, j), slot(scr, j)[4])):
                out_ref[pl.ds(64 * i + 32 * j + 8 * k, 8), :] = r
        return carry

    lax.fori_loop(0, MINE // 2, two, 0)


def emit(y_refs, up_ref, down_ref):
    for i in range(12):
        y = y_refs[8 * i : 8 * i + 8, :]
        down_ref[4 * i : 4 * i + 4, :] = y[0:4]
        up_ref[4 * i : 4 * i + 4, :] = y[4:8]


def emit_edges(first, last, inner_ref, outer_ref, core):
    odd = core > 0.5
    inner_ref[...] = jnp.where(odd, first, last)
    outer_ref[...] = jnp.where(odd, last, first)


def edges_of(inner, outer, core):
    odd = core > 0.5
    from_pair = jnp.where(odd, inner[0:24, :], inner[24:48, :])
    return jnp.where(odd, from_pair, outer[...]), jnp.where(odd, outer[...], from_pair)


def emit_partial(y_refs, cols_ref, part_ref):
    y = [y_refs[24 * b : 24 * b + 24, :] for b in range(MINE)]
    for r in range(16):
        total = cols_ref[0, MINE * r] * y[0]
        for b in range(1, MINE):
            total = total + cols_ref[0, MINE * r + b] * y[b]
        part_ref[24 * r : 24 * r + 24, :] = total


def spread(ref, out_ref):
    for k in range(3):
        for block in range(8):
            out_ref[pl.ds(8 * k + block, 4, stride=24), :] = ref[k, :, 128 * block : 128 * block + 128]


def pack_kernel(x_ref, *refs):
    out_ref = refs[-1]
    spread(x_ref, out_ref)
    for i, ref in enumerate(refs[:-1]):
        out_ref[96 + 8 * i : 104 + 8 * i, :] = ref[...]


def unpack(value_ref, out_ref, base):
    for k in range(3):
        for block in range(8):
            out_ref[base + k, :, 128 * block : 128 * block + 128] = value_ref[pl.ds(8 * k + block, 4, stride=24), :]


def start_kernel(cols_ref, x_ref, y_ref, up_ref, down_ref, inner_ref, outer_ref, part_ref):
    centre = (2.0 * cols_ref[0, SLAB_AT] + 1.0, 1.0, 1.0)
    for i in range(12):
        y_ref[8 * i : 8 * i + 8, :] = x_ref[8 * i : 8 * i + 8, :] - centre[i % 3]
    emit(y_ref, up_ref, down_ref)
    emit_edges(y_ref[0:24, :], y_ref[72:96, :], inner_ref, outer_ref, cols_ref[0, CORE_AT])
    emit_partial(y_ref, cols_ref, part_ref)


def near_halo_body(rate, p_ref, m_ref, y_ref, v_ref, r_ref, left, right, wide_l, wide_r, edges, store, scr):
    chain = scr[10]
    for i in range(2):
        init_rows(*slot(scr, i)[:2])
    own = p_ref[A_ROW : A_ROW + 8, :]
    mass = m_ref[M_ROW : M_ROW + 8, :]
    inverse = 1.0 / mass
    share = halves(wide_l[WIDE + 4 : WIDE + 8, :], wide_r[WIDE : WIDE + 4, :])
    chain[0:24, :], chain[120:144, :] = edges
    chain[24:120, :] = y_ref[...]
    shift = jnp.where(lax.broadcasted_iota(jnp.int32, (8, 128), 0) < 4, -2.0, 2.0).astype(f32)

    def two(i, carry):
        at = pl.multiple_of(48 * i, 8)
        lows = left[pl.ds(pl.multiple_of(24 * i, 8), 24), :]
        highs = right[pl.ds(pl.multiple_of(24 * i, 8), 24), :]
        tasks = []
        places = []
        for j in range(2):
            src, tgt, qs, lhs, _ = slot(scr, j)
            coords = [y_ref[pl.ds(at + 24 * j + 8 * k, 8), :] for k in range(3)]
            far = []
            for k in range(3):
                h = 12 * j + 4 * k
                far.append(halves(lows[h : h + 4], highs[h : h + 4]))
            far[0] = far[0] + shift
            q = put_sources(src, qs, lhs, far, share, NEAR)
            rhs = put_targets(tgt, coords, NEAR)
            tasks += chunks(lhs, 0, 512, rhs, 0, 512, q, j)
            tasks += chunks(lhs, 512, 1024, rhs, 512, 1024, q, j)
            places.append(coords)
        totals = stream(tasks)
        for j in range(2):
            coords = places[j]
            sums = sums_of(joined(totals, j), slot(scr, j)[4])
            mine = pl.multiple_of(64 * i, 8) + 32 * j
            sums = [s + r_ref[pl.ds(mine + 8 * k, 8), :] for k, s in enumerate(sums)]
            force = field(coords, sums, own, NEAR)
            for k in range(3):
                r = at + 24 * j + 8 * k
                spring = 2.0 * coords[k] - chain[pl.ds(r, 8), :] - chain[pl.ds(r + 48, 8), :]
                total = force[k] - SPRING * mass * spring
                store(r, coords[k], v_ref[pl.ds(r, 8), :] + rate * total * inverse)
        return carry

    lax.fori_loop(0, MINE // 2, two, 0)


def near_slow_kernel(rate, cols_ref, p_ref, m_ref, y_ref, v_ref, r_ref, left, right, wide_l, wide_r, inner, outer, vo_ref, *rest):
    def store(r, y, v):
        vo_ref[pl.ds(r, 8), :] = v

    core = cols_ref[0, CORE_AT]
    edges = edges_of(inner, outer, core)
    scr = rest[-len(SCRATCH) - 1 :]
    near_halo_body(rate, p_ref, m_ref, y_ref, v_ref, r_ref, left, right, wide_l, wide_r, edges, store, scr)
    if len(rest) > len(scr):
        first = y_ref[0:24, :] + TIME_STEP * vo_ref[0:24, :]
        last = y_ref[72:96, :] + TIME_STEP * vo_ref[72:96, :]
        emit_edges(first, last, rest[0], rest[1], core)


def near_fast_kernel(cols_ref, p_ref, m_ref, y_ref, v_ref, r_ref, left, right, wide_l, wide_r, before, after, *rest):
    vo_ref, yo_ref, up_ref, down_ref, in_ref, ou_ref, part_ref = rest[:7]
    scr = rest[7:]

    def store(r, y, v):
        vo_ref[pl.ds(r, 8), :] = v
        yo_ref[pl.ds(r, 8), :] = y + TIME_STEP * v

    edges = (before[...], after[...])
    near_halo_body(TIME_STEP, p_ref, m_ref, y_ref, v_ref, r_ref, left, right, wide_l, wide_r, edges, store, scr)
    emit(yo_ref, up_ref, down_ref)
    emit_edges(yo_ref[0:24, :], yo_ref[72:96, :], in_ref, ou_ref, cols_ref[0, CORE_AT])
    emit_partial(yo_ref, cols_ref, part_ref)


def gather_kernel(wide, recv_ref, up_ref, down_ref, p_ref, yc_ref, up_out, down_out):
    total = recv_ref[0:24, :]
    for r in range(1, 16):
        total = total + recv_ref[24 * r : 24 * r + 24, :]
    yc_ref[...] = total
    for out, ref in ((up_out, up_ref), (down_out, down_ref)):
        out[0:48, :] = ref[...]
        out[48:72, :] = total
        if wide:
            out[WIDE : WIDE + 16, :] = p_ref[A_ROW : A_ROW + 16, :]


def far_kernel(yc_ref, p_ref, left, right, wide_l, wide_r, out_ref, *scr):
    coords = bead_at(yc_ref, 0)
    src, tgt, qs, lhs, rows_of = slot(scr, 0)
    init_rows(src, tgt)
    q = put_sources(src, qs, lhs, coords, p_ref[Q_ROW : Q_ROW + 8, :], FAR)
    rhs = put_targets(tgt, coords, FAR)
    tasks = chunks(lhs, 0, 1024, rhs, 0, 1024, q, 0)
    for i, (block, rows) in enumerate(((left, wide_l), (right, wide_r))):
        src, tgt, qs, lhs, _ = slot(scr, i + 1)
        init_rows(src, tgt)
        there = [block[48 + 8 * k : 56 + 8 * k, :] for k in range(3)]
        there[0] = there[0] + (2.0 if i else -2.0)
        q = put_sources(src, qs, lhs, there, rows[WIDE + 8 : WIDE + 16, :], FAR)
        if i == 0:
            tasks += chunks(lhs, 0, 512, rhs, 0, 512, q, 0)
            tasks += chunks(lhs, 512, 1024, rhs, 0, 1024, q, 0)
        else:
            tasks += chunks(lhs, 0, 512, rhs, 0, 1024, q, 0)
            tasks += chunks(lhs, 512, 1024, rhs, 512, 1024, q, 0)
    sums = sums_of(joined(stream(tasks), 0), rows_of)
    force = field(coords, sums, p_ref[Q_ROW : Q_ROW + 8, :], FAR)
    for r in range(16):
        for k in range(3):
            out_ref[24 * r + 8 * k : 24 * r + 8 * k + 8, :] = force[k]


def kick(rate, cols_ref, p_ref, v_ref, far_ref):
    inverse = (rate * BEADS / CBEADS) / p_ref[M_ROW : M_ROW + 8, :]
    inverse = jnp.concatenate([inverse] * 3, axis=0)
    out = []
    far = [far_ref[24 * r : 24 * r + 24, :] for r in range(16)]
    for b in range(MINE):
        total = cols_ref[0, b] * far[0]
        for r in range(1, 16):
            total = total + cols_ref[0, MINE * r + b] * far[r]
        out.append(v_ref[24 * b : 24 * b + 24, :] + inverse * total)
    return out


def update_kernel(rate, cols_ref, p_ref, y_ref, v_ref, far_ref, inner, outer,
                  vo_ref, yo_ref, up_ref, down_ref, before_ref, after_ref):
    for b, v in enumerate(kick(rate, cols_ref, p_ref, v_ref, far_ref)):
        vo_ref[24 * b : 24 * b + 24, :] = v
        yo_ref[24 * b : 24 * b + 24, :] = y_ref[24 * b : 24 * b + 24, :] + TIME_STEP * v
    emit(yo_ref, up_ref, down_ref)
    inverse = (TIME_STEP * rate * BEADS / CBEADS) / p_ref[M_ROW : M_ROW + 8, :]
    inverse = jnp.concatenate([inverse] * 3, axis=0)
    edges = edges_of(inner, outer, cols_ref[0, CORE_AT])
    for e, out in enumerate((before_ref, after_ref)):
        total = cols_ref[0, EDGE_AT + e] * far_ref[0:24, :]
        for r in range(1, 16):
            total = total + cols_ref[0, EDGE_AT + 2 * r + e] * far_ref[24 * r : 24 * r + 24, :]
        out[...] = edges[e] + inverse * total


def final_kernel(rate, cols_ref, p_ref, v_ref, y_ref, first_ref, far_ref, out_ref, rows):
    for i in range(12):
        rows[8 * i : 8 * i + 8, :] = y_ref[8 * i : 8 * i + 8, :] - first_ref[8 * i : 8 * i + 8, :]
    unpack(rows, out_ref, 0)
    for b, v in enumerate(kick(rate, cols_ref, p_ref, v_ref, far_ref)):
        rows[24 * b : 24 * b + 24, :] = v
    unpack(rows, out_ref, 3)


def call(kernel, outs, cols, args, scratch=(), flops=1000, order=(), passed=()):
    specs = [] if cols is None else [pl.BlockSpec(memory_space=pltpu.SMEM)]
    specs += [pl.BlockSpec(memory_space=pltpu.VMEM)] * len(args)
    used = len(specs)
    specs += [pl.BlockSpec(memory_space=pl.ANY)] * (len(order) + len(passed))
    given = ([] if cols is None else [cols]) + list(args) + list(order) + list(passed)
    base = used + len(order)

    def body(*refs):
        kernel(*refs[:used], *refs[len(given) : len(given) + len(outs)], *refs[len(given) + len(outs) + len(passed) :])

    shapes = [jax.ShapeDtypeStruct(s, f32) for s in outs] + [jax.ShapeDtypeStruct(x.shape, f32) for x in passed]
    return pl.pallas_call(
        body,
        out_shape=shapes,
        in_specs=specs,
        out_specs=[pl.BlockSpec(memory_space=pltpu.VMEM)] * len(outs) + [pl.BlockSpec(memory_space=pl.ANY)] * len(passed),
        scratch_shapes=list(scratch),
        input_output_aliases={base + i: len(outs) + i for i in range(len(passed))},
        cost_estimate=pl.CostEstimate(flops=flops, bytes_accessed=400000, transcendentals=0),
        compiler_params=pltpu.CompilerParams(vmem_limit_bytes=12 * 1024 * 1024),
    )(*given)


HALO = (48, 128)
BEAD = (24, 128)
STATE = (96, 128)
TEAM_ROWS = (16, 24, 128)
BOTH = (6, 4, 1024)


def exchange_team(x):
    x = lax.all_to_all(x.reshape(TEAM_ROWS), TEAM, split_axis=0, concat_axis=0, tiled=True)
    return x.reshape(384, 128)


def send(x, moves):
    return lax.ppermute(x, AXES, moves)


def pack(x, rows, shape):
    args = [jnp.transpose(x, (1, 0, 2))] + [r.reshape(8, 128) for r in rows]
    (packed,) = call(pack_kernel, [shape], None, args)
    return packed


def pair(x):
    return lax.all_gather(x, "core", axis=0, tiled=True)


CHAIN = pltpu.VMEM((144, 128), f32)


def shards(positions, velocities, masses, amplitudes, charges):
    places = pack(positions, (amplitudes, charges), PLACES)
    p = send(places, MOVE_IN)
    motion = pack(velocities, (masses,), MOTION)
    cols = lax.dynamic_slice_in_dim(jnp.asarray(SETTINGS), lax.axis_index(AXES), 1, 0)
    y, up, down, inner, outer, part = call(start_kernel, [STATE, HALO, HALO, BEAD, BEAD, (384, 128)], cols, [p])
    first = y
    wide_l = wide_r = None
    big = 400_000_000
    for stage in range(5):
        slow = stage % 2 == 0
        if not slow:
            left = send(up, SLAB_UP)
            right = send(down, SLAB_DOWN)
            (sums,) = call(near_own_kernel, [(128, 128)], None, [y, p], SCRATCH, big)
            v, y, up, down, inner, outer, part = call(
                near_fast_kernel,
                [STATE, STATE, HALO, HALO, BEAD, BEAD, (384, 128)],
                cols,
                [p, motion, y, v, sums, left, right, wide_l, wide_r, before, after],
                SCRATCH + [CHAIN],
                big // 2,
            )
            continue
        edge = stage in (0, 4)
        got = exchange_team(part)
        inner = pair(inner)
        if stage == 0:
            sums, motion = call(near_own_kernel, [(128, 128)], None, [y, p], SCRATCH, big, passed=[motion])
            v = motion = send(motion, MOVE_IN)
        else:
            (sums,) = call(near_own_kernel, [(128, 128)], None, [y, p], SCRATCH, big)

        def gather(*refs, wide=stage == 0):
            gather_kernel(wide, *refs)

        size = (WIDE + 16 * (stage == 0), 128)
        yc, up, down, outer = call(gather, [BEAD, size, size], None, [got, up, down, p], order=[sums], passed=[outer])
        left = send(up, SLAB_UP)
        right = send(down, SLAB_DOWN)
        outer = send(outer, BEAD_SWAP)
        if stage == 0:
            wide_l, wide_r = left, right
        (copies,) = call(
            far_kernel, [(384, 128)], None, [yc, p, left, right, wide_l, wide_r], SCRATCH + SCRATCH[:5], big // 2
        )
        far = exchange_team(copies)
        rate = TIME_STEP * (0.5 if edge else 1.0)

        def near_slow(*refs, rate=rate):
            near_slow_kernel(rate, *refs)

        v, *ends = call(
            near_slow,
            [STATE] + [BEAD] * (2 * (stage < 4)),
            cols,
            [p, motion, y, v, sums, left, right, wide_l, wide_r, inner, outer],
            SCRATCH + [CHAIN],
            big // 2,
        )
        rate = OUTER_STEP * (0.5 if edge else 1.0)
        if stage == 4:

            def final(*refs, rate=rate):
                final_kernel(rate, *refs)

            (both,) = call(final, [BOTH], cols, [motion, v, y, first, far], [pltpu.VMEM(STATE, f32)])
        else:

            def update(*refs, rate=rate):
                update_kernel(rate, *refs)

            inner = pair(ends[0])
            outer = send(ends[1], BEAD_SWAP)
            v, y, up, down, before, after = call(
                update, [STATE, STATE, HALO, HALO, BEAD, BEAD], cols, [motion, y, v, far, inner, outer]
            )
    both = jnp.transpose(lax.ppermute(both, AXES, MOVE_OUT), (1, 0, 2))
    return both[:, 0:3], both[:, 3:6]


def solution(mesh):
    fine = Mesh(mesh.devices.reshape((2,) * 9), AXES)
    bead = ("z2", "z1", "z0", "core")
    slab = ("zh", "x1", "x0", "y1", "y0")
    wide = P(bead, None, slab)
    flat = P(slab)
    return jax.shard_map(
        shards,
        mesh=fine,
        in_specs=(wide, wide, flat, flat, flat),
        out_specs=(wide, wide),
        check_vma=False,
    )
```

```python
import math

import jax
import jax.numpy as jnp
import numpy as np
from jax import lax
from jax.experimental import pallas as pl
from jax.experimental.pallas import tpu as pltpu
from jax.sharding import Mesh, PartitionSpec as P


TIME_STEP = 0.05
OUTER_STEP = 0.1
SPRING = 25.0
NEAR = 4.0
FAR = 2.0
BEADS = 64
CBEADS = 16
SLABS = 32
MINE = BEADS // CBEADS
STEP = 256
WIDTH = 256
AHEAD = 4

M_ROW = 96
A_ROW = 104
Q_ROW = 112
PACKED = 120
WIDE = 72

AXES = ("z2", "z1", "z0", "core", "zh", "x1", "x0", "y1", "y0")
TEAM = ("x0", "y1", "y0", "core")
f32 = jnp.float32
bf16 = jnp.bfloat16


def _place():
    ring = [(0, z) for z in range(16)] + [(1, z) for z in range(15, -1, -1)]
    cycle = [(0, 0), (0, 1), (0, 2), (0, 3), (1, 3), (1, 2), (1, 1), (1, 0)]
    device = np.zeros((CBEADS, SLABS), np.int64)
    role = np.zeros((512, 2), np.int64)
    member = np.zeros((2, 16), np.int64)
    half_of = np.zeros(SLABS, np.int64)
    for s in range(SLABS):
        half, z = ring[(s - 8) % SLABS]
        half_of[s] = half
        for b in range(CBEADS):
            q, core = divmod(b, 2)
            xx, y = cycle[q]
            x = xx if half == 0 else 3 - xx
            d = ((z % 8) * 2 + core) * 32 + (z // 8) * 16 + x * 4 + y
            device[b, s] = d
            role[d] = (b, s)
            member[half, (x % 2) * 8 + y * 2 + core] = b
    return device, role, member, half_of


DEVICE, ROLE, MEMBER, HALF = _place()


def _table():
    b = np.arange(BEADS)[None, :] / BEADS
    c = np.arange(CBEADS)[:, None] / CBEADS
    t = 2.0 * np.pi * (b - c)
    total = 1.0 + np.cos(0.5 * CBEADS * t)
    for k in range(1, CBEADS // 2):
        total = total + 2.0 * np.cos(k * t)
    return (total / BEADS).astype(np.float32)


def _settings():
    table = _table()
    out = np.zeros((CBEADS * SLABS, 128), np.float32)
    for d in range(CBEADS * SLABS):
        b, s = ROLE[d]
        out[d, : 16 * MINE] = table[MEMBER[HALF[s]]][:, b * MINE : (b + 1) * MINE].reshape(-1)
        out[d, SLAB_AT] = s
        out[d, CORE_AT] = b % 2
        edges = table[MEMBER[HALF[s]]][:, [(b * MINE - 1) % BEADS, (b * MINE + MINE) % BEADS]]
        out[d, EDGE_AT : EDGE_AT + 32] = edges.reshape(-1)
    return out


SLAB_AT = 16 * MINE
CORE_AT = SLAB_AT + 1
EDGE_AT = SLAB_AT + 2
SETTINGS = _settings()


def _moves(f):
    return [
        (int(DEVICE[b, s]), int(DEVICE[f(b, s)]))
        for b in range(CBEADS)
        for s in range(SLABS)
    ]


SLAB_UP = _moves(lambda b, s: (b, (s + 1) % SLABS))
SLAB_DOWN = _moves(lambda b, s: (b, (s - 1) % SLABS))
BEAD_SWAP = _moves(lambda b, s: ((b + (1 if b % 2 else -1)) % CBEADS, s))
MOVE_IN = [(b * SLABS + s, int(DEVICE[b, s])) for b in range(CBEADS) for s in range(SLABS)]
MOVE_OUT = [(d, h) for h, d in MOVE_IN]


def pieces(v):
    high = v.astype(bf16).astype(f32)
    rest = v - high
    mid = rest.astype(bf16).astype(f32)
    return high, mid, rest - mid


def halves(lower, upper):
    return jnp.concatenate([lower, upper], axis=0)


def put(ref, row, value):
    ref[pl.ds(row, 8, stride=8), :] = value


def wide(ref):
    return jnp.concatenate([ref[8 * k : 8 * k + 8, :] for k in range(8)], axis=1)


def init_rows(src, tgt):
    ones = jnp.ones((8, 128), f32)
    zeros = jnp.zeros((8, 128), f32)
    put(src, 4, ones)
    put(tgt, 3, ones)
    for k in range(5, 8):
        put(src, k, zeros)
        put(tgt, k, zeros)


def scaled(coords, scale):
    alpha = math.sqrt(scale * math.log2(math.e))
    a = [alpha * y for y in coords]
    return a, -0.5 * (a[0] * a[0] + a[1] * a[1] + a[2] * a[2])


def put_sources(src, qs, lhs, coords, share, scale):
    a, norm = scaled(coords, scale)
    for k, v in enumerate(a + [norm]):
        put(src, k, v)
    for k, v in enumerate([share] + [share * y for y in coords]):
        put(qs, k, v)
        put(qs, 4 + k, v)
    high, mid, low = pieces(wide(src))
    rows = jnp.concatenate([high, high, mid, mid, high, low], axis=0)
    for block in range(8):
        part = slice(128 * block, 128 * block + 128)
        lhs[part, :] = rows[:, part].T.astype(bf16)
    high, mid, low = pieces(wide(qs))
    upper = lax.broadcasted_iota(jnp.int32, (8, 1024), 0) < 4
    return jnp.concatenate([jnp.where(upper, high, mid), jnp.where(upper, low, 0.0)], axis=0).astype(bf16)


def put_targets(tgt, coords, scale):
    a, norm = scaled(coords, scale)
    for k, v in enumerate(a):
        put(tgt, k, v)
    put(tgt, 4, norm)
    high, mid, low = pieces(wide(tgt))
    return jnp.concatenate([high, mid, high, mid, low, high], axis=0).astype(bf16)


def stream(tasks, ahead=AHEAD):
    totals = {}
    ready = []
    for t in range(len(tasks) + ahead):
        if t < len(tasks):
            lhs, first, rhs, q, key = tasks[t]
            ready.append(jnp.dot(lhs[first : first + STEP, :], rhs, preferred_element_type=f32))
        if t < ahead:
            continue
        lhs, first, rhs, q, key = tasks[t - ahead]
        weight = jnp.exp2(ready[t - ahead])
        high = weight.astype(bf16)
        low = (weight - high.astype(f32)).astype(bf16)
        mine = q[:, first : first + STEP]
        part = jnp.dot(mine, high, preferred_element_type=f32)
        part = part + jnp.dot(mine, low, preferred_element_type=f32)
        totals[key] = totals[key] + part if key in totals else part
    return totals


def chunks(lhs, first, last, rhs, start, stop, q, key):
    return [
        (lhs, j, rhs[:, i : i + WIDTH], q, (key, i))
        for j in range(first, last, STEP)
        for i in range(start, stop, WIDTH)
    ]


def joined(totals, key):
    return jnp.concatenate([totals[key, i] for i in range(0, 1024, WIDTH)], axis=1)


def sums_of(total, rows):
    r = total[0:8]
    r = r + jnp.concatenate([r[4:8], r[0:4]], axis=0) + total[8:16]
    for block in range(8):
        rows[8 * block : 8 * block + 8, :] = r[:, 128 * block : 128 * block + 128]
    return [rows[pl.ds(k, 8, stride=8), :] for k in range(4)]


def field(coords, sums, share, scale):
    return [share * scale * (coords[k] * sums[0] - sums[1 + k]) for k in range(3)]


def slot(scr, i):
    return scr[5 * i : 5 * i + 5]


SCRATCH = 2 * [
    pltpu.VMEM((64, 128), f32),
    pltpu.VMEM((64, 128), f32),
    pltpu.VMEM((64, 128), f32),
    pltpu.VMEM((1024, 48), bf16),
    pltpu.VMEM((64, 128), f32),
]


def bead_at(ref, b):
    return [ref[pl.ds(24 * b + 8 * k, 8), :] for k in range(3)]


def near_own_kernel(y_ref, p_ref, out_ref, *scr):
    share = p_ref[A_ROW : A_ROW + 8, :]
    for i in range(2):
        init_rows(*slot(scr, i)[:2])

    def two(i, carry):
        tasks = []
        for j in range(2):
            src, tgt, qs, lhs, _ = slot(scr, j)
            coords = bead_at(y_ref, 2 * i + j)
            q = put_sources(src, qs, lhs, coords, share, NEAR)
            rhs = put_targets(tgt, coords, NEAR)
            tasks += chunks(lhs, 0, 1024, rhs, 0, 1024, q, j)
        totals = stream(tasks)
        for j in range(2):
            for k, r in enumerate(sums_of(joined(totals, j), slot(scr, j)[4])):
                out_ref[pl.ds(64 * i + 32 * j + 8 * k, 8), :] = r
        return carry

    lax.fori_loop(0, MINE // 2, two, 0)


def emit(y_refs, up_ref, down_ref):
    for i in range(12):
        y = y_refs[8 * i : 8 * i + 8, :]
        down_ref[4 * i : 4 * i + 4, :] = y[0:4]
        up_ref[4 * i : 4 * i + 4, :] = y[4:8]


def emit_edges(first, last, inner_ref, outer_ref, core):
    odd = core > 0.5
    inner_ref[...] = jnp.where(odd, first, last)
    outer_ref[...] = jnp.where(odd, last, first)


def edges_of(inner, outer, core):
    odd = core > 0.5
    n = outer.shape[0]
    from_pair = jnp.where(odd, inner[0:n, :], inner[n : 2 * n, :])
    return jnp.where(odd, from_pair, outer[...]), jnp.where(odd, outer[...], from_pair)


def emit_partial(y_refs, cols_ref, part_ref):
    y = [y_refs[24 * b : 24 * b + 24, :] for b in range(MINE)]
    for r in range(16):
        total = cols_ref[0, MINE * r] * y[0]
        for b in range(1, MINE):
            total = total + cols_ref[0, MINE * r + b] * y[b]
        part_ref[24 * r : 24 * r + 24, :] = total


def spread(ref, out_ref, centre):
    for k in range(3):
        for block in range(8):
            value = ref[k, :, 128 * block : 128 * block + 128]
            out_ref[pl.ds(8 * k + block, 4, stride=24), :] = value if centre is None else value - centre[k]


def pack_kernel(v_ref, m_ref, a_ref, q_ref, out_ref):
    spread(v_ref, out_ref, None)
    out_ref[M_ROW : M_ROW + 8, :] = m_ref[...]
    out_ref[A_ROW : A_ROW + 8, :] = a_ref[...]
    out_ref[Q_ROW : Q_ROW + 8, :] = q_ref[...]


def unpack(value_ref, out_ref, base):
    for k in range(3):
        for block in range(8):
            out_ref[base + k, :, 128 * block : 128 * block + 128] = value_ref[pl.ds(8 * k + block, 4, stride=24), :]


def start_kernel(cols_ref, x_ref, y_ref, up_ref, down_ref, inner_ref, outer_ref, part_ref):
    spread(x_ref, y_ref, (2.0 * cols_ref[0, SLAB_AT] + 1.0, 1.0, 1.0))
    emit(y_ref, up_ref, down_ref)
    emit_edges(y_ref[0:24, :], y_ref[72:96, :], inner_ref, outer_ref, cols_ref[0, CORE_AT])
    emit_partial(y_ref, cols_ref, part_ref)


def near_halo_body(rate, p_ref, y_ref, v_ref, r_ref, left, right, wide_l, wide_r, edges, store, scr):
    chain = scr[10]
    for i in range(2):
        init_rows(*slot(scr, i)[:2])
    own = p_ref[A_ROW : A_ROW + 8, :]
    mass = p_ref[M_ROW : M_ROW + 8, :]
    inverse = 1.0 / mass
    share = halves(wide_l[WIDE + 4 : WIDE + 8, :], wide_r[WIDE : WIDE + 4, :])
    chain[0:24, :], chain[120:144, :] = edges
    chain[24:120, :] = y_ref[...]
    shift = jnp.where(lax.broadcasted_iota(jnp.int32, (8, 128), 0) < 4, -2.0, 2.0).astype(f32)

    def two(i, carry):
        at = pl.multiple_of(48 * i, 8)
        lows = left[pl.ds(pl.multiple_of(24 * i, 8), 24), :]
        highs = right[pl.ds(pl.multiple_of(24 * i, 8), 24), :]
        tasks = []
        places = []
        for j in range(2):
            src, tgt, qs, lhs, _ = slot(scr, j)
            coords = [y_ref[pl.ds(at + 24 * j + 8 * k, 8), :] for k in range(3)]
            far = []
            for k in range(3):
                h = 12 * j + 4 * k
                far.append(halves(lows[h : h + 4], highs[h : h + 4]))
            far[0] = far[0] + shift
            q = put_sources(src, qs, lhs, far, share, NEAR)
            rhs = put_targets(tgt, coords, NEAR)
            tasks += chunks(lhs, 0, 512, rhs, 0, 512, q, j)
            tasks += chunks(lhs, 512, 1024, rhs, 512, 1024, q, j)
            places.append(coords)
        totals = stream(tasks)
        for j in range(2):
            coords = places[j]
            sums = sums_of(joined(totals, j), slot(scr, j)[4])
            mine = pl.multiple_of(64 * i, 8) + 32 * j
            sums = [s + r_ref[pl.ds(mine + 8 * k, 8), :] for k, s in enumerate(sums)]
            force = field(coords, sums, own, NEAR)
            for k in range(3):
                r = at + 24 * j + 8 * k
                spring = 2.0 * coords[k] - chain[pl.ds(r, 8), :] - chain[pl.ds(r + 48, 8), :]
                total = force[k] - SPRING * mass * spring
                store(r, coords[k], v_ref[pl.ds(r, 8), :] + rate * total * inverse)
        return carry

    lax.fori_loop(0, MINE // 2, two, 0)


def near_slow_kernel(rate, cols_ref, p_ref, y_ref, v_ref, r_ref, left, right, wide_l, wide_r, vo_ref, *rest):
    def store(r, y, v):
        vo_ref[pl.ds(r, 8), :] = v

    none = jnp.zeros((24, 128), f32)
    scr = rest[-len(SCRATCH) - 1 :]
    near_halo_body(rate, p_ref, y_ref, v_ref, r_ref, left, right, wide_l, wide_r, (none, none), store, scr)
    if len(rest) > len(scr):
        ends = []
        for at in (0, 72):
            y = y_ref[at : at + 24, :]
            ends.append(jnp.concatenate([y, y + TIME_STEP * vo_ref[at : at + 24, :]], axis=0))
        emit_edges(ends[0], ends[1], rest[0], rest[1], cols_ref[0, CORE_AT])


def near_fast_kernel(cols_ref, p_ref, y_ref, v_ref, r_ref, left, right, wide_l, wide_r, before, after, *rest):
    vo_ref, yo_ref, up_ref, down_ref, in_ref, ou_ref, part_ref = rest[:7]
    scr = rest[7:]

    def store(r, y, v):
        vo_ref[pl.ds(r, 8), :] = v
        yo_ref[pl.ds(r, 8), :] = y + TIME_STEP * v

    edges = (before[...], after[...])
    near_halo_body(TIME_STEP, p_ref, y_ref, v_ref, r_ref, left, right, wide_l, wide_r, edges, store, scr)
    emit(yo_ref, up_ref, down_ref)
    emit_edges(yo_ref[0:24, :], yo_ref[72:96, :], in_ref, ou_ref, cols_ref[0, CORE_AT])
    emit_partial(yo_ref, cols_ref, part_ref)


def gather_kernel(wide, recv_ref, up_ref, down_ref, p_ref, yc_ref, up_out, down_out):
    total = recv_ref[0:24, :]
    for r in range(1, 16):
        total = total + recv_ref[24 * r : 24 * r + 24, :]
    yc_ref[...] = total
    for out, ref in ((up_out, up_ref), (down_out, down_ref)):
        out[0:48, :] = ref[...]
        out[48:72, :] = total
        if wide:
            out[WIDE : WIDE + 16, :] = p_ref[A_ROW : A_ROW + 16, :]


def far_own_kernel(yc_ref, p_ref, out_ref, src, tgt, qs, lhs, rows):
    init_rows(src, tgt)
    coords = bead_at(yc_ref, 0)
    q = put_sources(src, qs, lhs, coords, p_ref[Q_ROW : Q_ROW + 8, :], FAR)
    rhs = put_targets(tgt, coords, FAR)
    total = joined(stream(chunks(lhs, 0, 1024, rhs, 0, 1024, q, 0)), 0)
    for k, r in enumerate(sums_of(total, rows)):
        out_ref[8 * k : 8 * k + 8, :] = r


def far_halo_kernel(yc_ref, p_ref, r_ref, left, right, wide_l, wide_r, out_ref, *scr):
    coords = bead_at(yc_ref, 0)
    tasks = []
    for i, (block, rows) in enumerate(((left, wide_l), (right, wide_r))):
        src, tgt, qs, lhs, _ = slot(scr, i)
        init_rows(src, tgt)
        if i == 0:
            rhs = put_targets(tgt, coords, FAR)
        there = [block[48 + 8 * k : 56 + 8 * k, :] for k in range(3)]
        there[0] = there[0] + (2.0 if i else -2.0)
        q = put_sources(src, qs, lhs, there, rows[WIDE + 8 : WIDE + 16, :], FAR)
        if i == 0:
            tasks += chunks(lhs, 0, 512, rhs, 0, 512, q, 0)
            tasks += chunks(lhs, 512, 1024, rhs, 0, 1024, q, 0)
        else:
            tasks += chunks(lhs, 0, 512, rhs, 0, 1024, q, 0)
            tasks += chunks(lhs, 512, 1024, rhs, 512, 1024, q, 0)
    totals = stream(tasks)
    total = joined(totals, 0)
    sums = [s + r_ref[8 * k : 8 * k + 8, :] for k, s in enumerate(sums_of(total, slot(scr, 0)[4]))]
    force = field(coords, sums, p_ref[Q_ROW : Q_ROW + 8, :], FAR)
    for r in range(16):
        for k in range(3):
            out_ref[24 * r + 8 * k : 24 * r + 8 * k + 8, :] = force[k]


def kick(rate, cols_ref, p_ref, v_ref, far_ref):
    inverse = (rate * BEADS / CBEADS) / p_ref[M_ROW : M_ROW + 8, :]
    inverse = jnp.concatenate([inverse] * 3, axis=0)
    out = []
    far = [far_ref[24 * r : 24 * r + 24, :] for r in range(16)]
    for b in range(MINE):
        total = cols_ref[0, b] * far[0]
        for r in range(1, 16):
            total = total + cols_ref[0, MINE * r + b] * far[r]
        out.append(v_ref[24 * b : 24 * b + 24, :] + inverse * total)
    return out


def pulled(speeds, pull, before, after):
    speeds[0] = speeds[0] + pull * before
    speeds[-1] = speeds[-1] + pull * after
    return speeds


def update_kernel(near_rate, rate, cols_ref, p_ref, y_ref, v_ref, far_ref, inner, outer,
                  vo_ref, yo_ref, up_ref, down_ref, before_ref, after_ref):
    pull = near_rate * SPRING
    edges = edges_of(inner, outer, cols_ref[0, CORE_AT])
    speeds = pulled(kick(rate, cols_ref, p_ref, v_ref, far_ref), pull, edges[0][0:24], edges[1][0:24])
    for b, v in enumerate(speeds):
        vo_ref[24 * b : 24 * b + 24, :] = v
        yo_ref[24 * b : 24 * b + 24, :] = y_ref[24 * b : 24 * b + 24, :] + TIME_STEP * v
    emit(yo_ref, up_ref, down_ref)
    inverse = (TIME_STEP * rate * BEADS / CBEADS) / p_ref[M_ROW : M_ROW + 8, :]
    inverse = jnp.concatenate([inverse] * 3, axis=0)
    for e, out in enumerate((before_ref, after_ref)):
        total = cols_ref[0, EDGE_AT + e] * far_ref[0:24, :]
        for r in range(1, 16):
            total = total + cols_ref[0, EDGE_AT + 2 * r + e] * far_ref[24 * r : 24 * r + 24, :]
        out[...] = edges[e][24:48] + (TIME_STEP * pull) * y_ref[72 * e : 72 * e + 24, :] + inverse * total


def final_kernel(near_rate, rate, cols_ref, p_ref, v_ref, y_ref, first_ref, far_ref, inner, outer, out_ref, rows):
    for i in range(12):
        rows[8 * i : 8 * i + 8, :] = y_ref[8 * i : 8 * i + 8, :] - first_ref[8 * i : 8 * i + 8, :]
    unpack(rows, out_ref, 0)
    before, after = edges_of(inner, outer, cols_ref[0, CORE_AT])
    speeds = pulled(kick(rate, cols_ref, p_ref, v_ref, far_ref), near_rate * SPRING, before, after)
    for b, v in enumerate(speeds):
        rows[24 * b : 24 * b + 24, :] = v
    unpack(rows, out_ref, 3)


def call(kernel, outs, cols, args, scratch=(), flops=1000, order=(), passed=()):
    specs = [] if cols is None else [pl.BlockSpec(memory_space=pltpu.SMEM)]
    specs += [pl.BlockSpec(memory_space=pltpu.VMEM)] * len(args)
    used = len(specs)
    specs += [pl.BlockSpec(memory_space=pl.ANY)] * (len(order) + len(passed))
    given = ([] if cols is None else [cols]) + list(args) + list(order) + list(passed)
    base = used + len(order)

    def body(*refs):
        kernel(*refs[:used], *refs[len(given) : len(given) + len(outs)], *refs[len(given) + len(outs) + len(passed) :])

    shapes = [jax.ShapeDtypeStruct(s, f32) for s in outs] + [jax.ShapeDtypeStruct(x.shape, f32) for x in passed]
    return pl.pallas_call(
        body,
        out_shape=shapes,
        in_specs=specs,
        out_specs=[pl.BlockSpec(memory_space=pltpu.VMEM)] * len(outs) + [pl.BlockSpec(memory_space=pl.ANY)] * len(passed),
        scratch_shapes=list(scratch),
        input_output_aliases={base + i: len(outs) + i for i in range(len(passed))},
        cost_estimate=pl.CostEstimate(flops=flops, bytes_accessed=400000, transcendentals=0),
        compiler_params=pltpu.CompilerParams(vmem_limit_bytes=12 * 1024 * 1024),
    )(*given)


HALO = (48, 128)
BEAD = (24, 128)
STATE = (96, 128)
TEAM_ROWS = (16, 24, 128)
BOTH = (6, 4, 1024)


def exchange_team(x):
    x = lax.all_to_all(x.reshape(TEAM_ROWS), TEAM, split_axis=0, concat_axis=0, tiled=True)
    return x.reshape(384, 128)


def send(x, moves):
    return lax.ppermute(x, AXES, moves)


def pair(x):
    return lax.all_gather(x, "core", axis=0, tiled=True)


CHAIN = pltpu.VMEM((144, 128), f32)


def shards(positions, velocities, masses, amplitudes, charges):
    x = send(jnp.transpose(positions, (1, 0, 2)), MOVE_IN)
    (packed,) = call(
        pack_kernel,
        [(PACKED, 128)],
        None,
        [
            jnp.transpose(velocities, (1, 0, 2)),
            masses.reshape(8, 128),
            amplitudes.reshape(8, 128),
            charges.reshape(8, 128),
        ],
    )
    p = send(packed, MOVE_IN)
    cols = lax.dynamic_slice_in_dim(jnp.asarray(SETTINGS), lax.axis_index(AXES), 1, 0)
    y, up, down, inner, outer, part = call(start_kernel, [STATE, HALO, HALO, BEAD, BEAD, (384, 128)], cols, [x])
    first = y
    v = p
    wide_l = wide_r = None
    big = 400_000_000
    for stage in range(5):
        slow = stage % 2 == 0
        if not slow:
            left = send(up, SLAB_UP)
            right = send(down, SLAB_DOWN)
            (sums,) = call(near_own_kernel, [(128, 128)], None, [y, p], SCRATCH, big)
            v, y, up, down, inner, outer, part = call(
                near_fast_kernel,
                [STATE, STATE, HALO, HALO, BEAD, BEAD, (384, 128)],
                cols,
                [p, y, v, sums, left, right, wide_l, wide_r, before, after],
                SCRATCH + [CHAIN],
                big // 2,
            )
            continue
        edge = stage in (0, 4)
        got = exchange_team(part)
        if stage == 4:
            inner = pair(inner)
        (sums,) = call(near_own_kernel, [(128, 128)], None, [y, p], SCRATCH, big)

        def gather(*refs, wide=stage == 0):
            gather_kernel(wide, *refs)

        size = (WIDE + 16 * (stage == 0), 128)
        yc, up, down = call(gather, [BEAD, size, size], None, [got, up, down, p], order=[sums])
        left = send(up, SLAB_UP)
        right = send(down, SLAB_DOWN)
        if stage == 0:
            wide_l, wide_r = left, right
        (far_sums,) = call(far_own_kernel, [(32, 128)], None, [yc, p], SCRATCH[:5], big // 4)
        copies, *late = call(
            far_halo_kernel,
            [(384, 128)],
            None,
            [yc, p, far_sums, left, right, wide_l, wide_r],
            SCRATCH,
            big // 4,
            passed=[outer] * (stage == 4),
        )
        far = exchange_team(copies)
        if stage == 4:
            outer = send(late[0], BEAD_SWAP)
        near_rate = TIME_STEP * (0.5 if edge else 1.0)

        def near_slow(*refs, rate=near_rate):
            near_slow_kernel(rate, *refs)

        v, *ends = call(
            near_slow,
            [STATE] + [HALO] * (2 * (stage < 4)),
            cols,
            [p, y, v, sums, left, right, wide_l, wide_r],
            SCRATCH + [CHAIN],
            big // 2,
        )
        rate = OUTER_STEP * (0.5 if edge else 1.0)
        if stage == 4:

            def final(*refs, rate=rate, near_rate=near_rate):
                final_kernel(near_rate, rate, *refs)

            (both,) = call(final, [BOTH], cols, [p, v, y, first, far, inner, outer], [pltpu.VMEM(STATE, f32)])
        else:

            def update(*refs, rate=rate, near_rate=near_rate):
                update_kernel(near_rate, rate, *refs)

            inner = pair(ends[0])
            outer = send(ends[1], BEAD_SWAP)
            v, y, up, down, before, after = call(
                update, [STATE, STATE, HALO, HALO, BEAD, BEAD], cols, [p, y, v, far, inner, outer]
            )
    both = jnp.transpose(lax.ppermute(both, AXES, MOVE_OUT), (1, 0, 2))
    return both[:, 0:3], both[:, 3:6]


def solution(mesh):
    fine = Mesh(mesh.devices.reshape((2,) * 9), AXES)
    bead = ("z2", "z1", "z0", "core")
    slab = ("zh", "x1", "x0", "y1", "y0")
    wide = P(bead, None, slab)
    flat = P(slab)
    return jax.shard_map(
        shards,
        mesh=fine,
        in_specs=(wide, wide, flat, flat, flat),
        out_specs=(wide, wide),
        check_vma=False,
    )
```

```python
import math

import jax
import jax.numpy as jnp
import numpy as np
from jax import lax
from jax.experimental import pallas as pl
from jax.experimental.pallas import tpu as pltpu
from jax.sharding import Mesh, PartitionSpec as P


TIME_STEP = 0.05
OUTER_STEP = 0.1
SPRING = 25.0
NEAR = 4.0
FAR = 2.0
BEADS = 64
CBEADS = 16
SLABS = 32
MINE = BEADS // CBEADS
STEP = 256
WIDTH = 256
AHEAD = 4

M_ROW = 96
A_ROW = 104
Q_ROW = 112
PACKED = 120
WIDE = 72

AXES = ("z2", "z1", "z0", "core", "zh", "x1", "x0", "y1", "y0")
TEAM = ("x0", "y1", "y0", "core")
f32 = jnp.float32
bf16 = jnp.bfloat16


def _place():
    ring = [((0, 1, 1, 0)[s % 4], s // 2) for s in range(SLABS)]
    cycle = [(0, 0), (0, 1), (0, 2), (0, 3), (1, 3), (1, 2), (1, 1), (1, 0)]
    device = np.zeros((CBEADS, SLABS), np.int64)
    role = np.zeros((512, 2), np.int64)
    member = np.zeros((2, 16), np.int64)
    half_of = np.zeros(SLABS, np.int64)
    for s in range(SLABS):
        half, z = ring[s]
        half_of[s] = half
        for b in range(CBEADS):
            q, core = divmod(b, 2)
            xx, y = cycle[(q + 2) % 8]
            x = xx if half == 0 else 3 - xx
            d = ((z % 8) * 2 + core) * 32 + (z // 8) * 16 + x * 4 + y
            device[b, s] = d
            role[d] = (b, s)
            member[half, (x % 2) * 8 + y * 2 + core] = b
    return device, role, member, half_of


DEVICE, ROLE, MEMBER, HALF = _place()


def _table():
    b = np.arange(BEADS)[None, :] / BEADS
    c = np.arange(CBEADS)[:, None] / CBEADS
    t = 2.0 * np.pi * (b - c)
    total = 1.0 + np.cos(0.5 * CBEADS * t)
    for k in range(1, CBEADS // 2):
        total = total + 2.0 * np.cos(k * t)
    return (total / BEADS).astype(np.float32)


def _settings():
    table = _table()
    out = np.zeros((CBEADS * SLABS, 128), np.float32)
    for d in range(CBEADS * SLABS):
        b, s = ROLE[d]
        out[d, : 16 * MINE] = table[MEMBER[HALF[s]]][:, b * MINE : (b + 1) * MINE].reshape(-1)
        out[d, SLAB_AT] = s
        out[d, CORE_AT] = b % 2
        edges = table[MEMBER[HALF[s]]][:, [(b * MINE - 1) % BEADS, (b * MINE + MINE) % BEADS]]
        out[d, EDGE_AT : EDGE_AT + 32] = edges.reshape(-1)
    return out


SLAB_AT = 16 * MINE
CORE_AT = SLAB_AT + 1
EDGE_AT = SLAB_AT + 2
SETTINGS = _settings()


def _moves(f):
    return [
        (int(DEVICE[b, s]), int(DEVICE[f(b, s)]))
        for b in range(CBEADS)
        for s in range(SLABS)
    ]


SLAB_UP = _moves(lambda b, s: (b, (s + 1) % SLABS))
SLAB_DOWN = _moves(lambda b, s: (b, (s - 1) % SLABS))
BEAD_SWAP = _moves(lambda b, s: ((b + (1 if b % 2 else -1)) % CBEADS, s))
MOVE_IN = [(b * SLABS + s, int(DEVICE[b, s])) for b in range(CBEADS) for s in range(SLABS)]
MOVE_OUT = [(d, h) for h, d in MOVE_IN]


def pieces(v):
    high = v.astype(bf16).astype(f32)
    rest = v - high
    mid = rest.astype(bf16).astype(f32)
    return high, mid, rest - mid


def halves(lower, upper):
    return jnp.concatenate([lower, upper], axis=0)


def put(ref, row, value):
    ref[pl.ds(row, 8, stride=8), :] = value


def wide(ref):
    return jnp.concatenate([ref[8 * k : 8 * k + 8, :] for k in range(8)], axis=1)


def init_rows(src, tgt):
    ones = jnp.ones((8, 128), f32)
    zeros = jnp.zeros((8, 128), f32)
    put(src, 4, ones)
    put(tgt, 3, ones)
    for k in range(5, 8):
        put(src, k, zeros)
        put(tgt, k, zeros)


def scaled(coords, scale):
    alpha = math.sqrt(scale * math.log2(math.e))
    a = [alpha * y for y in coords]
    return a, -0.5 * (a[0] * a[0] + a[1] * a[1] + a[2] * a[2])


def put_sources(src, qs, lhs, coords, share, scale):
    a, norm = scaled(coords, scale)
    for k, v in enumerate(a + [norm]):
        put(src, k, v)
    for k, v in enumerate([share] + [share * y for y in coords]):
        put(qs, k, v)
        put(qs, 4 + k, v)
    high, mid, low = pieces(wide(src))
    rows = jnp.concatenate([high, high, mid, mid, high, low], axis=0)
    for block in range(8):
        part = slice(128 * block, 128 * block + 128)
        lhs[part, :] = rows[:, part].T.astype(bf16)
    high, mid, low = pieces(wide(qs))
    upper = lax.broadcasted_iota(jnp.int32, (8, 1024), 0) < 4
    return jnp.concatenate([jnp.where(upper, high, mid), jnp.where(upper, low, 0.0)], axis=0).astype(bf16)


def put_targets(tgt, coords, scale):
    a, norm = scaled(coords, scale)
    for k, v in enumerate(a):
        put(tgt, k, v)
    put(tgt, 4, norm)
    high, mid, low = pieces(wide(tgt))
    return jnp.concatenate([high, mid, high, mid, low, high], axis=0).astype(bf16)


def stream(tasks, ahead=AHEAD):
    totals = {}
    ready = []
    for t in range(len(tasks) + ahead):
        if t < len(tasks):
            lhs, first, rhs, q, key = tasks[t]
            ready.append(jnp.dot(lhs[first : first + STEP, :], rhs, preferred_element_type=f32))
        if t < ahead:
            continue
        lhs, first, rhs, q, key = tasks[t - ahead]
        weight = jnp.exp2(ready[t - ahead])
        high = weight.astype(bf16)
        low = (weight - high.astype(f32)).astype(bf16)
        mine = q[:, first : first + STEP]
        part = jnp.dot(mine, high, preferred_element_type=f32)
        part = part + jnp.dot(mine, low, preferred_element_type=f32)
        totals[key] = totals[key] + part if key in totals else part
    return totals


def chunks(lhs, first, last, rhs, start, stop, q, key):
    return [
        (lhs, j, rhs[:, i : i + WIDTH], q, (key, i))
        for j in range(first, last, STEP)
        for i in range(start, stop, WIDTH)
    ]


def joined(totals, key):
    return jnp.concatenate([totals[key, i] for i in range(0, 1024, WIDTH)], axis=1)


def sums_of(total, rows):
    r = total[0:8]
    r = r + jnp.concatenate([r[4:8], r[0:4]], axis=0) + total[8:16]
    for block in range(8):
        rows[8 * block : 8 * block + 8, :] = r[:, 128 * block : 128 * block + 128]
    return [rows[pl.ds(k, 8, stride=8), :] for k in range(4)]


def field(coords, sums, share, scale):
    return [share * scale * (coords[k] * sums[0] - sums[1 + k]) for k in range(3)]


def slot(scr, i):
    return scr[5 * i : 5 * i + 5]


SCRATCH = 2 * [
    pltpu.VMEM((64, 128), f32),
    pltpu.VMEM((64, 128), f32),
    pltpu.VMEM((64, 128), f32),
    pltpu.VMEM((1024, 48), bf16),
    pltpu.VMEM((64, 128), f32),
]


def bead_at(ref, b):
    return [ref[pl.ds(24 * b + 8 * k, 8), :] for k in range(3)]


def near_own_kernel(y_ref, p_ref, out_ref, *scr):
    share = p_ref[A_ROW : A_ROW + 8, :]
    for i in range(2):
        init_rows(*slot(scr, i)[:2])

    def two(i, carry):
        tasks = []
        for j in range(2):
            src, tgt, qs, lhs, _ = slot(scr, j)
            coords = bead_at(y_ref, 2 * i + j)
            q = put_sources(src, qs, lhs, coords, share, NEAR)
            rhs = put_targets(tgt, coords, NEAR)
            tasks += chunks(lhs, 0, 1024, rhs, 0, 1024, q, j)
        totals = stream(tasks)
        for j in range(2):
            for k, r in enumerate(sums_of(joined(totals, j), slot(scr, j)[4])):
                out_ref[pl.ds(64 * i + 32 * j + 8 * k, 8), :] = r
        return carry

    lax.fori_loop(0, MINE // 2, two, 0)


def emit(y_refs, up_ref, down_ref):
    for i in range(12):
        y = y_refs[8 * i : 8 * i + 8, :]
        down_ref[4 * i : 4 * i + 4, :] = y[0:4]
        up_ref[4 * i : 4 * i + 4, :] = y[4:8]


def emit_edges(first, last, inner_ref, outer_ref, core):
    odd = core > 0.5
    inner_ref[...] = jnp.where(odd, first, last)
    outer_ref[...] = jnp.where(odd, last, first)


def edges_of(inner, outer, core):
    odd = core > 0.5
    n = outer.shape[0]
    from_pair = jnp.where(odd, inner[0:n, :], inner[n : 2 * n, :])
    return jnp.where(odd, from_pair, outer[...]), jnp.where(odd, outer[...], from_pair)


def emit_partial(y_refs, cols_ref, part_ref):
    y = [y_refs[24 * b : 24 * b + 24, :] for b in range(MINE)]
    for r in range(16):
        total = cols_ref[0, MINE * r] * y[0]
        for b in range(1, MINE):
            total = total + cols_ref[0, MINE * r + b] * y[b]
        part_ref[24 * r : 24 * r + 24, :] = total


def spread(ref, out_ref, centre):
    for k in range(3):
        for block in range(8):
            value = ref[k, :, 128 * block : 128 * block + 128]
            out_ref[pl.ds(8 * k + block, 4, stride=24), :] = value if centre is None else value - centre[k]


def pack_kernel(v_ref, m_ref, a_ref, q_ref, out_ref):
    spread(v_ref, out_ref, None)
    out_ref[M_ROW : M_ROW + 8, :] = m_ref[...]
    out_ref[A_ROW : A_ROW + 8, :] = a_ref[...]
    out_ref[Q_ROW : Q_ROW + 8, :] = q_ref[...]


def unpack(value_ref, out_ref, base):
    for k in range(3):
        for block in range(8):
            out_ref[base + k, :, 128 * block : 128 * block + 128] = value_ref[pl.ds(8 * k + block, 4, stride=24), :]


def start_kernel(cols_ref, x_ref, y_ref, up_ref, down_ref, inner_ref, outer_ref, part_ref):
    spread(x_ref, y_ref, (2.0 * cols_ref[0, SLAB_AT] + 1.0, 1.0, 1.0))
    emit(y_ref, up_ref, down_ref)
    emit_edges(y_ref[0:24, :], y_ref[72:96, :], inner_ref, outer_ref, cols_ref[0, CORE_AT])
    emit_partial(y_ref, cols_ref, part_ref)


def near_halo_body(rate, p_ref, y_ref, v_ref, r_ref, left, right, wide_l, wide_r, edges, store, scr):
    chain = scr[10]
    for i in range(2):
        init_rows(*slot(scr, i)[:2])
    own = p_ref[A_ROW : A_ROW + 8, :]
    mass = p_ref[M_ROW : M_ROW + 8, :]
    inverse = 1.0 / mass
    share = halves(wide_l[WIDE + 4 : WIDE + 8, :], wide_r[WIDE : WIDE + 4, :])
    chain[0:24, :], chain[120:144, :] = edges
    chain[24:120, :] = y_ref[...]
    shift = jnp.where(lax.broadcasted_iota(jnp.int32, (8, 128), 0) < 4, -2.0, 2.0).astype(f32)

    def two(i, carry):
        at = pl.multiple_of(48 * i, 8)
        lows = left[pl.ds(pl.multiple_of(24 * i, 8), 24), :]
        highs = right[pl.ds(pl.multiple_of(24 * i, 8), 24), :]
        tasks = []
        places = []
        for j in range(2):
            src, tgt, qs, lhs, _ = slot(scr, j)
            coords = [y_ref[pl.ds(at + 24 * j + 8 * k, 8), :] for k in range(3)]
            far = []
            for k in range(3):
                h = 12 * j + 4 * k
                far.append(halves(lows[h : h + 4], highs[h : h + 4]))
            far[0] = far[0] + shift
            q = put_sources(src, qs, lhs, far, share, NEAR)
            rhs = put_targets(tgt, coords, NEAR)
            tasks += chunks(lhs, 0, 512, rhs, 0, 512, q, j)
            tasks += chunks(lhs, 512, 1024, rhs, 512, 1024, q, j)
            places.append(coords)
        totals = stream(tasks)
        for j in range(2):
            coords = places[j]
            sums = sums_of(joined(totals, j), slot(scr, j)[4])
            mine = pl.multiple_of(64 * i, 8) + 32 * j
            sums = [s + r_ref[pl.ds(mine + 8 * k, 8), :] for k, s in enumerate(sums)]
            force = field(coords, sums, own, NEAR)
            for k in range(3):
                r = at + 24 * j + 8 * k
                spring = 2.0 * coords[k] - chain[pl.ds(r, 8), :] - chain[pl.ds(r + 48, 8), :]
                total = force[k] - SPRING * mass * spring
                store(r, coords[k], v_ref[pl.ds(r, 8), :] + rate * total * inverse)
        return carry

    lax.fori_loop(0, MINE // 2, two, 0)


def near_slow_kernel(rate, cols_ref, p_ref, y_ref, v_ref, r_ref, left, right, wide_l, wide_r, vo_ref, *rest):
    def store(r, y, v):
        vo_ref[pl.ds(r, 8), :] = v

    none = jnp.zeros((24, 128), f32)
    scr = rest[-len(SCRATCH) - 1 :]
    near_halo_body(rate, p_ref, y_ref, v_ref, r_ref, left, right, wide_l, wide_r, (none, none), store, scr)
    if len(rest) > len(scr):
        ends = []
        for at in (0, 72):
            y = y_ref[at : at + 24, :]
            ends.append(jnp.concatenate([y, y + TIME_STEP * vo_ref[at : at + 24, :]], axis=0))
        emit_edges(ends[0], ends[1], rest[0], rest[1], cols_ref[0, CORE_AT])


def near_fast_kernel(cols_ref, p_ref, y_ref, v_ref, r_ref, left, right, wide_l, wide_r, before, after, *rest):
    vo_ref, yo_ref, up_ref, down_ref, in_ref, ou_ref, part_ref = rest[:7]
    scr = rest[7:]

    def store(r, y, v):
        vo_ref[pl.ds(r, 8), :] = v
        yo_ref[pl.ds(r, 8), :] = y + TIME_STEP * v

    edges = (before[...], after[...])
    near_halo_body(TIME_STEP, p_ref, y_ref, v_ref, r_ref, left, right, wide_l, wide_r, edges, store, scr)
    emit(yo_ref, up_ref, down_ref)
    emit_edges(yo_ref[0:24, :], yo_ref[72:96, :], in_ref, ou_ref, cols_ref[0, CORE_AT])
    emit_partial(yo_ref, cols_ref, part_ref)


def gather_kernel(wide, recv_ref, up_ref, down_ref, p_ref, yc_ref, up_out, down_out):
    total = recv_ref[0:24, :]
    for r in range(1, 16):
        total = total + recv_ref[24 * r : 24 * r + 24, :]
    yc_ref[...] = total
    for out, ref in ((up_out, up_ref), (down_out, down_ref)):
        out[0:48, :] = ref[...]
        out[48:72, :] = total
        if wide:
            out[WIDE : WIDE + 16, :] = p_ref[A_ROW : A_ROW + 16, :]


def far_own_kernel(yc_ref, p_ref, out_ref, src, tgt, qs, lhs, rows):
    init_rows(src, tgt)
    coords = bead_at(yc_ref, 0)
    q = put_sources(src, qs, lhs, coords, p_ref[Q_ROW : Q_ROW + 8, :], FAR)
    rhs = put_targets(tgt, coords, FAR)
    total = joined(stream(chunks(lhs, 0, 1024, rhs, 0, 1024, q, 0)), 0)
    for k, r in enumerate(sums_of(total, rows)):
        out_ref[8 * k : 8 * k + 8, :] = r


def far_halo_kernel(yc_ref, p_ref, r_ref, left, right, wide_l, wide_r, out_ref, *scr):
    coords = bead_at(yc_ref, 0)
    tasks = []
    for i, (block, rows) in enumerate(((left, wide_l), (right, wide_r))):
        src, tgt, qs, lhs, _ = slot(scr, i)
        init_rows(src, tgt)
        if i == 0:
            rhs = put_targets(tgt, coords, FAR)
        there = [block[48 + 8 * k : 56 + 8 * k, :] for k in range(3)]
        there[0] = there[0] + (2.0 if i else -2.0)
        q = put_sources(src, qs, lhs, there, rows[WIDE + 8 : WIDE + 16, :], FAR)
        if i == 0:
            tasks += chunks(lhs, 0, 512, rhs, 0, 512, q, 0)
            tasks += chunks(lhs, 512, 1024, rhs, 0, 1024, q, 0)
        else:
            tasks += chunks(lhs, 0, 512, rhs, 0, 1024, q, 0)
            tasks += chunks(lhs, 512, 1024, rhs, 512, 1024, q, 0)
    totals = stream(tasks)
    total = joined(totals, 0)
    sums = [s + r_ref[8 * k : 8 * k + 8, :] for k, s in enumerate(sums_of(total, slot(scr, 0)[4]))]
    force = field(coords, sums, p_ref[Q_ROW : Q_ROW + 8, :], FAR)
    for r in range(16):
        for k in range(3):
            out_ref[24 * r + 8 * k : 24 * r + 8 * k + 8, :] = force[k]


def kick(rate, cols_ref, p_ref, v_ref, far_ref):
    inverse = (rate * BEADS / CBEADS) / p_ref[M_ROW : M_ROW + 8, :]
    inverse = jnp.concatenate([inverse] * 3, axis=0)
    out = []
    far = [far_ref[24 * r : 24 * r + 24, :] for r in range(16)]
    for b in range(MINE):
        total = cols_ref[0, b] * far[0]
        for r in range(1, 16):
            total = total + cols_ref[0, MINE * r + b] * far[r]
        out.append(v_ref[24 * b : 24 * b + 24, :] + inverse * total)
    return out


def pulled(speeds, pull, before, after):
    speeds[0] = speeds[0] + pull * before
    speeds[-1] = speeds[-1] + pull * after
    return speeds


def update_kernel(near_rate, rate, cols_ref, p_ref, y_ref, v_ref, far_ref, inner, outer,
                  vo_ref, yo_ref, up_ref, down_ref, before_ref, after_ref):
    pull = near_rate * SPRING
    edges = edges_of(inner, outer, cols_ref[0, CORE_AT])
    speeds = pulled(kick(rate, cols_ref, p_ref, v_ref, far_ref), pull, edges[0][0:24], edges[1][0:24])
    for b, v in enumerate(speeds):
        vo_ref[24 * b : 24 * b + 24, :] = v
        yo_ref[24 * b : 24 * b + 24, :] = y_ref[24 * b : 24 * b + 24, :] + TIME_STEP * v
    emit(yo_ref, up_ref, down_ref)
    inverse = (TIME_STEP * rate * BEADS / CBEADS) / p_ref[M_ROW : M_ROW + 8, :]
    inverse = jnp.concatenate([inverse] * 3, axis=0)
    for e, out in enumerate((before_ref, after_ref)):
        total = cols_ref[0, EDGE_AT + e] * far_ref[0:24, :]
        for r in range(1, 16):
            total = total + cols_ref[0, EDGE_AT + 2 * r + e] * far_ref[24 * r : 24 * r + 24, :]
        out[...] = edges[e][24:48] + (TIME_STEP * pull) * y_ref[72 * e : 72 * e + 24, :] + inverse * total


def final_kernel(near_rate, rate, cols_ref, p_ref, v_ref, y_ref, first_ref, far_ref, inner, outer, out_ref, rows):
    for i in range(12):
        rows[8 * i : 8 * i + 8, :] = y_ref[8 * i : 8 * i + 8, :] - first_ref[8 * i : 8 * i + 8, :]
    unpack(rows, out_ref, 0)
    before, after = edges_of(inner, outer, cols_ref[0, CORE_AT])
    speeds = pulled(kick(rate, cols_ref, p_ref, v_ref, far_ref), near_rate * SPRING, before, after)
    for b, v in enumerate(speeds):
        rows[24 * b : 24 * b + 24, :] = v
    unpack(rows, out_ref, 3)


def call(kernel, outs, cols, args, scratch=(), flops=1000, order=(), passed=()):
    specs = [] if cols is None else [pl.BlockSpec(memory_space=pltpu.SMEM)]
    specs += [pl.BlockSpec(memory_space=pltpu.VMEM)] * len(args)
    used = len(specs)
    specs += [pl.BlockSpec(memory_space=pl.ANY)] * (len(order) + len(passed))
    given = ([] if cols is None else [cols]) + list(args) + list(order) + list(passed)
    base = used + len(order)

    def body(*refs):
        kernel(*refs[:used], *refs[len(given) : len(given) + len(outs)], *refs[len(given) + len(outs) + len(passed) :])

    shapes = [jax.ShapeDtypeStruct(s, f32) for s in outs] + [jax.ShapeDtypeStruct(x.shape, f32) for x in passed]
    return pl.pallas_call(
        body,
        out_shape=shapes,
        in_specs=specs,
        out_specs=[pl.BlockSpec(memory_space=pltpu.VMEM)] * len(outs) + [pl.BlockSpec(memory_space=pl.ANY)] * len(passed),
        scratch_shapes=list(scratch),
        input_output_aliases={base + i: len(outs) + i for i in range(len(passed))},
        cost_estimate=pl.CostEstimate(flops=flops, bytes_accessed=400000, transcendentals=0),
        compiler_params=pltpu.CompilerParams(vmem_limit_bytes=12 * 1024 * 1024),
    )(*given)


HALO = (48, 128)
BEAD = (24, 128)
STATE = (96, 128)
TEAM_ROWS = (16, 24, 128)
BOTH = (6, 4, 1024)


def exchange_team(x):
    x = lax.all_to_all(x.reshape(TEAM_ROWS), TEAM, split_axis=0, concat_axis=0, tiled=True)
    return x.reshape(384, 128)


def send(x, moves):
    return lax.ppermute(x, AXES, moves)


def pair(x):
    return lax.all_gather(x, "core", axis=0, tiled=True)


CHAIN = pltpu.VMEM((144, 128), f32)


def shards(positions, velocities, masses, amplitudes, charges):
    x = send(jnp.transpose(positions, (1, 0, 2)), MOVE_IN)
    (packed,) = call(
        pack_kernel,
        [(PACKED, 128)],
        None,
        [
            jnp.transpose(velocities, (1, 0, 2)),
            masses.reshape(8, 128),
            amplitudes.reshape(8, 128),
            charges.reshape(8, 128),
        ],
    )
    p = send(packed, MOVE_IN)
    cols = lax.dynamic_slice_in_dim(jnp.asarray(SETTINGS), lax.axis_index(AXES), 1, 0)
    y, up, down, inner, outer, part = call(start_kernel, [STATE, HALO, HALO, BEAD, BEAD, (384, 128)], cols, [x])
    first = y
    v = p
    wide_l = wide_r = None
    big = 400_000_000
    for stage in range(5):
        slow = stage % 2 == 0
        if not slow:
            left = send(up, SLAB_UP)
            right = send(down, SLAB_DOWN)
            (sums,) = call(near_own_kernel, [(128, 128)], None, [y, p], SCRATCH, big)
            v, y, up, down, inner, outer, part = call(
                near_fast_kernel,
                [STATE, STATE, HALO, HALO, BEAD, BEAD, (384, 128)],
                cols,
                [p, y, v, sums, left, right, wide_l, wide_r, before, after],
                SCRATCH + [CHAIN],
                big // 2,
            )
            continue
        edge = stage in (0, 4)
        got = exchange_team(part)
        if stage == 4:
            inner = pair(inner)
        (sums,) = call(near_own_kernel, [(128, 128)], None, [y, p], SCRATCH, big)

        def gather(*refs, wide=stage == 0):
            gather_kernel(wide, *refs)

        size = (WIDE + 16 * (stage == 0), 128)
        yc, up, down = call(gather, [BEAD, size, size], None, [got, up, down, p], order=[sums])
        left = send(up, SLAB_UP)
        right = send(down, SLAB_DOWN)
        if stage == 0:
            wide_l, wide_r = left, right
        (far_sums,) = call(far_own_kernel, [(32, 128)], None, [yc, p], SCRATCH[:5], big // 4)
        copies, *late = call(
            far_halo_kernel,
            [(384, 128)],
            None,
            [yc, p, far_sums, left, right, wide_l, wide_r],
            SCRATCH,
            big // 4,
            passed=[outer] * (stage == 4),
        )
        far = exchange_team(copies)
        if stage == 4:
            outer = send(late[0], BEAD_SWAP)
        near_rate = TIME_STEP * (0.5 if edge else 1.0)

        def near_slow(*refs, rate=near_rate):
            near_slow_kernel(rate, *refs)

        v, *ends = call(
            near_slow,
            [STATE] + [HALO] * (2 * (stage < 4)),
            cols,
            [p, y, v, sums, left, right, wide_l, wide_r],
            SCRATCH + [CHAIN],
            big // 2,
        )
        rate = OUTER_STEP * (0.5 if edge else 1.0)
        if stage == 4:

            def final(*refs, rate=rate, near_rate=near_rate):
                final_kernel(near_rate, rate, *refs)

            (both,) = call(final, [BOTH], cols, [p, v, y, first, far, inner, outer], [pltpu.VMEM(STATE, f32)])
        else:

            def update(*refs, rate=rate, near_rate=near_rate):
                update_kernel(near_rate, rate, *refs)

            inner = pair(ends[0])
            outer = send(ends[1], BEAD_SWAP)
            v, y, up, down, before, after = call(
                update, [STATE, STATE, HALO, HALO, BEAD, BEAD], cols, [p, y, v, far, inner, outer]
            )
    both = jnp.transpose(lax.ppermute(both, AXES, MOVE_OUT), (1, 0, 2))
    return both[:, 0:3], both[:, 3:6]


def solution(mesh):
    fine = Mesh(mesh.devices.reshape((2,) * 9), AXES)
    bead = ("z2", "z1", "z0", "core")
    slab = ("zh", "x1", "x0", "y1", "y0")
    wide = P(bead, None, slab)
    flat = P(slab)
    return jax.shard_map(
        shards,
        mesh=fine,
        in_specs=(wide, wide, flat, flat, flat),
        out_specs=(wide, wide),
        check_vma=False,
    )
```
